128 devices in a mesh: dp: 2 (over core), seq: 16 (over y, x), tensor: 4 (over z).
Axes of the slice: x: 4, y: 4, z: 4, core: 2. Of those that a mesh axis runs over, the one named last changes fastest.
Arguments:
- tokens: bfloat16 [2, 8192, 2048], P('dp', ('seq', 'tensor')), may hold values from -6 to 6
- attn_gain: float32 [2048], replicated, may hold values from 0.5 to 1.5
- w_qkv: bfloat16 [3, 2048, 2048], P(None, None, 'tensor'), may hold values from -1 to 1
- w_out: bfloat16 [2048, 2048], P('tensor'), may hold values from -0.125 to 0.125
- mlp_gain: float32 [2048], replicated, may hold values from 0.5 to 1.5
- w_up: bfloat16 [2048, 8192], P(None, 'tensor'), may hold values from -0.125 to 0.125
- w_down: bfloat16 [8192, 2048], P('tensor'), may hold values from -0.0625 to 0.0625
- pool_gain: float32 [2048], replicated, may hold values from -8 to 8
- pool_bias: float32 [2048], replicated, may hold values from 0.5 to 5
- value_weight: float32 [2048], replicated, may hold values from -6 to 6
- valid_frames: int32 [2], replicated, may hold values from 16 to 32, as said below
Outputs:
- hidden: bfloat16 [2, 8192, 2048], P('dp', ('seq', 'tensor'))
- frame_values: float32 [2, 32], P('dp', 'seq')
- advantages: float32 [2, 32], P('dp', 'seq')
The draws below stay inside these ranges and needn't reach their ends.
Inputs may be any that keep to these rules, and one draw needn't show every extreme that they name: `valid_frames`: at least one rollout keeps all 32 frames and at least one keeps 32 // 2 of them.
All inputs are finite; a program needn't handle non-finite values.
Results may differ from the reference program's by a relative error of at most 0.017.
Values may be sent and summed in bfloat16 or wider, within the bound.
A program may use at most 256 MiB of HBM per device.

```python
import jax
import jax.numpy as jnp
from jax import lax

D = 2048
HEADS = 16
HEAD_DIM = 128
FF = 8192
TOK_FRAME = 256
FRAMES = 32
TOKENS = 8192
ROLLOUTS = 2


def draw_tokens(key, part):
    noise_key = jax.random.fold_in(key, 11)
    values = jax.random.truncated_normal(noise_key, -6.0, 6.0, (ROLLOUTS, TOKENS, D), jnp.float32)
    return values.astype(jnp.bfloat16)


def draw_w_qkv(key, part):
    base = jax.random.truncated_normal(jax.random.fold_in(key, 21), -6.0, 6.0, (3, D, D), jnp.float32) / jnp.sqrt(jnp.float32(D))
    return base.astype(jnp.bfloat16)


def draw_valid_frames(key, part):
    base = jax.random.randint(jax.random.fold_in(key, 31), (ROLLOUTS,), FRAMES // 2, FRAMES + 1, dtype=jnp.int32)
    rank = jax.random.permutation(jax.random.fold_in(key, 32), jnp.arange(ROLLOUTS, dtype=jnp.int32))
    longest = jnp.full((ROLLOUTS,), FRAMES, jnp.int32)
    shortest = jnp.full((ROLLOUTS,), FRAMES // 2, jnp.int32)
    return jnp.where(rank == 0, longest, jnp.where(rank == 1, shortest, base)).astype(jnp.int32)


def shard_levels(stream_key, shape, split, least, high):
    level = 1.0
    for dim, parts in split:
        heights = jax.random.uniform(jax.random.fold_in(jax.random.fold_in(stream_key, 6), dim), (parts,), jnp.float32, least / len(split), high / len(split))
        level = level * jnp.repeat(jnp.exp(heights), shape[dim] // parts).reshape((-1,) + (1,) * (len(shape) - 1 - dim))
    return level


def normal_values(rng, dims, scale, reach, shards=(), held_as=jnp.bfloat16):
    array = scale * jax.random.normal(rng, dims, jnp.float32)
    if shards:
        array = array * shard_levels(rng, dims, shards, -0.22, 0.18)
    return jnp.clip(array, -reach, reach).astype(held_as)


def setup_inputs(seed: int = 0) -> dict:
    key_list = jax.random.split(jax.random.key(seed), 12)
    tokens = draw_tokens(jax.random.fold_in(key_list[11], 71), 0)
    attn_gain = jnp.clip(1.0 + 0.1 * jax.random.normal(key_list[1], (D,), jnp.float32), 0.5, 1.5)
    w_qkv = draw_w_qkv(jax.random.fold_in(key_list[11], 71), 0)
    w_out = normal_values(key_list[3], (D, D), D ** -0.5, 0.125, ((0, 4),))
    mlp_gain = jnp.clip(1.0 + 0.1 * jax.random.normal(key_list[4], (D,), jnp.float32), 0.5, 1.5)
    w_up = normal_values(key_list[5], (D, FF), D ** -0.5, 0.125, ((1, 4),))
    w_down = normal_values(key_list[6], (FF, D), FF ** -0.5, 0.0625, ((0, 4),))
    pool_gain = jnp.clip(jax.random.uniform(key_list[7], (D,), jnp.float32, -8.0, 8.0), -8.0, 8.0)
    pool_bias = jnp.clip(jax.random.uniform(key_list[8], (D,), jnp.float32, 0.5, 5.0), 0.5, 5.0)
    value_weight = normal_values(key_list[9], (D,), 1.0, 6.0, (), jnp.float32)
    valid_frames = draw_valid_frames(jax.random.fold_in(key_list[11], 71), 0)
    return dict(tokens=tokens, attn_gain=attn_gain, w_qkv=w_qkv, w_out=w_out, mlp_gain=mlp_gain, w_up=w_up, w_down=w_down, pool_gain=pool_gain, pool_bias=pool_bias, value_weight=value_weight, valid_frames=valid_frames)


def rms_norm(values, gain):
    floats = values.astype(jnp.float32)
    square = lax.optimization_barrier(jnp.mean(floats * floats, axis=-1, keepdims=True))
    return (floats * lax.rsqrt(square + 1e-05) * gain).astype(jnp.bfloat16)

def reference(tokens, attn_gain, w_qkv, w_out, mlp_gain, w_up, w_down, pool_gain, pool_bias, value_weight, valid_frames):
    scale = 1.0 / HEAD_DIM ** 0.5
    frame_of = jnp.arange(TOKENS, dtype=jnp.int32) // TOK_FRAME

    def layer(args):
        rows, length = args
        normed = rms_norm(rows, attn_gain)
        qkv = jnp.einsum('nd,cde->nce', normed.astype(jnp.float32), w_qkv.astype(jnp.float32)).astype(jnp.bfloat16)
        query = qkv[:, 0].reshape(TOKENS, HEADS, HEAD_DIM).transpose(1, 0, 2)
        keys = qkv[:, 1].reshape(TOKENS, HEADS, HEAD_DIM).transpose(1, 0, 2)
        vals = qkv[:, 2].reshape(TOKENS, HEADS, HEAD_DIM).transpose(1, 0, 2)
        allowed = (frame_of[None, :] <= frame_of[:, None]) & (frame_of[None, :] < length)

        def head(trio):
            qh, kh, vh = trio
            scores = jnp.dot(qh, kh.T, preferred_element_type=jnp.float32) * scale
            scores = jnp.where(allowed, scores, -1e+30)
            peak = lax.optimization_barrier(jnp.max(scores, axis=-1, keepdims=True))
            weights = jnp.where(allowed, jnp.exp(scores - peak), 0.0)
            total = lax.optimization_barrier(jnp.sum(weights, axis=-1, keepdims=True))
            numer = jnp.dot(weights.astype(jnp.bfloat16), vh, preferred_element_type=jnp.float32)
            return numer / total
        mixed = lax.map(head, (query, keys, vals)).transpose(1, 0, 2).reshape(TOKENS, D).astype(jnp.bfloat16)
        after_attn = (rows.astype(jnp.float32) + jnp.dot(mixed, w_out, preferred_element_type=jnp.float32)).astype(jnp.bfloat16)
        normed2 = rms_norm(after_attn, mlp_gain)
        up = jax.nn.gelu(jnp.dot(normed2, w_up, preferred_element_type=jnp.float32), approximate=True).astype(jnp.bfloat16)
        return (after_attn.astype(jnp.float32) + jnp.dot(up, w_down, preferred_element_type=jnp.float32)).astype(jnp.bfloat16)
    hidden = lax.map(layer, (tokens, valid_frames))
    means = lax.optimization_barrier(jnp.mean(hidden.astype(jnp.float32).reshape(ROLLOUTS, FRAMES, TOK_FRAME, D), axis=2))
    frame_ids = jnp.arange(FRAMES, dtype=jnp.int32)
    valid = frame_ids[None, :] < valid_frames[:, None]

    def advance(state, inputs):
        mean_f, valid_f = inputs
        gate = jax.nn.sigmoid(mean_f * pool_gain + pool_bias)
        new = gate * state + (1.0 - gate) * mean_f
        state = jnp.where(valid_f[:, None], new, state)
        return (state, state)
    start = jnp.zeros((ROLLOUTS, D), jnp.float32)
    _, states = lax.scan(advance, start, (means.transpose(1, 0, 2), valid.T))
    states = states.transpose(1, 0, 2)
    frame_values = jnp.where(valid, lax.optimization_barrier(jnp.sum(states * value_weight, axis=-1)), 0.0)
    last = frame_ids[None, :] == valid_frames[:, None] - 1
    reward = lax.optimization_barrier(jnp.sum(jnp.where(last, frame_values, 0.0), axis=1))
    gap = jnp.where(valid, reward[:, None] - frame_values, 0.0)
    count = jnp.sum(valid_frames).astype(jnp.float32)
    mean = jnp.sum(gap) / count
    centered = jnp.where(valid, gap - mean, 0.0)
    variance = jnp.sum(centered * centered) / count
    advantages = jnp.where(valid, centered * lax.rsqrt(variance + 1e-05), 0.0)
    return (hidden, frame_values, advantages)
```

```python
import functools
import math

import jax
import jax.numpy as jnp
from jax import lax
from jax.experimental import pallas as pl
from jax.experimental.pallas import tpu as pltpu
from jax.sharding import PartitionSpec as P

HEAD_DIM = 128
TOK_FRAME = 256
ROWS = 128
BLOCK = 512
D = 2048
BF16 = jnp.bfloat16
F32 = jnp.float32
MESH = pl.DeviceIdType.MESH
QSCALE = math.log2(math.e) / math.sqrt(HEAD_DIM)
NEG = -1e30


def remote(src, dst, send_sem, recv_sem, where):
    return pltpu.make_async_remote_copy(
        src_ref=src, dst_ref=dst, send_sem=send_sem, recv_sem=recv_sem,
        device_id=where, device_id_type=MESH,
    )


def al(i, m):
    return pl.multiple_of(i, m)


class Place:
    def __init__(self):
        self.c = lax.axis_index("dp")
        s = lax.axis_index("seq")
        self.s = s
        self.z = lax.axis_index("tensor")
        y, x = s // 4, s % 4
        self.p = y * (1 - self.c) + x * self.c
        self.g = x * (1 - self.c) + y * self.c

    def seq(self, p, g):
        return (p * 4 + g) * (1 - self.c) + (g * 4 + p) * self.c

    def flip(self, p):
        return (1 - self.c) * (1 - p % 2) + self.c * (p // 2)

    def gq(self, p, g):
        return g + self.flip(p) * (3 - 2 * g)


def norm_rows(src, gain_ref, dst, rows):
    def body(i, carry):
        at = pl.ds(al(i * 16, 16), 16)
        x = src[at, :].astype(F32)
        square = jnp.mean(x * x, axis=-1, keepdims=True)
        dst[at, :] = (x * lax.rsqrt(square + 1e-5) * gain_ref[...]).astype(BF16)
        return carry

    lax.fori_loop(0, rows // 16, body, 0)


def attn_kernel(
    vf_ref, tok_hbm, gain_ref, w_hbm, mixed_ref,
    tok, w, normed, stage, qx, kx, vx, m_s, acc, o_stage,
    tl_sem, w_sem, ts_sem, tr_sem, a_send, q_recv, k_recv, v_recv, qs_recv,
    g_send, gk_recv, gv_recv, r_recv, o_send, o_recv,
):
    me = Place()
    c, z, p, g = me.c, me.z, me.p, me.g
    zp, zm, z2 = (z + 1) % 4, (z + 3) % 4, (z + 2) % 4
    gp, gm, g2 = (g + 1) % 4, (g + 3) % 4, (g + 2) % 4
    flip = me.flip(p)

    own_in = pltpu.make_async_copy(tok_hbm, tok.at[z], tl_sem)
    own_in.start()
    w_in = [pltpu.make_async_copy(w_hbm.at[k], w.at[k], w_sem.at[k]) for k in range(3)]
    for copy in w_in:
        copy.start()

    barrier = pltpu.get_barrier_semaphore()
    for t in (zp, zm):
        pl.semaphore_signal(barrier, inc=1, device_id={"tensor": t}, device_id_type=MESH)
    for d in (1, 2, 3):
        pl.semaphore_signal(barrier, inc=1, device_id={"seq": me.seq((p + d) % 4, g)}, device_id_type=MESH)
    for d in range(4):
        pl.semaphore_signal(barrier, inc=1, device_id={"seq": me.seq((p + d) % 4, 3 - g)}, device_id_type=MESH)
    for k in (gp, gm):
        pl.semaphore_signal(barrier, inc=1, device_id={"seq": me.seq(p, k)}, device_id_type=MESH)
    own_in.wait()
    pl.semaphore_wait(barrier, 11)

    lo, hi = pl.ds(0, 64), pl.ds(64, 64)
    halves = (lo, hi)
    sends = []

    def tok_send(direction, k, t, half):
        to = zp if direction == 0 else zm
        copy = remote(
            tok.at[t, halves[half], :], tok.at[t, halves[half], :],
            ts_sem.at[direction, k], tr_sem.at[direction, k], {"tensor": to},
        )
        copy.start()
        sends.append(copy)

    def tok_wait(direction, k, t, half):
        remote(
            tok.at[t, halves[half], :], tok.at[t, halves[half], :],
            ts_sem.at[direction, k], tr_sem.at[direction, k], {"tensor": zp},
        ).wait_recv()

    tok_send(0, 0, z, 0)
    tok_send(1, 0, z, 1)
    tok_send(0, 1, z, 1)
    tok_send(1, 1, z, 0)

    def project(t):
        norm_rows(tok.at[t], gain_ref, normed, ROWS)
        for k in range(3):
            for pair in range(2):
                out = jnp.dot(
                    normed[...], w[k, :, pair * 256 : pair * 256 + 256], preferred_element_type=F32
                )
                if k == 0:
                    out = out * QSCALE
                out = out.astype(BF16)
                stage[t, 2 * pair, k] = out[:, :128]
                stage[t, 2 * pair + 1, k] = out[:, 128:]

    def hand_out(t):
        rows = pl.ds(al(t * ROWS, ROWS), ROWS)
        for d in (1, 2, 3):
            h = (p + d) % 4
            to_q = {"seq": me.seq(h, me.gq(p, g))}
            to_kv = {"seq": me.seq(h, g)}
            for k, (dst, sem, to) in enumerate(
                (
                    (qx.at[p, rows, pl.ds(0, 128)], q_recv.at[t], to_q),
                    (kx.at[g * 4 + p, rows, pl.ds(0, 128)], k_recv.at[t], to_kv),
                    (vx.at[g * 4 + p, rows, pl.ds(0, 128)], v_recv.at[t], to_kv),
                )
            ):
                copy = remote(stage.at[t, h, k], dst, a_send.at[t, d - 1, k], sem, to)
                copy.start()
                sends.append(copy)
        kx[g * 4 + p, rows, 0:128] = stage[t, p, 1]
        vx[g * 4 + p, rows, 0:128] = stage[t, p, 2]

        @pl.when(flip == 1)
        def _():
            remote(
                stage.at[t, p, 0], qx.at[p, rows, pl.ds(0, 128)], a_send.at[t, 3, 0], qs_recv.at[t],
                {"seq": me.seq(p, 3 - g)},
            ).start()

        @pl.when(flip == 0)
        def _():
            qx[p, rows, 0:128] = stage[t, p, 0]

    three = pl.ds(0, 3)

    def three_in(sem, buf, t):
        rows = pl.ds(al(t * ROWS, ROWS), ROWS)
        ref = buf.at[three, rows, pl.ds(0, 128)]
        remote(ref, ref, sem, sem, {"tensor": zp}).wait_recv()

    def group_ref(buf, gg, t):
        return buf.at[pl.ds(gg * 4, 4), pl.ds(al(t * ROWS, ROWS), ROWS), pl.ds(0, 128)]

    def ring_out(t):
        three_in(k_recv.at[t], kx, t)
        three_in(v_recv.at[t], vx, t)
        for direction in (0, 1):
            to = {"seq": me.seq(p, gp if direction == 0 else gm)}
            pair = ((kx, gk_recv, 0), (vx, gv_recv, 1))
            for buf, sem, k in pair if direction == 0 else pair[::-1]:
                ref = group_ref(buf, g, t)
                copy = remote(ref, ref, g_send.at[direction, t, k], sem.at[direction, t], to)
                copy.start()
                sends.append(copy)

    def ring_wait(buf, sem, gg, t):
        ref = group_ref(buf, gg, t)
        remote(ref, ref, sem, sem, {"tensor": zp}).wait_recv()

    def relay(t):
        ring_wait(kx, gk_recv.at[0, t], gm, t)
        ref = group_ref(kx, gm, t)
        copy = remote(ref, ref, g_send.at[0, t, 2], r_recv.at[0, t], {"seq": me.seq(p, gp)})
        copy.start()
        sends.append(copy)
        ring_wait(vx, gv_recv.at[1, t], gp, t)
        ref = group_ref(vx, gp, t)
        copy = remote(ref, ref, g_send.at[1, t, 2], r_recv.at[1, t], {"seq": me.seq(p, gm)})
        copy.start()
        sends.append(copy)

    for copy in w_in:
        copy.wait()
    project(z)
    hand_out(z)

    length = vf_ref[c]
    lane = lax.broadcasted_iota(jnp.int32, (BLOCK, 128), 1)
    row = lax.broadcasted_iota(jnp.int32, (BLOCK, 128), 0)

    def fill(slot, carry):
        block = me.seq(slot % 4, slot // 4)
        frame = 2 * block + row // TOK_FRAME
        bias = jnp.where((lane == 0) & (frame >= length), NEG, 0.0)
        mine = 0
        for i in range(4):
            mine = mine + (lane == 1 + i).astype(jnp.int32) * (
                me.seq(i, me.gq(i, g)) == block
            ).astype(jnp.int32)
        bias = jnp.where((mine > 0) & (row >= TOK_FRAME), NEG, bias)
        kx[slot, :, 128:256] = bias.astype(BF16)
        vx[slot, :, 128:256] = jnp.ones((BLOCK, 128), BF16)
        return carry

    lax.fori_loop(0, 16, fill, 0)
    for i in range(4):
        on = (lane == 0) | ((lane == 1 + i) & (row < TOK_FRAME))
        qx[i, :, 128:256] = jnp.where(on, 1.0, 0.0).astype(BF16)
        m_s[i] = jnp.full((BLOCK, 128), -1e38, F32)
        acc[i] = jnp.zeros((BLOCK, 256), F32)

    tok_wait(0, 0, zm, 0)
    tok_send(0, 2, zm, 0)
    tok_wait(1, 0, zp, 1)
    tok_send(1, 2, zp, 1)
    ring_out(z)
    tok_wait(0, 1, zm, 1)
    project(zm)
    hand_out(zm)
    tok_wait(1, 1, zp, 0)
    project(zp)
    hand_out(zp)
    relay(z)
    ring_out(zm)
    ring_out(zp)
    tok_wait(0, 2, z2, 0)
    tok_wait(1, 2, z2, 1)
    project(z2)
    hand_out(z2)
    relay(zm)
    relay(zp)
    ring_out(z2)
    for k in range(4):
        t = (z + k) % 4
        three_in(q_recv.at[t], qx, t)

        @pl.when(flip == 1)
        def _():
            ref = qx.at[p, pl.ds(al(t * ROWS, ROWS), ROWS), pl.ds(0, 128)]
            remote(ref, ref, qs_recv.at[t], qs_recv.at[t], {"tensor": zp}).wait_recv()

    def group(gg):
        def per_q(i, carry):
            n = me.seq(i, me.gq(i, g))
            first = me.seq(0, gg)
            step = 4 * (1 - c) + c
            count = jnp.clip((n - first + step) // step, 0, 4)

            def pair(j, carry):
                slot = gg * 4 + j
                for a in range(2):
                    at = pl.ds(a * 256, 256)
                    s = lax.dot_general(
                        qx[i, at, :], kx[slot], (((1,), (1,)), ((), ())), preferred_element_type=F32
                    )
                    before = m_s[i, at, :]
                    after = jnp.maximum(before, jnp.max(s, axis=1, keepdims=True))
                    weights = jnp.exp2(s - after[:, :1]).astype(BF16)
                    keep = jnp.exp2(before - after)
                    m_s[i, at, :] = after
                    acc[i, at, :] = acc[i, at, :] * jnp.concatenate([keep, keep], axis=1) + jnp.dot(
                        weights, vx[slot], preferred_element_type=F32
                    )
                return carry

            lax.fori_loop(0, count, pair, 0)
            return carry

        lax.fori_loop(0, 4, per_q, 0)

    group(g)
    relay(z2)
    for k in range(4):
        ring_wait(vx, gv_recv.at[0, (z + k) % 4], gm, (z + k) % 4)
    group(gm)
    for k in range(4):
        ring_wait(kx, gk_recv.at[1, (z + k) % 4], gp, (z + k) % 4)
    group(gp)
    for k in range(4):
        ring_wait(kx, r_recv.at[0, (z + k) % 4], g2, (z + k) % 4)
        ring_wait(vx, r_recv.at[1, (z + k) % 4], g2, (z + k) % 4)
    group(g2)

    def finish(i):
        o_stage[i] = (acc[i, :, 0:128] / acc[i, :, 128:256]).astype(BF16)

    for d in (1, 2, 3):
        i = (p + d) % 4
        finish(i)
        copy = remote(
            o_stage.at[i], mixed_ref.at[p], o_send.at[d - 1], o_recv.at[p],
            {"seq": me.seq(i, me.gq(i, g))},
        )
        copy.start()
        sends.append(copy)
    finish(p)

    @pl.when(flip == 1)
    def _():
        remote(
            o_stage.at[p], mixed_ref.at[p], o_send.at[3], o_recv.at[p], {"seq": me.seq(p, 3 - g)}
        ).start()

    @pl.when(flip == 0)
    def _():
        mixed_ref[p] = o_stage[p]

    for d in (1, 2, 3):
        h = (p + d) % 4
        remote(o_stage.at[0], mixed_ref.at[h], o_send.at[0], o_recv.at[h], {"tensor": zp}).wait_recv()

    @pl.when(flip == 1)
    def _():
        back = remote(
            o_stage.at[p], mixed_ref.at[p], o_send.at[3], o_recv.at[p], {"seq": me.seq(p, 3 - g)}
        )
        back.wait_recv()
        back.wait_send()
        for t in range(4):
            rows = pl.ds(t * ROWS, ROWS)
            remote(
                stage.at[t, p, 0], qx.at[p, rows, pl.ds(0, 128)], a_send.at[t, 3, 0], qs_recv.at[t],
                {"seq": me.seq(p, 3 - g)},
            ).wait_send()

    for copy in sends:
        copy.wait_send()


def attention(tokens, gain, w_qkv, lengths):
    vmem = pltpu.VMEM
    dma = pltpu.SemaphoreType.DMA
    return pl.pallas_call(
        attn_kernel,
        out_shape=jax.ShapeDtypeStruct((4, BLOCK, HEAD_DIM), BF16),
        in_specs=[
            pl.BlockSpec(memory_space=pltpu.SMEM),
            pl.BlockSpec(memory_space=pl.ANY),
            pl.BlockSpec(memory_space=pltpu.VMEM),
            pl.BlockSpec(memory_space=pl.ANY),
        ],
        out_specs=pl.BlockSpec(memory_space=pltpu.VMEM),
        scratch_shapes=[
            vmem((4, ROWS, D), BF16),
            vmem((3, D, BLOCK), BF16),
            vmem((ROWS, D), BF16),
            vmem((4, 4, 3, ROWS, HEAD_DIM), BF16),
            vmem((4, BLOCK, 256), BF16),
            vmem((16, BLOCK, 256), BF16),
            vmem((16, BLOCK, 256), BF16),
            vmem((4, BLOCK, 128), F32),
            vmem((4, BLOCK, 256), F32),
            vmem((4, BLOCK, HEAD_DIM), BF16),
            dma,
            dma((3,)),
            dma((2, 3)),
            dma((2, 3)),
            dma((4, 4, 3)),
            dma((4,)),
            dma((4,)),
            dma((4,)),
            dma((4,)),
            dma((2, 4, 3)),
            dma((2, 4)),
            dma((2, 4)),
            dma((2, 4)),
            dma((4,)),
            dma((4,)),
        ],
        compiler_params=pltpu.CompilerParams(
            collective_id=0, has_side_effects=True, vmem_limit_bytes=52 * 2**20
        ),
        cost_estimate=pl.CostEstimate(flops=2 * 10**10, bytes_accessed=2 * 10**7, transcendentals=10**7),
    )(lengths, tokens, gain.reshape(1, D), w_qkv)


FR_DEV = 2


def laid_out(blocks, dim):
    shape = list(blocks.shape[1:])
    shape[dim] *= blocks.shape[0]
    return jnp.moveaxis(blocks, 0, dim).reshape(shape)


def sent_to_all(array, axis):
    copies = jnp.broadcast_to(array, (lax.axis_size(axis), *array.shape))
    return lax.all_to_all(copies, axis, split_axis=0, concat_axis=0, tiled=True)


def gathered_copies(array, axis, dim):
    return laid_out(sent_to_all(array, axis), dim)


def cut_along(array, dim, size):
    shape = array.shape
    blocks = array.reshape(*shape[:dim], size, shape[dim] // size, *shape[dim + 1 :])
    return jnp.moveaxis(blocks, dim, 0)


def summed_on_arrival(array, axis, dim):
    size = lax.axis_size(axis)
    blocks = lax.all_to_all(cut_along(array, dim, size), axis, 0, 0, tiled=True)
    return jnp.sum(blocks.astype(jnp.float32), axis=0)


def over_copies(array, axis):
    everything = sent_to_all(array, axis)
    return jnp.sum(everything, axis=0)


def collected_together(array, axis):
    leaves = jax.tree.leaves(array)
    sequence = sorted(range(len(leaves)), key=lambda k: -leaves[k].size)
    width = (1, *leaves[sequence[0]].shape)[-1]
    lines = [
        jnp.pad(leaves[k].reshape(-1), (0, -leaves[k].size % width)).reshape(-1, width)
        for k in sequence
    ]
    both, at, found = (sent_to_all(jnp.concatenate(lines), axis), 0, {})
    for k, line in zip(sequence, lines):
        piece = both[:, at : at + len(line)].reshape(len(both), -1)
        found[k] = piece[:, : leaves[k].size].reshape(-1, *leaves[k].shape)
        at += len(line)
    numbers = iter(range(len(leaves)))
    return jax.tree.map(lambda _: found[next(numbers)], array)


def combined_pairwise(pieces, combine):
    while len(jax.tree.leaves(pieces)[0]) > 1:
        pieces = jax.vmap(combine)(
            *(jax.tree.map(lambda part: part[side::2], pieces) for side in (0, 1))
        )
    return jax.tree.map(lambda part: part[0], pieces)


def entering_2(array, axis, combine, identity):
    size, index = (lax.axis_size(axis), lax.axis_index(axis))
    passed = jnp.arange(size) < index

    def kept(part, zero, own):
        part = jnp.where(
            passed.reshape(-1, *(1 for _ in own.shape)), part, jnp.asarray(zero, own.dtype)
        )
        return part

    pieces = collected_together(array, axis)
    return combined_pairwise(jax.tree.map(kept, pieces, identity, array), combine)


def rms_norm(values, gain):
    floats = values.astype(jnp.float32)
    square = jnp.mean(floats * floats, axis=-1, keepdims=True)
    return (floats * lax.rsqrt(square + 1e-05) * gain).astype(jnp.bfloat16)


def compose(earlier, later):
    return (earlier[0] * later[0], later[0] * earlier[1] + later[1])


def local(
    tokens,
    attn_gain,
    w_qkv,
    w_out,
    mlp_gain,
    w_up,
    w_down,
    pool_gain,
    pool_bias,
    value_weight,
    valid_frames,
):
    rows = tokens[0]
    row_count = rows.shape[0]
    seq_index = lax.axis_index("seq")
    tensor_index = lax.axis_index("tensor")
    roll_index = lax.axis_index("dp")
    length = valid_frames[roll_index]
    heads = attention(rows, attn_gain, w_qkv, valid_frames)
    mixed = heads.transpose(1, 0, 2).reshape(BLOCK, 4 * HEAD_DIM)
    attn_sum = summed_on_arrival(
        jnp.dot(mixed, w_out, preferred_element_type=jnp.float32).astype(jnp.bfloat16), "tensor", 0
    )
    after_attn = (rows.astype(jnp.float32) + attn_sum).astype(jnp.bfloat16)
    normed2 = rms_norm(after_attn, mlp_gain)
    up = jax.nn.gelu(
        jnp.dot(gathered_copies(normed2, "tensor", 0), w_up, preferred_element_type=jnp.float32),
        approximate=True,
    ).astype(jnp.bfloat16)
    down_sum = summed_on_arrival(
        jnp.dot(up, w_down, preferred_element_type=jnp.float32).astype(jnp.bfloat16), "tensor", 0
    )
    hidden = (after_attn.astype(jnp.float32) + down_sum).astype(jnp.bfloat16)
    local_frame = (tensor_index * row_count + jnp.arange(row_count, dtype=jnp.int32)) // TOK_FRAME
    selector = (local_frame[None, :] == jnp.arange(FR_DEV, dtype=jnp.int32)[:, None]).astype(
        jnp.bfloat16
    )
    sums = jnp.dot(selector, hidden, preferred_element_type=jnp.float32)
    sums = over_copies(sums, "tensor")
    gain, offset, head_weight = (pool_gain, pool_bias, value_weight)
    means = sums / TOK_FRAME
    frame_global = seq_index * FR_DEV + jnp.arange(FR_DEV, dtype=jnp.int32)
    valid = frame_global < length
    gate = jax.nn.sigmoid(means * gain + offset)
    decay = jnp.where(valid[:, None], gate, 1.0)
    source = jnp.where(valid[:, None], (1.0 - gate) * means, 0.0)
    agg_decay = jnp.ones_like(means[0])
    agg_source = jnp.zeros_like(means[0])
    for frame in range(FR_DEV):
        agg_decay, agg_source = compose((agg_decay, agg_source), (decay[frame], source[frame]))
    entering = entering_2(
        (agg_decay, agg_source),
        "seq",
        compose,
        (jnp.ones_like(agg_decay), jnp.zeros_like(agg_source)),
    )
    state = entering[1]
    collected = []
    for frame in range(FR_DEV):
        state = decay[frame] * state + source[frame]
        collected.append(jnp.sum(state * head_weight))
    partial_values = jnp.stack(collected)
    values = jnp.where(valid, partial_values, 0.0)
    pick = jnp.sum(jnp.where(frame_global == length - 1, values, 0.0))
    count = jnp.sum(valid_frames).astype(jnp.float32)
    slot = (jnp.arange(lax.axis_size("dp"), dtype=jnp.int32) == roll_index).astype(jnp.float32)
    entries = jnp.stack([pick, jnp.sum(values), jnp.sum(values * values)])
    table = over_copies(entries[:, None] * slot[None, :], ("dp", "seq"))
    finals, first_sums, second_sums = (table[0], table[1], table[2])
    lengths = valid_frames.astype(jnp.float32)
    mean = jnp.sum(lengths * finals - first_sums) / count
    squares = jnp.sum(lengths * finals * finals - 2.0 * finals * first_sums + second_sums) / count
    variance = squares - mean * mean
    final = jnp.sum(finals * slot)
    gap = jnp.where(valid, final - values, 0.0)
    centered = jnp.where(valid, gap - mean, 0.0)
    advantages = jnp.where(valid, centered * lax.rsqrt(variance + 1e-05), 0.0)
    return (hidden[None], values[None], advantages[None])


def solution(mesh):
    in_specs = (
        P("dp", ("seq", "tensor"), None),
        P(),
        P(None, None, "tensor"),
        P("tensor", None),
        P(),
        P(None, "tensor"),
        P("tensor", None),
        P(),
        P(),
        P(),
        P(),
    )
    out_specs = (P("dp", ("seq", "tensor"), None), P("dp", "seq"), P("dp", "seq"))
    return jax.shard_map(local, mesh=mesh, in_specs=in_specs, out_specs=out_specs, check_vma=False)
```

```python
import functools
import math

import jax
import jax.numpy as jnp
from jax import lax
from jax.experimental import pallas as pl
from jax.experimental.pallas import tpu as pltpu
from jax.sharding import PartitionSpec as P

HEAD_DIM = 128
TOK_FRAME = 256
ROWS = 128
BLOCK = 512
D = 2048
BF16 = jnp.bfloat16
F32 = jnp.float32
MESH = pl.DeviceIdType.MESH
QSCALE = math.log2(math.e) / math.sqrt(HEAD_DIM)
NEG = -1e30


def remote(src, dst, send_sem, recv_sem, where):
    return pltpu.make_async_remote_copy(
        src_ref=src, dst_ref=dst, send_sem=send_sem, recv_sem=recv_sem,
        device_id=where, device_id_type=MESH,
    )


def al(i, m):
    return pl.multiple_of(i, m)


class Place:
    def __init__(self):
        self.c = lax.axis_index("dp")
        s = lax.axis_index("seq")
        self.s = s
        self.z = lax.axis_index("tensor")
        y, x = s // 4, s % 4
        self.p = y * (1 - self.c) + x * self.c
        self.g = x * (1 - self.c) + y * self.c

    def seq(self, p, g):
        return (p * 4 + g) * (1 - self.c) + (g * 4 + p) * self.c

    def flip(self, p):
        return (1 - self.c) * (1 - p % 2) + self.c * (p // 2)

    def gq(self, p, g):
        return g + self.flip(p) * (3 - 2 * g)


def norm_rows(src, gain_ref, dst, rows):
    def body(i, carry):
        at = pl.ds(al(i * 16, 16), 16)
        x = src[at, :].astype(F32)
        square = jnp.mean(x * x, axis=-1, keepdims=True)
        dst[at, :] = (x * lax.rsqrt(square + 1e-5) * gain_ref[...]).astype(BF16)
        return carry

    lax.fori_loop(0, rows // 16, body, 0)


def attn_kernel(
    vf_ref, tok_hbm, gain_ref, w_hbm, mixed_ref,
    tok, w, normed, stage, qx, kx, vx, m_s, acc, o_stage,
    tl_sem, w_sem, ts_sem, tr_sem, a_send, q_recv, k_recv, v_recv, qs_recv,
    g_send, gk_recv, gv_recv, r_recv, o_send, o_recv,
):
    me = Place()
    c, z, p, g = me.c, me.z, me.p, me.g
    zp, zm, z2 = (z + 1) % 4, (z + 3) % 4, (z + 2) % 4
    gp, gm, g2 = (g + 1) % 4, (g + 3) % 4, (g + 2) % 4
    flip = me.flip(p)

    own_in = pltpu.make_async_copy(tok_hbm, tok.at[z], tl_sem)
    own_in.start()
    w_in = [pltpu.make_async_copy(w_hbm.at[k], w.at[k], w_sem.at[k]) for k in range(3)]
    for copy in w_in:
        copy.start()

    barrier = pltpu.get_barrier_semaphore()
    for t in (zp, zm):
        pl.semaphore_signal(barrier, inc=1, device_id={"tensor": t}, device_id_type=MESH)
    for d in (1, 2, 3):
        pl.semaphore_signal(barrier, inc=1, device_id={"seq": me.seq((p + d) % 4, g)}, device_id_type=MESH)
    for d in range(4):
        pl.semaphore_signal(barrier, inc=1, device_id={"seq": me.seq((p + d) % 4, 3 - g)}, device_id_type=MESH)
    for k in (gp, gm):
        pl.semaphore_signal(barrier, inc=1, device_id={"seq": me.seq(p, k)}, device_id_type=MESH)
    own_in.wait()
    pl.semaphore_wait(barrier, 11)

    lo, hi = pl.ds(0, 64), pl.ds(64, 64)
    halves = (lo, hi)
    sends = []

    def tok_send(direction, k, t, half):
        to = zp if direction == 0 else zm
        copy = remote(
            tok.at[t, halves[half], :], tok.at[t, halves[half], :],
            ts_sem.at[direction, k], tr_sem.at[direction, k], {"tensor": to},
        )
        copy.start()
        sends.append(copy)

    def tok_wait(direction, k, t, half):
        remote(
            tok.at[t, halves[half], :], tok.at[t, halves[half], :],
            ts_sem.at[direction, k], tr_sem.at[direction, k], {"tensor": zp},
        ).wait_recv()

    tok_send(0, 0, z, 0)
    tok_send(1, 0, z, 1)
    tok_send(0, 1, z, 1)
    tok_send(1, 1, z, 0)

    def project(t):
        norm_rows(tok.at[t], gain_ref, normed, ROWS)
        for k in range(3):
            for pair in range(2):
                out = jnp.dot(
                    normed[...], w[k, :, pair * 256 : pair * 256 + 256], preferred_element_type=F32
                )
                if k == 0:
                    out = out * QSCALE
                out = out.astype(BF16)
                stage[t, 2 * pair, k] = out[:, :128]
                stage[t, 2 * pair + 1, k] = out[:, 128:]

    def hand_out(t):
        rows = pl.ds(al(t * ROWS, ROWS), ROWS)
        for d in (1, 2, 3):
            h = (p + d) % 4
            to_q = {"seq": me.seq(h, me.gq(p, g))}
            to_kv = {"seq": me.seq(h, g)}
            for k, (dst, sem, to) in enumerate(
                (
                    (qx.at[p, rows, pl.ds(0, 128)], q_recv.at[t], to_q),
                    (kx.at[g * 4 + p, rows, pl.ds(0, 128)], k_recv.at[t], to_kv),
                    (vx.at[g * 4 + p, rows, pl.ds(0, 128)], v_recv.at[t], to_kv),
                )
            ):
                copy = remote(stage.at[t, h, k], dst, a_send.at[t, d - 1, k], sem, to)
                copy.start()
                sends.append(copy)
        kx[g * 4 + p, rows, 0:128] = stage[t, p, 1]
        vx[g * 4 + p, rows, 0:128] = stage[t, p, 2]

        @pl.when(flip == 1)
        def _():
            remote(
                stage.at[t, p, 0], qx.at[p, rows, pl.ds(0, 128)], a_send.at[t, 3, 0], qs_recv.at[t],
                {"seq": me.seq(p, 3 - g)},
            ).start()

        @pl.when(flip == 0)
        def _():
            qx[p, rows, 0:128] = stage[t, p, 0]

    three = pl.ds(0, 3)

    def three_in(sem, buf, t):
        rows = pl.ds(al(t * ROWS, ROWS), ROWS)
        ref = buf.at[three, rows, pl.ds(0, 128)]
        remote(ref, ref, sem, sem, {"tensor": zp}).wait_recv()

    def group_ref(buf, gg, t):
        return buf.at[pl.ds(gg * 4, 4), pl.ds(al(t * ROWS, ROWS), ROWS), pl.ds(0, 128)]

    def ring_out(t):
        three_in(k_recv.at[t], kx, t)
        three_in(v_recv.at[t], vx, t)
        for direction in (0, 1):
            to = {"seq": me.seq(p, gp if direction == 0 else gm)}
            pair = ((kx, gk_recv, 0), (vx, gv_recv, 1))
            for buf, sem, k in pair if direction == 0 else pair[::-1]:
                ref = group_ref(buf, g, t)
                copy = remote(ref, ref, g_send.at[direction, t, k], sem.at[direction, t], to)
                copy.start()
                sends.append(copy)

    def ring_wait(buf, sem, gg, t):
        ref = group_ref(buf, gg, t)
        remote(ref, ref, sem, sem, {"tensor": zp}).wait_recv()

    def relay(t):
        ring_wait(kx, gk_recv.at[0, t], gm, t)
        ref = group_ref(kx, gm, t)
        copy = remote(ref, ref, g_send.at[0, t, 2], r_recv.at[0, t], {"seq": me.seq(p, gp)})
        copy.start()
        sends.append(copy)
        ring_wait(vx, gv_recv.at[1, t], gp, t)
        ref = group_ref(vx, gp, t)
        copy = remote(ref, ref, g_send.at[1, t, 2], r_recv.at[1, t], {"seq": me.seq(p, gm)})
        copy.start()
        sends.append(copy)

    for copy in w_in:
        copy.wait()
    project(z)
    hand_out(z)

    length = vf_ref[c]
    lane = lax.broadcasted_iota(jnp.int32, (BLOCK, 128), 1)
    row = lax.broadcasted_iota(jnp.int32, (BLOCK, 128), 0)

    def fill(slot, carry):
        block = me.seq(slot % 4, slot // 4)
        frame = 2 * block + row // TOK_FRAME
        bias = jnp.where((lane == 0) & (frame >= length), NEG, 0.0)
        mine = 0
        for i in range(4):
            mine = mine + (lane == 1 + i).astype(jnp.int32) * (
                me.seq(i, me.gq(i, g)) == block
            ).astype(jnp.int32)
        bias = jnp.where((mine > 0) & (row >= TOK_FRAME), NEG, bias)
        kx[slot, :, 128:256] = bias.astype(BF16)
        vx[slot, :, 128:256] = jnp.ones((BLOCK, 128), BF16)
        return carry

    lax.fori_loop(0, 16, fill, 0)
    for i in range(4):
        on = (lane == 0) | ((lane == 1 + i) & (row < TOK_FRAME))
        qx[i, :, 128:256] = jnp.where(on, 1.0, 0.0).astype(BF16)
        m_s[i] = jnp.full((BLOCK, 128), -1e38, F32)
        acc[i] = jnp.zeros((BLOCK, 256), F32)

    tok_wait(0, 0, zm, 0)
    tok_send(0, 2, zm, 0)
    tok_wait(1, 0, zp, 1)
    tok_send(1, 2, zp, 1)
    ring_out(z)
    tok_wait(0, 1, zm, 1)
    project(zm)
    hand_out(zm)
    tok_wait(1, 1, zp, 0)
    project(zp)
    hand_out(zp)
    relay(z)
    ring_out(zm)
    ring_out(zp)
    tok_wait(0, 2, z2, 0)
    tok_wait(1, 2, z2, 1)
    project(z2)
    hand_out(z2)
    relay(zm)
    relay(zp)
    ring_out(z2)
    for k in range(4):
        t = (z + k) % 4
        three_in(q_recv.at[t], qx, t)

        @pl.when(flip == 1)
        def _():
            ref = qx.at[p, pl.ds(al(t * ROWS, ROWS), ROWS), pl.ds(0, 128)]
            remote(ref, ref, qs_recv.at[t], qs_recv.at[t], {"tensor": zp}).wait_recv()

    def group(gg):
        def per_q(i, carry):
            n = me.seq(i, me.gq(i, g))
            first = me.seq(0, gg)
            step = 4 * (1 - c) + c
            count = jnp.clip((n - first + step) // step, 0, 4)

            def pair(j, carry):
                slot = gg * 4 + j
                for a in range(2):
                    at = pl.ds(a * 256, 256)
                    s = lax.dot_general(
                        qx[i, at, :], kx[slot], (((1,), (1,)), ((), ())), preferred_element_type=F32
                    )
                    before = m_s[i, at, :]
                    after = jnp.maximum(before, jnp.max(s, axis=1, keepdims=True))
                    weights = jnp.exp2(s - after[:, :1]).astype(BF16)
                    keep = jnp.exp2(before - after)
                    m_s[i, at, :] = after
                    acc[i, at, :] = acc[i, at, :] * jnp.concatenate([keep, keep], axis=1) + jnp.dot(
                        weights, vx[slot], preferred_element_type=F32
                    )
                return carry

            lax.fori_loop(0, count, pair, 0)
            return carry

        lax.fori_loop(0, 4, per_q, 0)

    group(g)
    relay(z2)
    for k in range(4):
        ring_wait(vx, gv_recv.at[0, (z + k) % 4], gm, (z + k) % 4)
    group(gm)
    for k in range(4):
        ring_wait(kx, gk_recv.at[1, (z + k) % 4], gp, (z + k) % 4)
    group(gp)
    for k in range(4):
        ring_wait(kx, r_recv.at[0, (z + k) % 4], g2, (z + k) % 4)
        ring_wait(vx, r_recv.at[1, (z + k) % 4], g2, (z + k) % 4)
    group(g2)

    def finish(i):
        o_stage[i] = (acc[i, :, 0:128] / acc[i, :, 128:256]).astype(BF16)

    for d in (1, 2, 3):
        i = (p + d) % 4
        finish(i)
        copy = remote(
            o_stage.at[i], mixed_ref.at[p], o_send.at[d - 1], o_recv.at[p],
            {"seq": me.seq(i, me.gq(i, g))},
        )
        copy.start()
        sends.append(copy)
    finish(p)

    @pl.when(flip == 1)
    def _():
        remote(
            o_stage.at[p], mixed_ref.at[p], o_send.at[3], o_recv.at[p], {"seq": me.seq(p, 3 - g)}
        ).start()

    @pl.when(flip == 0)
    def _():
        mixed_ref[p] = o_stage[p]

    for d in (1, 2, 3):
        h = (p + d) % 4
        remote(o_stage.at[0], mixed_ref.at[h], o_send.at[0], o_recv.at[h], {"tensor": zp}).wait_recv()

    @pl.when(flip == 1)
    def _():
        back = remote(
            o_stage.at[p], mixed_ref.at[p], o_send.at[3], o_recv.at[p], {"seq": me.seq(p, 3 - g)}
        )
        back.wait_recv()
        back.wait_send()
        for t in range(4):
            rows = pl.ds(t * ROWS, ROWS)
            remote(
                stage.at[t, p, 0], qx.at[p, rows, pl.ds(0, 128)], a_send.at[t, 3, 0], qs_recv.at[t],
                {"seq": me.seq(p, 3 - g)},
            ).wait_send()

    for copy in sends:
        copy.wait_send()


def attention(tokens, gain, w_qkv, lengths):
    vmem = pltpu.VMEM
    dma = pltpu.SemaphoreType.DMA
    return pl.pallas_call(
        attn_kernel,
        out_shape=jax.ShapeDtypeStruct((4, BLOCK, HEAD_DIM), BF16),
        in_specs=[
            pl.BlockSpec(memory_space=pltpu.SMEM),
            pl.BlockSpec(memory_space=pl.ANY),
            pl.BlockSpec(memory_space=pltpu.VMEM),
            pl.BlockSpec(memory_space=pl.ANY),
        ],
        out_specs=pl.BlockSpec(memory_space=pltpu.VMEM),
        scratch_shapes=[
            vmem((4, ROWS, D), BF16),
            vmem((3, D, BLOCK), BF16),
            vmem((ROWS, D), BF16),
            vmem((4, 4, 3, ROWS, HEAD_DIM), BF16),
            vmem((4, BLOCK, 256), BF16),
            vmem((16, BLOCK, 256), BF16),
            vmem((16, BLOCK, 256), BF16),
            vmem((4, BLOCK, 128), F32),
            vmem((4, BLOCK, 256), F32),
            vmem((4, BLOCK, HEAD_DIM), BF16),
            dma,
            dma((3,)),
            dma((2, 3)),
            dma((2, 3)),
            dma((4, 4, 3)),
            dma((4,)),
            dma((4,)),
            dma((4,)),
            dma((4,)),
            dma((2, 4, 3)),
            dma((2, 4)),
            dma((2, 4)),
            dma((2, 4)),
            dma((4,)),
            dma((4,)),
        ],
        compiler_params=pltpu.CompilerParams(
            collective_id=0, has_side_effects=True, vmem_limit_bytes=52 * 2**20
        ),
        cost_estimate=pl.CostEstimate(flops=2 * 10**10, bytes_accessed=2 * 10**7, transcendentals=10**7),
    )(lengths, tokens, gain.reshape(1, D), w_qkv)


def gelu(x):
    return 0.5 * x * (1.0 + jnp.tanh(math.sqrt(2.0 / math.pi) * (x + 0.044715 * (x * x * x))))


def mlp_kernel(
    vf_ref, mixed_ref, tok_ref, gain_ref, pg_ref, pb_ref, vw_ref, wo_hbm, wu_hbm, wd_hbm,
    hid_ref, fv_ref, adv_ref,
    wo, wu, wd, part, mid, fin, nrm, after, own, up, fs, zs, means, states, vals,
    w_sem, rs_send, mid_recv, fin_recv, ag_send, ag_recv, z_send, z_recv, s_send, s_recv, v_sem,
):
    c, s, z = lax.axis_index("dp"), lax.axis_index("seq"), lax.axis_index("tensor")
    zp, zm, z2 = (z + 1) % 4, (z + 3) % 4, (z + 2) % 4
    w_in = [
        pltpu.make_async_copy(src, dst, w_sem.at[k])
        for k, (src, dst) in enumerate(((wo_hbm, wo), (wu_hbm, wu), (wd_hbm, wd)))
    ]
    for copy in w_in:
        copy.start()
    barrier = pltpu.get_barrier_semaphore()
    for t in (zp, zm, z2):
        pl.semaphore_signal(barrier, inc=1, device_id={"tensor": t}, device_id_type=MESH)
    for d in range(1, 16):
        pl.semaphore_signal(barrier, inc=1, device_id={"seq": (s + d) % 16}, device_id_type=MESH)
    pl.semaphore_signal(barrier, inc=1, device_id={"dp": 1 - c}, device_id_type=MESH)

    lo, hi = pl.ds(0, 64), pl.ds(64, 64)
    sends = []

    def send(src, dst, send_sem, recv_sem, to):
        copy = remote(src, dst, send_sem, recv_sem, to)
        copy.start()
        sends.append(copy)

    def arrive(ref, sem):
        remote(ref, ref, sem, sem, {"tensor": zp}).wait_recv()

    def out_project(t):
        rows = pl.ds(al(t * ROWS, ROWS), ROWS)
        lhs = jnp.concatenate([mixed_ref[h, rows, :] for h in range(4)], axis=1)
        for n in range(4):
            cols = slice(n * 512, n * 512 + 512)
            part[0, t, :, cols] = jnp.dot(lhs, wo[:, cols], preferred_element_type=F32).astype(BF16)

    def send_mids(k):
        send(part.at[k, z2, lo, :], mid.at[k, 0], rs_send.at[k, 0], mid_recv.at[k, 0], {"tensor": zp})
        send(part.at[k, z2, hi, :], mid.at[k, 1], rs_send.at[k, 1], mid_recv.at[k, 1], {"tensor": zm})

    def send_direct(k):
        send(part.at[k, zp, hi, :], fin.at[k, 0, hi, :], rs_send.at[k, 2], fin_recv.at[k, 0, 1], {"tensor": zp})
        send(part.at[k, zm, lo, :], fin.at[k, 1, lo, :], rs_send.at[k, 3], fin_recv.at[k, 1, 0], {"tensor": zm})

    def send_sums(k):
        for direction, (t, half) in enumerate(((zp, 0), (zm, 64))):
            arrive(mid.at[k, direction], mid_recv.at[k, direction])

            def add(i, carry):
                at = pl.ds(al(i * 16, 16), 16)
                to = pl.ds(al(half + i * 16, 16), 16)
                part[k, t, to, :] = (part[k, t, to, :].astype(F32) + mid[k, direction, at, :].astype(F32)).astype(BF16)
                return carry

            lax.fori_loop(0, 4, add, 0)
            rows = pl.ds(half, 64)
            send(
                part.at[k, t, rows, :], fin.at[k, direction, rows, :], rs_send.at[k, 4 + direction],
                fin_recv.at[k, direction, direction], {"tensor": t},
            )

    def wait_final(k):
        for direction in (0, 1):
            for half, rows in enumerate((lo, hi)):
                arrive(fin.at[k, direction, rows, :], fin_recv.at[k, direction, half])

    w_in[0].wait()
    out_project(z2)
    pl.semaphore_wait(barrier, 19)
    send_mids(0)
    out_project(zp)
    out_project(zm)
    send_direct(0)
    out_project(z)
    send_sums(0)
    wait_final(0)

    def settle(i, carry):
        at = pl.ds(al(i * 16, 16), 16)
        total = part[0, z, at, :].astype(F32) + fin[0, 0, at, :].astype(F32) + fin[0, 1, at, :].astype(F32)
        x = (tok_ref[at, :].astype(F32) + total).astype(BF16)
        after[at, :] = x
        x = x.astype(F32)
        square = jnp.mean(x * x, axis=-1, keepdims=True)
        nrm[z, at, :] = (x * lax.rsqrt(square + 1e-5) * gain_ref[...]).astype(BF16)
        return carry

    lax.fori_loop(0, 8, settle, 0)

    halves = (lo, hi)

    def ring_send(direction, k, t, half):
        ref = nrm.at[t, halves[half], :]
        send(ref, ref, ag_send.at[direction, k], ag_recv.at[direction, k], {"tensor": zp if direction == 0 else zm})

    def ring_wait(direction, k, t, half):
        arrive(nrm.at[t, halves[half], :], ag_recv.at[direction, k])

    ring_send(0, 0, z, 0)
    ring_send(1, 0, z, 1)
    ring_send(0, 1, z, 1)
    ring_send(1, 1, z, 0)

    for k in (0, 1):
        fs[k] = jnp.zeros((8, D), F32)

    def up_down(ts, keep):
        rows = ROWS * len(ts)

        def up_step(n, carry):
            cols = pl.ds(al(n * 256, 256), 256)
            lhs = jnp.concatenate([nrm[t] for t in ts], axis=0) if len(ts) > 1 else nrm[ts[0]]
            x = jnp.dot(lhs, wu[:, cols], preferred_element_type=F32)
            up[0:rows, cols] = gelu(x).astype(BF16)
            return carry

        lax.fori_loop(0, 8, up_step, 0)

        def down_step(n, carry):
            cols = pl.ds(al(n * 256, 256), 256)
            x = jnp.dot(up[0:rows, :], wd[:, cols], preferred_element_type=F32)
            for k, t in enumerate(ts):
                y = x[k * ROWS : (k + 1) * ROWS]
                fs[t // 2, :, cols] += jnp.sum(y.reshape(16, 8, 256), axis=0)
                if keep:
                    own[:, cols] = y
                else:
                    part[1, t, :, cols] = y.astype(BF16)
            return carry

        lax.fori_loop(0, 8, down_step, 0)

    w_in[1].wait()
    w_in[2].wait()
    up_down((z,), True)
    ring_wait(0, 0, zm, 0)
    ring_send(0, 2, zm, 0)
    ring_wait(1, 0, zp, 1)
    ring_send(1, 2, zp, 1)

    def residual(i, carry):
        at = pl.ds(al(i * 16, 16), 16)
        fs[z // 2] += jnp.sum(after[at, :].astype(F32).reshape(2, 8, D), axis=0)
        return carry

    lax.fori_loop(0, 8, residual, 0)
    ring_wait(0, 1, zm, 1)
    ring_wait(1, 1, zp, 0)
    up_down((zm, zp), False)
    send_direct(1)
    ring_wait(0, 2, z2, 0)
    ring_wait(1, 2, z2, 1)
    up_down((z2,), False)

    for k in (0, 1):
        zs[z, k : k + 1, :] = jnp.sum(fs[k], axis=0, keepdims=True)
    for d in (1, 2, 3):
        send(zs.at[z], zs.at[z], z_send.at[d - 1], z_recv.at[z], {"tensor": (z + d) % 4})
    send_mids(1)
    for d in (1, 2, 3):
        t = (z + d) % 4
        arrive(zs.at[t], z_recv.at[t])
    means[s] = (zs[0] + zs[1] + zs[2] + zs[3]) * (1.0 / TOK_FRAME)
    for d in range(1, 16):
        send(means.at[s], means.at[s], s_send.at[d - 1], s_recv.at[s], {"seq": (s + d) % 16})
    send_sums(1)

    for d in range(1, 16):
        t = (s + d) % 16
        arrive(means.at[t], s_recv.at[t])
    length = vf_ref[c]
    frame = 2 * lax.broadcasted_iota(jnp.int32, (16, 2, 128), 0) + lax.broadcasted_iota(jnp.int32, (16, 2, 128), 1)
    pg, pb, vw = pg_ref[...], pb_ref[...], vw_ref[...]

    def scan(i, state):
        m = means[i]
        gate = jax.nn.sigmoid(m * pg + pb)
        source = (1.0 - gate) * m
        for k in (0, 1):
            new = gate[k : k + 1] * state + source[k : k + 1]
            state = jnp.where(2 * i + k < length, new, state)
            states[i, k : k + 1, :] = state
        return state

    lax.fori_loop(0, 16, scan, jnp.zeros((1, D), F32))
    total = jnp.sum(states[...] * vw.reshape(1, 1, D), axis=-1, keepdims=True)
    values = jnp.where(frame < length, jnp.broadcast_to(total, (16, 2, 128)), 0.0)
    vals[0] = values
    send(vals.at[0], vals.at[1], v_sem.at[0], v_sem.at[1], {"dp": 1 - c})

    wait_final(1)

    def output(i, carry):
        at = pl.ds(al(i * 16, 16), 16)
        total = own[at, :] + fin[1, 0, at, :].astype(F32) + fin[1, 1, at, :].astype(F32)
        hid_ref[at, :] = (after[at, :].astype(F32) + total).astype(BF16)
        return carry

    lax.fori_loop(0, 8, output, 0)

    arrive(vals.at[1], v_sem.at[1])

    def gaps(v, n):
        valid = frame < n
        reward = jnp.sum(jnp.where(frame == n - 1, v, 0.0), axis=(0, 1), keepdims=True)
        return valid, jnp.where(valid, reward - v, 0.0)

    other = vf_ref[1 - c]
    count = (length + other).astype(F32)
    valid, gap = gaps(values, length)
    valid_o, gap_o = gaps(vals[1], other)
    add = lambda a: jnp.sum(a, axis=(0, 1), keepdims=True)
    mean = (add(gap) + add(gap_o)) / count
    centered = jnp.where(valid, gap - mean, 0.0)
    centered_o = jnp.where(valid_o, gap_o - mean, 0.0)
    variance = (add(centered * centered) + add(centered_o * centered_o)) / count
    adv = jnp.where(valid, centered * lax.rsqrt(variance + 1e-5), 0.0)
    lane = lax.broadcasted_iota(jnp.int32, (1, 128), 1)

    def own_pair(a):
        first = jnp.sum(jnp.where(frame == 2 * s, a, 0.0), axis=(0, 1))
        second = jnp.sum(jnp.where(frame == 2 * s + 1, a, 0.0), axis=(0, 1))
        return jnp.where(lane == 0, first.reshape(1, 128), second.reshape(1, 128))[:, 0:2]

    fv_ref[...] = own_pair(values)
    adv_ref[...] = own_pair(adv)
    for copy in sends:
        copy.wait_send()


def rest(heads, tokens, w_out, mlp_gain, w_up, w_down, pool_gain, pool_bias, value_weight, lengths):
    vmem = pltpu.VMEM
    dma = pltpu.SemaphoreType.DMA
    inside = pl.BlockSpec(memory_space=pltpu.VMEM)
    outside = pl.BlockSpec(memory_space=pl.ANY)
    return pl.pallas_call(
        mlp_kernel,
        out_shape=(
            jax.ShapeDtypeStruct((ROWS, D), BF16),
            jax.ShapeDtypeStruct((1, 2), F32),
            jax.ShapeDtypeStruct((1, 2), F32),
        ),
        in_specs=[pl.BlockSpec(memory_space=pltpu.SMEM)] + [inside] * 6 + [outside] * 3,
        out_specs=(inside,) * 3,
        scratch_shapes=[
            vmem((BLOCK, D), BF16),
            vmem((D, D), BF16),
            vmem((D, D), BF16),
            vmem((2, 4, ROWS, D), BF16),
            vmem((2, 2, 64, D), BF16),
            vmem((2, 2, ROWS, D), BF16),
            vmem((4, ROWS, D), BF16),
            vmem((ROWS, D), BF16),
            vmem((ROWS, D), F32),
            vmem((2 * ROWS, D), BF16),
            vmem((2, 8, D), F32),
            vmem((4, 2, D), F32),
            vmem((16, 2, D), F32),
            vmem((16, 2, D), F32),
            vmem((2, 16, 2, 128), F32),
            dma((3,)),
            dma((2, 6)),
            dma((2, 2)),
            dma((2, 2, 2)),
            dma((2, 3)),
            dma((2, 3)),
            dma((3,)),
            dma((4,)),
            dma((15,)),
            dma((16,)),
            dma((2,)),
        ],
        compiler_params=pltpu.CompilerParams(
            collective_id=1, has_side_effects=True, vmem_limit_bytes=56 * 2**20
        ),
        cost_estimate=pl.CostEstimate(flops=2 * 10**10, bytes_accessed=4 * 10**7, transcendentals=10**6),
    )(
        lengths, heads, tokens, mlp_gain.reshape(1, D), pool_gain.reshape(1, D), pool_bias.reshape(1, D),
        value_weight.reshape(1, D), w_out, w_up, w_down,
    )


def local(
    tokens, attn_gain, w_qkv, w_out, mlp_gain, w_up, w_down, pool_gain, pool_bias, value_weight, valid_frames
):
    heads = attention(tokens[0], attn_gain, w_qkv, valid_frames)
    hidden, values, advantages = rest(
        heads, tokens[0], w_out, mlp_gain, w_up, w_down, pool_gain, pool_bias, value_weight, valid_frames
    )
    return hidden[None], values, advantages


def solution(mesh):
    in_specs = (
        P("dp", ("seq", "tensor"), None),
        P(),
        P(None, None, "tensor"),
        P("tensor", None),
        P(),
        P(None, "tensor"),
        P("tensor", None),
        P(),
        P(),
        P(),
        P(),
    )
    out_specs = (P("dp", ("seq", "tensor"), None), P("dp", "seq"), P("dp", "seq"))
    return jax.shard_map(local, mesh=mesh, in_specs=in_specs, out_specs=out_specs, check_vma=False)
```

```python
import functools
import math

import jax
import jax.numpy as jnp
from jax import lax
from jax.experimental import pallas as pl
from jax.experimental.pallas import tpu as pltpu
from jax.sharding import PartitionSpec as P

HEAD_DIM = 128
TOK_FRAME = 256
ROWS = 128
HALF = 64
BLOCK = 512
D = 2048
DEPTH = 144
BF16 = jnp.bfloat16
F32 = jnp.float32
MESH = pl.DeviceIdType.MESH
QSCALE = math.log2(math.e) / math.sqrt(HEAD_DIM)
NEG = -1e30
ONWARD = (0, 1)


def remote(src, dst, send_sem, recv_sem, where):
    return pltpu.make_async_remote_copy(
        src_ref=src, dst_ref=dst, send_sem=send_sem, recv_sem=recv_sem,
        device_id=where, device_id_type=MESH,
    )


def al(i, m):
    return pl.multiple_of(i, m)


class Place:
    def __init__(self):
        self.c = lax.axis_index("dp")
        s = lax.axis_index("seq")
        self.s = s
        self.z = lax.axis_index("tensor")
        y, x = s // 4, s % 4
        self.p = y * (1 - self.c) + x * self.c
        self.g = x * (1 - self.c) + y * self.c

    def seq(self, p, g):
        return (p * 4 + g) * (1 - self.c) + (g * 4 + p) * self.c

    def flip(self, p):
        return (1 - self.c) * (1 - p % 2) + self.c * (p // 2)

    def gq(self, p, g):
        return g + self.flip(p) * (3 - 2 * g)


def norm_rows(src, gain_ref, dst, rows):
    def body(i, carry):
        at = pl.ds(al(i * 16, 16), 16)
        x = src[at, :].astype(F32)
        square = jnp.mean(x * x, axis=-1, keepdims=True)
        dst[at, :] = (x * lax.rsqrt(square + 1e-5) * gain_ref[...]).astype(BF16)
        return carry

    lax.fori_loop(0, rows // 16, body, 0, unroll=True)


def attn_kernel(
    vf_ref, tok_hbm, gain_hbm, w_hbm, mixed_ref,
    tok, w, gain_ref, normed, stage, qx, kx, vt, m_s, acc, s0, s1, o_stage,
    tl_sem, w_sem, ts_sem, tr_sem, a_send, q_recv, k_recv, qs_recv,
    g_send, gk_recv, r_recv, o_send, o_recv,
):
    me = Place()
    c, z, p, g = me.c, me.z, me.p, me.g
    zp, zm, z2 = (z + 1) % 4, (z + 3) % 4, (z + 2) % 4
    gp, gm, g2 = (g + 1) % 4, (g + 3) % 4, (g + 2) % 4
    flip = me.flip(p)

    own_in = pltpu.make_async_copy(tok_hbm, tok.at[z], tl_sem.at[0])
    own_in.start()
    gain_in = pltpu.make_async_copy(gain_hbm, gain_ref, tl_sem.at[1])
    gain_in.start()
    w_in = [pltpu.make_async_copy(w_hbm.at[k], w.at[k], w_sem.at[k]) for k in range(3)]
    for copy in w_in:
        copy.start()

    barrier = pltpu.get_barrier_semaphore()
    for t in (zp, zm):
        pl.semaphore_signal(barrier, inc=1, device_id={"tensor": t}, device_id_type=MESH)
    for d in (1, 2, 3):
        pl.semaphore_signal(barrier, inc=1, device_id={"seq": me.seq((p + d) % 4, g)}, device_id_type=MESH)
    for d in range(4):
        pl.semaphore_signal(barrier, inc=1, device_id={"seq": me.seq((p + d) % 4, 3 - g)}, device_id_type=MESH)
    for k in (gp, gm):
        pl.semaphore_signal(barrier, inc=1, device_id={"seq": me.seq(p, k)}, device_id_type=MESH)
    own_in.wait()
    pl.semaphore_wait(barrier, 11)

    halves = (pl.ds(0, HALF), pl.ds(HALF, HALF))
    sends = []

    def send(src, dst, send_sem, recv_sem, to):
        copy = remote(src, dst, send_sem, recv_sem, to)
        copy.start()
        sends.append(copy)

    def arrive(ref, sem):
        remote(ref, ref, sem, sem, {"tensor": zp}).wait_recv()

    def tok_send(direction, k, t, half):
        ref = tok.at[t, halves[half], :]
        send(ref, ref, ts_sem.at[direction, k], tr_sem.at[direction, k], {"tensor": zp if direction == 0 else zm})

    def tok_wait(direction, k, t, half):
        arrive(tok.at[t, halves[half], :], tr_sem.at[direction, k])

    tok_send(0, 0, z, 0)
    tok_send(1, 0, z, 1)
    tok_send(0, 1, z, 1)
    tok_send(1, 1, z, 0)

    stages = (((z, 0), (z, 1)), ((zm, 0), (zp, 1)), ((zm, 1), (zp, 0)), ((z2, 0), (z2, 1)))

    def rows_of(piece):
        t, half = piece
        return pl.ds(al(t * ROWS + half * HALF, HALF), HALF)

    def project(n):
        for k, (t, half) in enumerate(stages[n]):
            norm_rows(tok.at[t, halves[half], :], gain_ref, normed.at[halves[k], :], HALF)
        for k in (1, 2, 0):
            for pair in range(2):
                out = jnp.dot(
                    normed[...], w[k, :, pair * 256 : pair * 256 + 256], preferred_element_type=F32
                )
                if k == 0:
                    out = out * QSCALE
                out = out.astype(BF16)
                at = slice((2 - k) * 128, (3 - k) * 128)
                stage[n, 2 * pair, :, at] = out[:, :128]
                stage[n, 2 * pair + 1, :, at] = out[:, 128:]

    both = pl.ds(0, 256)
    third = pl.ds(256, 128)
    lanes = pl.ds(0, HEAD_DIM)

    def pieces(n):
        if n in (0, 3):
            return ((pl.ds(0, ROWS), pl.ds(al(stages[n][0][0] * ROWS, ROWS), ROWS)),)
        return tuple((halves[k], rows_of(piece)) for k, piece in enumerate(stages[n]))

    def hand_out(n):
        for k, (buf, sem, part) in enumerate(((kx, k_recv, both), (qx, q_recv, third))):
            for d in (2, 1, 3):
                h = (p + d) % 4
                to = {"seq": me.seq(h, me.gq(p, g) if k else g)}
                slot = p if k else g * 4 + p
                for half, (src, dst) in enumerate(pieces(n)):
                    send(
                        stage.at[n, h, src, part], buf.at[slot, dst, lanes if k else both],
                        a_send.at[n, d - 1, k, half], sem.at[n], to,
                    )
        for src, dst in pieces(n):
            kx[g * 4 + p, dst, 0:256] = stage[n, p, src, 0:256]

        @pl.when(flip == 1)
        def _():
            for half, (src, dst) in enumerate(pieces(n)):
                remote(
                    stage.at[n, p, src, third], qx.at[p, dst, lanes],
                    a_send.at[n, 3, 0, half], qs_recv.at[n], {"seq": me.seq(p, 3 - g)},
                ).start()

        @pl.when(flip == 0)
        def _():
            for src, dst in pieces(n):
                qx[p, dst, 0:128] = stage[n, p, src, 256:384]

    def stage_in(count, buf, sem):
        arrive(buf.at[pl.ds(0, count), pl.ds(0, ROWS), lanes if buf is qx else both], sem)

    def ring_out(n):
        stage_in(3, kx, k_recv.at[n])
        for direction in (0, 1):
            to = {"seq": me.seq(p, gp if direction == 0 else gm)}
            for half, (_, dst) in enumerate(pieces(n)):
                ref = kx.at[pl.ds(g * 4, 4), dst, both]
                send(ref, ref, g_send.at[direction, n, half], gk_recv.at[direction, n], to)

    def relay(n):
        for direction in sorted(set(ONWARD)):
            stage_in(4, kx, gk_recv.at[direction, n])
            source, to = (gm, gp) if direction == 0 else (gp, gm)
            if ONWARD[0] == ONWARD[1]:
                runs = pieces(n)
            else:
                runs = ((0, rows_of(stages[n][direction])),)
            for half, (_, dst) in enumerate(runs):
                ref = kx.at[pl.ds(source * 4, 4), dst, both]
                send(ref, ref, g_send.at[direction, n, 2 + half], r_recv.at[n], {"seq": me.seq(p, to)})

    gain_in.wait()
    for copy in w_in:
        copy.wait()
    project(0)
    hand_out(0)

    length = vf_ref[c]
    lane = lax.broadcasted_iota(jnp.int32, (BLOCK, 128), 1)
    row = lax.broadcasted_iota(jnp.int32, (BLOCK, 128), 0)

    def fill(slot, carry):
        block = me.seq(slot % 4, slot // 4)
        frame = 2 * block + row // TOK_FRAME
        bias = jnp.where((lane == 0) & (frame >= length), NEG, 0.0)
        mine = 0
        for i in range(4):
            mine = mine + (lane == 1 + i).astype(jnp.int32) * (
                me.seq(i, me.gq(i, g)) == block
            ).astype(jnp.int32)
        bias = jnp.where((mine > 0) & (row >= TOK_FRAME), NEG, bias)
        kx[slot, :, 256:384] = bias.astype(BF16)
        vt[slot, 128:DEPTH, :] = jnp.ones((DEPTH - 128, BLOCK), BF16)
        return carry

    lax.fori_loop(0, 16, fill, 0)
    kx[16, :, 0:256] = jnp.zeros((BLOCK, 256), BF16)
    kx[16, :, 256:384] = jnp.where(lane == 0, NEG, 0.0).astype(BF16)
    vt[16] = jnp.zeros((DEPTH, BLOCK), BF16)
    for i in range(4):
        on = (lane == 0) | ((lane == 1 + i) & (row < TOK_FRAME))
        qx[i, :, 128:256] = jnp.where(on, 1.0, 0.0).astype(BF16)
        m_s[i] = jnp.full((8, BLOCK), -1e38, F32)
        acc[i] = jnp.zeros((DEPTH, BLOCK), F32)

    tok_wait(0, 0, zm, 0)
    tok_send(0, 2, zm, 0)
    tok_wait(1, 0, zp, 1)
    tok_send(1, 2, zp, 1)
    ring_out(0)
    project(1)
    hand_out(1)
    tok_wait(0, 1, zm, 1)
    tok_wait(1, 1, zp, 0)
    project(2)
    hand_out(2)
    ring_out(1)
    relay(0)
    tok_wait(0, 2, z2, 0)
    tok_wait(1, 2, z2, 1)
    project(3)
    hand_out(3)
    ring_out(2)
    relay(1)
    ring_out(3)
    relay(2)
    for n in range(4):
        stage_in(3, qx, q_recv.at[n])

        @pl.when(flip == 1)
        def _():
            stage_in(1, qx, qs_recv.at[n])

    def turn(gg):
        def body(j, carry):
            vt[gg * 4 + j, 0:128, :] = kx[gg * 4 + j, :, 0:128].T
            return carry

        lax.fori_loop(0, 4, body, 0)

    turn(g)
    relay(3)
    for direction in (0, 1):
        if direction not in ONWARD:
            for n in range(4):
                stage_in(4, kx, gk_recv.at[direction, n])
    turn(gm)
    turn(gp)
    for n in range(4):
        stage_in(4, kx, r_recv.at[n])
    turn(g2)

    def slot_of(b, count):
        pad = b // count
        slot = (1 - c) * ((b % 4) * 4 + b // 4) + c * b
        return (1 - pad) * slot + pad * 16

    def score(i, slot, buf):
        for a in (0, 256):
            buf[:, a : a + 256] = lax.dot_general(
                kx[slot, :, 128:384], qx[i, a : a + 256, :], (((1,), (1,)), ((), ())), preferred_element_type=F32
            )

    def gather(i, slot, buf):
        for a in (0, 256):
            at = slice(a, a + 256)
            s = buf[:, at]
            before = m_s[i, 0:1, at]
            peak = jnp.maximum(before, jnp.max(s, axis=0, keepdims=True))
            m_s[i, 0:1, at] = peak
            weights = jnp.exp2(s - peak).astype(BF16)
            acc[i, :, at] = acc[i, :, at] * jnp.exp2(before - peak) + jnp.dot(
                vt[slot], weights, preferred_element_type=F32
            )

    def back(i):
        return remote(
            o_stage.at[i], mixed_ref.at[p], o_send.at[i], o_recv.at[p], {"seq": me.seq(i, me.gq(i, g))}
        )

    score(0, 0, s0)
    for i in range(4):
        count = me.seq(i, me.gq(i, g)) + 1
        steps = (count + 1) // 2

        def two(n, carry):
            score(i, slot_of(2 * n + 1, count), s1)
            gather(i, slot_of(2 * n, count), s0)
            over = (n + 1) // steps
            score(min(i + 1, 3) * over + i * (1 - over), (1 - over) * slot_of(2 * n + 2, count), s0)
            gather(i, slot_of(2 * n + 1, count), s1)
            return carry

        lax.fori_loop(0, steps, two, 0)
        out = acc[i, 0:128, :] / acc[i, 128:129, :]
        o_stage[i] = out.T.astype(BF16)
        stays = (1 - flip) * (p == i).astype(jnp.int32)

        @pl.when(stays == 0)
        def _():
            back(i).start()

        @pl.when(stays == 1)
        def _():
            mixed_ref[p] = o_stage[i]

    for d in (1, 2, 3):
        h = (p + d) % 4
        arrive(mixed_ref.at[h], o_recv.at[h])

    @pl.when(flip == 1)
    def _():
        arrive(mixed_ref.at[p], o_recv.at[p])
        for n in range(4):
            for half, (src, dst) in enumerate(pieces(n)):
                remote(
                    stage.at[n, p, src, third], qx.at[p, dst, lanes],
                    a_send.at[n, 3, 0, half], qs_recv.at[n], {"seq": me.seq(p, 3 - g)},
                ).wait_send()

    for i in range(4):
        stays = (1 - flip) * (p == i).astype(jnp.int32)

        @pl.when(stays == 0)
        def _():
            back(i).wait_send()

    for copy in sends:
        copy.wait_send()


def attention(tokens, gain, w_qkv, lengths):
    vmem = pltpu.VMEM
    dma = pltpu.SemaphoreType.DMA
    outside = pl.BlockSpec(memory_space=pl.ANY)
    return pl.pallas_call(
        attn_kernel,
        out_shape=jax.ShapeDtypeStruct((4, BLOCK, HEAD_DIM), BF16),
        in_specs=[pl.BlockSpec(memory_space=pltpu.SMEM), outside, outside, outside],
        out_specs=pl.BlockSpec(memory_space=pltpu.VMEM),
        scratch_shapes=[
            vmem((4, ROWS, D), BF16),
            vmem((3, D, BLOCK), BF16),
            vmem((1, D), F32),
            vmem((ROWS, D), BF16),
            vmem((4, 4, ROWS, 384), BF16),
            vmem((4, BLOCK, 256), BF16),
            vmem((17, BLOCK, 384), BF16),
            vmem((17, DEPTH, BLOCK), BF16),
            vmem((4, 8, BLOCK), F32),
            vmem((4, DEPTH, BLOCK), F32),
            vmem((BLOCK, BLOCK), F32),
            vmem((BLOCK, BLOCK), F32),
            vmem((4, BLOCK, HEAD_DIM), BF16),
            dma((2,)),
            dma((3,)),
            dma((2, 3)),
            dma((2, 3)),
            dma((4, 4, 2, 2)),
            dma((4,)),
            dma((4,)),
            dma((4,)),
            dma((2, 4, 4)),
            dma((2, 4)),
            dma((4,)),
            dma((4,)),
            dma((4,)),
        ],
        compiler_params=pltpu.CompilerParams(
            collective_id=0, has_side_effects=True, vmem_limit_bytes=52 * 2**20
        ),
        cost_estimate=pl.CostEstimate(flops=2 * 10**10, bytes_accessed=2 * 10**7, transcendentals=10**7),
    )(lengths, tokens, gain.reshape(1, D), w_qkv)


def gelu(x):
    return 0.5 * x * (1.0 + jnp.tanh(math.sqrt(2.0 / math.pi) * (x + 0.044715 * (x * x * x))))


def mlp_kernel(
    vf_ref, mixed_ref, tok_ref, gain_ref, pg_ref, pb_ref, vw_ref, wo_hbm, wu_hbm, wd_hbm,
    hid_ref, fv_ref, adv_ref,
    wo, wu, wd, part, mid, fin, nrm, after, own, up, fs, zs, means, states, vals,
    w_sem, rs_send, mid_recv, fin_recv, ag_send, ag_recv, z_send, z_recv, s_send, s_recv, v_sem,
):
    c, s, z = lax.axis_index("dp"), lax.axis_index("seq"), lax.axis_index("tensor")
    zp, zm, z2 = (z + 1) % 4, (z + 3) % 4, (z + 2) % 4
    w_in = [
        pltpu.make_async_copy(src, dst, w_sem.at[k])
        for k, (src, dst) in enumerate(((wo_hbm, wo), (wu_hbm, wu), (wd_hbm, wd)))
    ]
    for copy in w_in:
        copy.start()
    barrier = pltpu.get_barrier_semaphore()
    for t in (zp, zm, z2):
        pl.semaphore_signal(barrier, inc=1, device_id={"tensor": t}, device_id_type=MESH)
    for d in range(1, 16):
        pl.semaphore_signal(barrier, inc=1, device_id={"seq": (s + d) % 16}, device_id_type=MESH)
    pl.semaphore_signal(barrier, inc=1, device_id={"dp": 1 - c}, device_id_type=MESH)

    lo, hi = pl.ds(0, 64), pl.ds(64, 64)
    sends = []

    def send(src, dst, send_sem, recv_sem, to):
        copy = remote(src, dst, send_sem, recv_sem, to)
        copy.start()
        sends.append(copy)

    def arrive(ref, sem):
        remote(ref, ref, sem, sem, {"tensor": zp}).wait_recv()

    def out_project(t):
        rows = pl.ds(al(t * ROWS, ROWS), ROWS)
        lhs = jnp.concatenate([mixed_ref[h, rows, :] for h in range(4)], axis=1)
        for n in range(4):
            cols = slice(n * 512, n * 512 + 512)
            part[0, t, :, cols] = jnp.dot(lhs, wo[:, cols], preferred_element_type=F32).astype(BF16)

    def send_mids(k):
        send(part.at[k, z2, lo, :], mid.at[k, 0], rs_send.at[k, 0], mid_recv.at[k, 0], {"tensor": zp})
        send(part.at[k, z2, hi, :], mid.at[k, 1], rs_send.at[k, 1], mid_recv.at[k, 1], {"tensor": zm})

    def send_direct(k):
        send(part.at[k, zp, hi, :], fin.at[k, 0, hi, :], rs_send.at[k, 2], fin_recv.at[k, 0, 1], {"tensor": zp})
        send(part.at[k, zm, lo, :], fin.at[k, 1, lo, :], rs_send.at[k, 3], fin_recv.at[k, 1, 0], {"tensor": zm})

    def send_sums(k):
        for direction, (t, half) in enumerate(((zp, 0), (zm, 64))):
            arrive(mid.at[k, direction], mid_recv.at[k, direction])

            def add(i, carry):
                at = pl.ds(al(i * 16, 16), 16)
                to = pl.ds(al(half + i * 16, 16), 16)
                part[k, t, to, :] = (part[k, t, to, :].astype(F32) + mid[k, direction, at, :].astype(F32)).astype(BF16)
                return carry

            lax.fori_loop(0, 4, add, 0)
            rows = pl.ds(half, 64)
            send(
                part.at[k, t, rows, :], fin.at[k, direction, rows, :], rs_send.at[k, 4 + direction],
                fin_recv.at[k, direction, direction], {"tensor": t},
            )

    def wait_final(k):
        for direction in (0, 1):
            for half, rows in enumerate((lo, hi)):
                arrive(fin.at[k, direction, rows, :], fin_recv.at[k, direction, half])

    w_in[0].wait()
    out_project(z2)
    pl.semaphore_wait(barrier, 19)
    send_mids(0)
    out_project(zp)
    out_project(zm)
    send_direct(0)
    out_project(z)
    send_sums(0)
    wait_final(0)

    def settle(i, carry):
        at = pl.ds(al(i * 16, 16), 16)
        total = part[0, z, at, :].astype(F32) + fin[0, 0, at, :].astype(F32) + fin[0, 1, at, :].astype(F32)
        x = (tok_ref[at, :].astype(F32) + total).astype(BF16)
        after[at, :] = x
        x = x.astype(F32)
        square = jnp.mean(x * x, axis=-1, keepdims=True)
        nrm[z, at, :] = (x * lax.rsqrt(square + 1e-5) * gain_ref[...]).astype(BF16)
        return carry

    lax.fori_loop(0, 8, settle, 0)

    halves = (lo, hi)

    def ring_send(direction, k, t, half):
        ref = nrm.at[t, halves[half], :]
        send(ref, ref, ag_send.at[direction, k], ag_recv.at[direction, k], {"tensor": zp if direction == 0 else zm})

    def ring_wait(direction, k, t, half):
        arrive(nrm.at[t, halves[half], :], ag_recv.at[direction, k])

    ring_send(0, 0, z, 0)
    ring_send(1, 0, z, 1)
    ring_send(0, 1, z, 1)
    ring_send(1, 1, z, 0)

    for k in (0, 1):
        fs[k] = jnp.zeros((8, D), F32)

    def up_down(ts, keep):
        rows = ROWS * len(ts)

        def up_step(n, carry):
            cols = pl.ds(al(n * 256, 256), 256)
            lhs = jnp.concatenate([nrm[t] for t in ts], axis=0) if len(ts) > 1 else nrm[ts[0]]
            x = jnp.dot(lhs, wu[:, cols], preferred_element_type=F32)
            up[0:rows, cols] = gelu(x).astype(BF16)
            return carry

        lax.fori_loop(0, 8, up_step, 0)

        def down_step(n, carry):
            cols = pl.ds(al(n * 256, 256), 256)
            x = jnp.dot(up[0:rows, :], wd[:, cols], preferred_element_type=F32)
            for k, t in enumerate(ts):
                y = x[k * ROWS : (k + 1) * ROWS]
                fs[t // 2, :, cols] += jnp.sum(y.reshape(16, 8, 256), axis=0)
                if keep:
                    own[:, cols] = y
                else:
                    part[1, t, :, cols] = y.astype(BF16)
            return carry

        lax.fori_loop(0, 8, down_step, 0)

    w_in[1].wait()
    w_in[2].wait()
    up_down((z,), True)
    ring_wait(0, 0, zm, 0)
    ring_send(0, 2, zm, 0)
    ring_wait(1, 0, zp, 1)
    ring_send(1, 2, zp, 1)

    def residual(i, carry):
        at = pl.ds(al(i * 16, 16), 16)
        fs[z // 2] += jnp.sum(after[at, :].astype(F32).reshape(2, 8, D), axis=0)
        return carry

    lax.fori_loop(0, 8, residual, 0)
    ring_wait(0, 1, zm, 1)
    ring_wait(1, 1, zp, 0)
    up_down((zm, zp), False)
    send_direct(1)
    ring_wait(0, 2, z2, 0)
    ring_wait(1, 2, z2, 1)
    up_down((z2,), False)

    for k in (0, 1):
        zs[z, k : k + 1, :] = jnp.sum(fs[k], axis=0, keepdims=True)
    for d in (1, 2, 3):
        send(zs.at[z], zs.at[z], z_send.at[d - 1], z_recv.at[z], {"tensor": (z + d) % 4})
    send_mids(1)
    for d in (1, 2, 3):
        t = (z + d) % 4
        arrive(zs.at[t], z_recv.at[t])
    means[s] = (zs[0] + zs[1] + zs[2] + zs[3]) * (1.0 / TOK_FRAME)
    for d in range(1, 16):
        send(means.at[s], means.at[s], s_send.at[d - 1], s_recv.at[s], {"seq": (s + d) % 16})
    send_sums(1)

    for d in range(1, 16):
        t = (s + d) % 16
        arrive(means.at[t], s_recv.at[t])
    length = vf_ref[c]
    frame = 2 * lax.broadcasted_iota(jnp.int32, (16, 2, 128), 0) + lax.broadcasted_iota(jnp.int32, (16, 2, 128), 1)
    pg, pb, vw = pg_ref[...], pb_ref[...], vw_ref[...]

    def scan(i, state):
        m = means[i]
        gate = jax.nn.sigmoid(m * pg + pb)
        source = (1.0 - gate) * m
        for k in (0, 1):
            new = gate[k : k + 1] * state + source[k : k + 1]
            state = jnp.where(2 * i + k < length, new, state)
            states[i, k : k + 1, :] = state
        return state

    lax.fori_loop(0, 16, scan, jnp.zeros((1, D), F32))
    total = jnp.sum(states[...] * vw.reshape(1, 1, D), axis=-1, keepdims=True)
    values = jnp.where(frame < length, jnp.broadcast_to(total, (16, 2, 128)), 0.0)
    vals[0] = values
    send(vals.at[0], vals.at[1], v_sem.at[0], v_sem.at[1], {"dp": 1 - c})

    wait_final(1)

    def output(i, carry):
        at = pl.ds(al(i * 16, 16), 16)
        total = own[at, :] + fin[1, 0, at, :].astype(F32) + fin[1, 1, at, :].astype(F32)
        hid_ref[at, :] = (after[at, :].astype(F32) + total).astype(BF16)
        return carry

    lax.fori_loop(0, 8, output, 0)

    arrive(vals.at[1], v_sem.at[1])

    def gaps(v, n):
        valid = frame < n
        reward = jnp.sum(jnp.where(frame == n - 1, v, 0.0), axis=(0, 1), keepdims=True)
        return valid, jnp.where(valid, reward - v, 0.0)

    other = vf_ref[1 - c]
    count = (length + other).astype(F32)
    valid, gap = gaps(values, length)
    valid_o, gap_o = gaps(vals[1], other)
    add = lambda a: jnp.sum(a, axis=(0, 1), keepdims=True)
    mean = (add(gap) + add(gap_o)) / count
    centered = jnp.where(valid, gap - mean, 0.0)
    centered_o = jnp.where(valid_o, gap_o - mean, 0.0)
    variance = (add(centered * centered) + add(centered_o * centered_o)) / count
    adv = jnp.where(valid, centered * lax.rsqrt(variance + 1e-5), 0.0)
    lane = lax.broadcasted_iota(jnp.int32, (1, 128), 1)

    def own_pair(a):
        first = jnp.sum(jnp.where(frame == 2 * s, a, 0.0), axis=(0, 1))
        second = jnp.sum(jnp.where(frame == 2 * s + 1, a, 0.0), axis=(0, 1))
        return jnp.where(lane == 0, first.reshape(1, 128), second.reshape(1, 128))[:, 0:2]

    fv_ref[...] = own_pair(values)
    adv_ref[...] = own_pair(adv)
    for copy in sends:
        copy.wait_send()


def rest(heads, tokens, w_out, mlp_gain, w_up, w_down, pool_gain, pool_bias, value_weight, lengths):
    vmem = pltpu.VMEM
    dma = pltpu.SemaphoreType.DMA
    inside = pl.BlockSpec(memory_space=pltpu.VMEM)
    outside = pl.BlockSpec(memory_space=pl.ANY)
    return pl.pallas_call(
        mlp_kernel,
        out_shape=(
            jax.ShapeDtypeStruct((ROWS, D), BF16),
            jax.ShapeDtypeStruct((1, 2), F32),
            jax.ShapeDtypeStruct((1, 2), F32),
        ),
        in_specs=[pl.BlockSpec(memory_space=pltpu.SMEM)] + [inside] * 6 + [outside] * 3,
        out_specs=(inside,) * 3,
        scratch_shapes=[
            vmem((BLOCK, D), BF16),
            vmem((D, D), BF16),
            vmem((D, D), BF16),
            vmem((2, 4, ROWS, D), BF16),
            vmem((2, 2, 64, D), BF16),
            vmem((2, 2, ROWS, D), BF16),
            vmem((4, ROWS, D), BF16),
            vmem((ROWS, D), BF16),
            vmem((ROWS, D), F32),
            vmem((2 * ROWS, D), BF16),
            vmem((2, 8, D), F32),
            vmem((4, 2, D), F32),
            vmem((16, 2, D), F32),
            vmem((16, 2, D), F32),
            vmem((2, 16, 2, 128), F32),
            dma((3,)),
            dma((2, 6)),
            dma((2, 2)),
            dma((2, 2, 2)),
            dma((2, 3)),
            dma((2, 3)),
            dma((3,)),
            dma((4,)),
            dma((15,)),
            dma((16,)),
            dma((2,)),
        ],
        compiler_params=pltpu.CompilerParams(
            collective_id=1, has_side_effects=True, vmem_limit_bytes=56 * 2**20
        ),
        cost_estimate=pl.CostEstimate(flops=2 * 10**10, bytes_accessed=4 * 10**7, transcendentals=10**6),
    )(
        lengths, heads, tokens, mlp_gain.reshape(1, D), pool_gain.reshape(1, D), pool_bias.reshape(1, D),
        value_weight.reshape(1, D), w_out, w_up, w_down,
    )


def local(
    tokens, attn_gain, w_qkv, w_out, mlp_gain, w_up, w_down, pool_gain, pool_bias, value_weight, valid_frames
):
    heads = attention(tokens[0], attn_gain, w_qkv, valid_frames)
    hidden, values, advantages = rest(
        heads, tokens[0], w_out, mlp_gain, w_up, w_down, pool_gain, pool_bias, value_weight, valid_frames
    )
    return hidden[None], values, advantages


def solution(mesh):
    in_specs = (
        P("dp", ("seq", "tensor"), None),
        P(),
        P(None, None, "tensor"),
        P("tensor", None),
        P(),
        P(None, "tensor"),
        P("tensor", None),
        P(),
        P(),
        P(),
        P(),
    )
    out_specs = (P("dp", ("seq", "tensor"), None), P("dp", "seq"), P("dp", "seq"))
    return jax.shard_map(local, mesh=mesh, in_specs=in_specs, out_specs=out_specs, check_vma=False)
```

```python
import functools
import math

import jax
import jax.numpy as jnp
from jax import lax
from jax.experimental import pallas as pl
from jax.experimental.pallas import tpu as pltpu
from jax.sharding import PartitionSpec as P

HEAD_DIM = 128
TOK_FRAME = 256
ROWS = 128
HALF = 64
BLOCK = 512
D = 2048
DEPTH = 144
BF16 = jnp.bfloat16
F32 = jnp.float32
MESH = pl.DeviceIdType.MESH
QSCALE = math.log2(math.e) / math.sqrt(HEAD_DIM)
NEG = -1e30
ONWARD = (0, 1)
HOOKS = (9, 11)


def remote(src, dst, send_sem, recv_sem, where):
    return pltpu.make_async_remote_copy(
        src_ref=src, dst_ref=dst, send_sem=send_sem, recv_sem=recv_sem,
        device_id=where, device_id_type=MESH,
    )


def al(i, m):
    return pl.multiple_of(i, m)


class Place:
    def __init__(self):
        self.c = lax.axis_index("dp")
        s = lax.axis_index("seq")
        self.s = s
        self.z = lax.axis_index("tensor")
        y, x = s // 4, s % 4
        self.p = y * (1 - self.c) + x * self.c
        self.g = x * (1 - self.c) + y * self.c

    def seq(self, p, g):
        return (p * 4 + g) * (1 - self.c) + (g * 4 + p) * self.c

    def flip(self, p):
        return (1 - self.c) * (1 - p % 2) + self.c * (p // 2)

    def gq(self, p, g):
        return g + self.flip(p) * (3 - 2 * g)


def norm_rows(src, gain_ref, dst, rows):
    def body(i, carry):
        at = pl.ds(al(i * 16, 16), 16)
        x = src[at, :].astype(F32)
        square = jnp.mean(x * x, axis=-1, keepdims=True)
        dst[at, :] = (x * lax.rsqrt(square + 1e-5) * gain_ref[...]).astype(BF16)
        return carry

    lax.fori_loop(0, rows // 16, body, 0, unroll=True)


def gelu(x):
    return 0.5 * x * (1.0 + jnp.tanh(math.sqrt(2.0 / math.pi) * (x + 0.044715 * (x * x * x))))


def layer_kernel(
    vf_ref, tok_hbm, w_hbm, wo_hbm, wu_hbm, wd_hbm, g1_hbm, g2_hbm, pg_hbm, pb_hbm, vw_hbm,
    hid_ref, fv_ref, adv_ref,
    tok, w, small, normed, stage, qx, kx, vt, m_s, acc, s0, s1, o_stage, mx, wo, wu, wd,
    part, mid, fin, nrm, up, fs, zs, means, states, vals,
    tl_sem, w_sem, ts_sem, tr_sem, a_send, q_recv, k_recv, qs_recv,
    g_send, gk_recv, r_recv, o_send, o_recv, m_send, m_recv, w1_send, w1_recv, w2_send, w2_recv, w2r_recv,
    d_send, d_recv, rs_send, mid_recv, fin_recv, z_send, z_recv, s_send, s_recv, v_sem,
):
    me = Place()
    c, s, z, p, g = me.c, me.s, me.z, me.p, me.g
    zp, zm, z2 = (z + 1) % 4, (z + 3) % 4, (z + 2) % 4
    gp, gm, g2 = (g + 1) % 4, (g + 3) % 4, (g + 2) % 4
    flip = me.flip(p)
    gain_ref, gain2_ref = small.at[0:1, :], small.at[1:2, :]

    own_in = pltpu.make_async_copy(tok_hbm, tok.at[z], tl_sem.at[0])
    own_in.start()
    small_in = [
        pltpu.make_async_copy(src, small.at[k : k + 1, :], tl_sem.at[1 + k])
        for k, src in enumerate((g1_hbm, g2_hbm, pg_hbm, pb_hbm, vw_hbm))
    ]
    small_in[0].start()
    w_in = [pltpu.make_async_copy(w_hbm.at[k], w.at[k], w_sem.at[k]) for k in range(3)]
    for copy in w_in:
        copy.start()
    late_in = [
        pltpu.make_async_copy(wo_hbm, wo.at[pl.ds(al(z * BLOCK, BLOCK), BLOCK), :], w_sem.at[3]),
        pltpu.make_async_copy(wu_hbm, wu, w_sem.at[4]),
        pltpu.make_async_copy(wd_hbm, wd, w_sem.at[5]),
    ]

    barrier = pltpu.get_barrier_semaphore()
    for t in (zp, zm, z2):
        pl.semaphore_signal(barrier, inc=1, device_id={"tensor": t}, device_id_type=MESH)
    for d in range(1, 16):
        pl.semaphore_signal(barrier, inc=1, device_id={"seq": (s + d) % 16}, device_id_type=MESH)
    pl.semaphore_signal(barrier, inc=1, device_id={"dp": 1 - c}, device_id_type=MESH)
    own_in.wait()
    pl.semaphore_wait(barrier, 19)

    halves = (pl.ds(0, HALF), pl.ds(HALF, HALF))
    sends = []

    def send(src, dst, send_sem, recv_sem, to):
        copy = remote(src, dst, send_sem, recv_sem, to)
        copy.start()
        sends.append(copy)

    def start_only(src, dst, send_sem, recv_sem, to):
        remote(src, dst, send_sem, recv_sem, to).start()

    def arrive(ref, sem):
        remote(ref, ref, sem, sem, {"tensor": zp}).wait_recv()

    def tok_send(direction, k, t, half):
        ref = tok.at[t, halves[half], :]
        start_only(ref, ref, ts_sem.at[direction, k], tr_sem.at[direction, k], {"tensor": zp if direction == 0 else zm})

    def tok_wait(direction, k, t, half):
        arrive(tok.at[t, halves[half], :], tr_sem.at[direction, k])

    tok_send(0, 0, z, 0)
    tok_send(1, 0, z, 1)
    tok_send(0, 1, z, 1)
    tok_send(1, 1, z, 0)

    stages = (((z, 0), (z, 1)), ((zm, 0), (zp, 1)), ((zm, 1), (zp, 0)), ((z2, 0), (z2, 1)))

    def rows_of(piece):
        t, half = piece
        return pl.ds(al(t * ROWS + half * HALF, HALF), HALF)

    def project(n):
        for k, (t, half) in enumerate(stages[n]):
            norm_rows(tok.at[t, halves[half], :], gain_ref, normed.at[halves[k], :], HALF)
        for k in (1, 2, 0):
            for pair in range(2):
                out = jnp.dot(
                    normed[...], w[k, :, pair * 256 : pair * 256 + 256], preferred_element_type=F32
                )
                if k == 0:
                    out = out * QSCALE
                out = out.astype(BF16)
                at = slice((2 - k) * 128, (3 - k) * 128)
                stage[n, 2 * pair, :, at] = out[:, :128]
                stage[n, 2 * pair + 1, :, at] = out[:, 128:]

    both = pl.ds(0, 256)
    third = pl.ds(256, 128)
    lanes = pl.ds(0, HEAD_DIM)

    def pieces(n):
        if n in (0, 3):
            return ((pl.ds(0, ROWS), pl.ds(al(stages[n][0][0] * ROWS, ROWS), ROWS)),)
        return tuple((halves[k], rows_of(piece)) for k, piece in enumerate(stages[n]))

    def hand_out(n):
        for k, (buf, sem, part) in enumerate(((kx, k_recv, both), (qx, q_recv, third))):
            for d in (2, 1, 3):
                h = (p + d) % 4
                to = {"seq": me.seq(h, me.gq(p, g) if k else g)}
                slot = p if k else g * 4 + p
                for half, (src, dst) in enumerate(pieces(n)):
                    send(
                        stage.at[n, h, src, part], buf.at[slot, dst, lanes if k else both],
                        a_send.at[n, d - 1, k, half], sem.at[n], to,
                    )
        for src, dst in pieces(n):
            kx[g * 4 + p, dst, 0:256] = stage[n, p, src, 0:256]

        @pl.when(flip == 1)
        def _():
            for half, (src, dst) in enumerate(pieces(n)):
                remote(
                    stage.at[n, p, src, third], qx.at[p, dst, lanes],
                    a_send.at[n, 3, 0, half], qs_recv.at[n], {"seq": me.seq(p, 3 - g)},
                ).start()

        @pl.when(flip == 0)
        def _():
            for src, dst in pieces(n):
                qx[p, dst, 0:128] = stage[n, p, src, 256:384]

    def stage_in(count, buf, sem):
        arrive(buf.at[pl.ds(0, count), pl.ds(0, ROWS), lanes if buf is qx else both], sem)

    def ring_out(n):
        stage_in(3, kx, k_recv.at[n])
        for direction in (0, 1):
            to = {"seq": me.seq(p, gp if direction == 0 else gm)}
            for half, (_, dst) in enumerate(pieces(n)):
                ref = kx.at[pl.ds(g * 4, 4), dst, both]
                send(ref, ref, g_send.at[direction, n, half], gk_recv.at[direction, n], to)

    def relay(n):
        for direction in sorted(set(ONWARD)):
            stage_in(4, kx, gk_recv.at[direction, n])
            source, to = (gm, gp) if direction == 0 else (gp, gm)
            if ONWARD[0] == ONWARD[1]:
                runs = pieces(n)
            else:
                runs = ((0, rows_of(stages[n][direction])),)
            for half, (_, dst) in enumerate(runs):
                ref = kx.at[pl.ds(source * 4, 4), dst, both]
                send(ref, ref, g_send.at[direction, n, 2 + half], r_recv.at[n], {"seq": me.seq(p, to)})

    def wo_rows(t, k, first, count):
        return wo.at[pl.ds(al(t * BLOCK + c * 256 + k * 64 + first, 32), count), :]

    def w1_copy(direction, k):
        to = zp if direction == 0 else zm
        t, first = ((z, 0), (z, 32), (zm, 0))[k] if direction == 0 else ((z, 32), (z, 0), (zp, 32))[k]
        ref = wo_rows(t, g, first, 32)
        return remote(ref, ref, w1_send.at[direction, k], w1_recv.at[direction, k], {"tensor": to})

    def w1_arrive(direction, k):
        arrive(wo.at[pl.ds(0, 32), :], w1_recv.at[direction, k])

    def w2_own():
        copies = []
        for direction in (0, 1):
            to = {"seq": me.seq(p, gp if direction == 0 else gm)}
            for k, t in enumerate((zp, zm, z2)):
                ref = wo_rows(t, g, 0, 64)
                copies.append(remote(ref, ref, w2_send.at[direction, k], w2_recv.at[direction], to))
        return copies

    def w2_relay():
        copies = []
        for direction in (0, 1):
            source, to = (gm, gp) if direction == 0 else (gp, gm)
            for k, ref in enumerate(
                (wo_rows(zm if direction else zp, source, 0, 64), wo_rows(z2, source, 32 * direction, 32))
            ):
                copies.append(
                    remote(ref, ref, w2_send.at[direction, 3 + k], w2r_recv.at[direction], {"seq": me.seq(p, to)})
                )
        return copies

    def d2d(n):
        k = (g, gm, gp, g2)[n]
        return [
            remote(ref, ref, d_send.at[n, i], d_recv, {"dp": 1 - c})
            for i, ref in enumerate(wo_rows(t, k, 0, 64) for t in (zp, zm, z2))
        ]

    def start(copies):
        for copy in copies:
            copy.start()

    small_in[0].wait()
    for copy in w_in:
        copy.wait()
    start(late_in)
    start(small_in[1:])
    project(0)
    hand_out(0)

    length = vf_ref[c]
    lane = lax.broadcasted_iota(jnp.int32, (BLOCK, 128), 1)
    row = lax.broadcasted_iota(jnp.int32, (BLOCK, 128), 0)

    def fill(slot, carry):
        block = me.seq(slot % 4, slot // 4)
        frame = 2 * block + row // TOK_FRAME
        bias = jnp.where((lane == 0) & (frame >= length), NEG, 0.0)
        mine = 0
        for i in range(4):
            mine = mine + (lane == 1 + i).astype(jnp.int32) * (
                me.seq(i, me.gq(i, g)) == block
            ).astype(jnp.int32)
        bias = jnp.where((mine > 0) & (row >= TOK_FRAME), NEG, bias)
        kx[slot, :, 256:384] = bias.astype(BF16)
        vt[slot, 128:DEPTH, :] = jnp.ones((DEPTH - 128, BLOCK), BF16)
        return carry

    lax.fori_loop(0, 16, fill, 0)
    kx[16, :, 0:256] = jnp.zeros((BLOCK, 256), BF16)
    kx[16, :, 256:384] = jnp.where(lane == 0, NEG, 0.0).astype(BF16)
    vt[16] = jnp.zeros((DEPTH, BLOCK), BF16)
    for i in range(4):
        on = (lane == 0) | ((lane == 1 + i) & (row < TOK_FRAME))
        qx[i, :, 128:256] = jnp.where(on, 1.0, 0.0).astype(BF16)

    tok_wait(0, 0, zm, 0)
    tok_send(0, 2, zm, 0)
    tok_wait(1, 0, zp, 1)
    tok_send(1, 2, zp, 1)
    ring_out(0)
    project(1)
    hand_out(1)
    tok_wait(0, 1, zm, 1)
    tok_wait(1, 1, zp, 0)
    project(2)
    hand_out(2)
    ring_out(1)
    relay(0)
    tok_wait(0, 2, z2, 0)
    tok_wait(1, 2, z2, 1)
    project(3)
    hand_out(3)
    late_in[0].wait()
    start([w1_copy(0, 0), w1_copy(1, 0), w1_copy(0, 1), w1_copy(1, 1)])
    ring_out(2)
    relay(1)
    ring_out(3)
    relay(2)
    for n in range(4):
        stage_in(3, qx, q_recv.at[n])

        @pl.when(flip == 1)
        def _():
            stage_in(1, qx, qs_recv.at[n])

    def turn(gg):
        def body(j, carry):
            vt[gg * 4 + j, 0:128, :] = kx[gg * 4 + j, :, 0:128].T
            return carry

        lax.fori_loop(0, 4, body, 0)

    w1_arrive(0, 0)
    w1_copy(0, 2).start()
    w1_arrive(1, 0)
    w1_copy(1, 2).start()
    turn(g)
    relay(3)
    for direction in (0, 1):
        if direction not in ONWARD:
            for n in range(4):
                stage_in(4, kx, gk_recv.at[direction, n])
    turn(gm)
    turn(gp)
    for n in range(4):
        stage_in(4, kx, r_recv.at[n])
    turn(g2)
    for direction in (0, 1):
        for k in (1, 2):
            w1_arrive(direction, k)
    start(w2_own())
    start(d2d(0))

    def slot_of(b, count):
        pad = b // count
        slot = (1 - c) * ((b % 4) * 4 + b // 4) + c * b
        return (1 - pad) * slot + pad * 16

    def score(i, a, slot, buf):
        buf[...] = lax.dot_general(
            kx[slot, :, 128:384], qx[i, pl.ds(al(a * 256, 256), 256), :], (((1,), (1,)), ((), ())),
            preferred_element_type=F32,
        )

    def gather(i, slot, buf):
        scores = buf[...]
        before = m_s[i, 0:1, :]
        peak = jnp.maximum(before, jnp.max(scores, axis=0, keepdims=True))
        m_s[i, 0:1, :] = peak
        weights = jnp.exp2(scores - peak).astype(BF16)
        acc[i] = acc[i] * jnp.exp2(before - peak) + jnp.dot(vt[slot], weights, preferred_element_type=F32)

    def back(i, a):
        rows = pl.ds(a * 256, 256)
        return remote(
            o_stage.at[i, rows, :], mx.at[z, p, rows, :], o_send.at[i, a], o_recv.at[p, a],
            {"seq": me.seq(i, me.gq(i, g))},
        )

    def o_arrive(a):
        rows = pl.ds(a * 256, 256)
        for d in (1, 2, 3):
            h = (p + d) % 4
            arrive(mx.at[z, h, rows, :], o_recv.at[h, a])

        @pl.when(flip == 1)
        def _():
            arrive(mx.at[z, p, rows, :], o_recv.at[p, a])

    def mx_copy(a, direction, k):
        to = zp if direction == 0 else zm
        t, half = ((z, 0), (z, 1), (zm, 0))[k] if direction == 0 else ((z, 1), (z, 0), (zp, 1))[k]
        ref = mx.at[t, :, pl.ds(a * 256 + half * ROWS, ROWS), :]
        return remote(ref, ref, m_send.at[a, direction, k], m_recv.at[a, direction, k], {"tensor": to})

    def mx_arrive(a, direction, k):
        arrive(mx.at[z, :, pl.ds(0, ROWS), :], m_recv.at[a, direction, k])

    def mx_own(a):
        start([mx_copy(a, 0, 0), mx_copy(a, 1, 0), mx_copy(a, 0, 1), mx_copy(a, 1, 1)])

    def mx_relay(a):
        for direction in (0, 1):
            mx_arrive(a, direction, 0)
            mx_copy(a, direction, 2).start()

    def w2_onward():
        for direction in (0, 1):
            arrive(wo.at[pl.ds(0, 192), :], w2_recv.at[direction])
        start(w2_relay())
        start(d2d(1))
        start(d2d(2))

    score(0, 0, 0, s0)
    for a in (0, 1):
        base = 0
        for i in range(4):
            m_s[i] = jnp.full((8, 256), -1e38, F32)
            acc[i] = jnp.zeros((DEPTH, 256), F32)
            count = me.seq(i, me.gq(i, g)) + 1
            steps = (count + 1) // 2

            def two(n, carry):
                if a == 1:
                    pl.when(base + n == HOOKS[0])(lambda: (o_arrive(0), mx_own(0))[0])
                    pl.when(base + n == HOOKS[1])(w2_onward)
                score(i, a, slot_of(2 * n + 1, count), s1)
                gather(i, slot_of(2 * n, count), s0)
                over = (n + 1) // steps
                last = i == 3
                score(
                    ((i + 1) % 4) * over + i * (1 - over), min(a + 1, 1) * over + a * (1 - over) if last else a,
                    (1 - over) * slot_of(2 * n + 2, count), s0,
                )
                gather(i, slot_of(2 * n + 1, count), s1)
                return carry

            lax.fori_loop(0, steps, two, 0)
            base = base + steps
            out = acc[i, 0:128, :] / acc[i, 128:129, :]
            o_stage[i, a * 256 : a * 256 + 256, :] = out.T.astype(BF16)
            stays = (1 - flip) * (p == i).astype(jnp.int32)

            @pl.when(stays == 0)
            def _():
                back(i, a).start()

            @pl.when(stays == 1)
            def _():
                mx[z, p, a * 256 : a * 256 + 256, :] = o_stage[i, a * 256 : a * 256 + 256, :]

    mx_relay(0)
    o_arrive(1)
    mx_own(1)
    for direction in (0, 1):
        arrive(wo.at[pl.ds(0, 96), :], w2r_recv.at[direction])
    start(d2d(3))
    for copy in small_in[1:]:
        copy.wait()
    for direction in (0, 1):
        for k in range(3):
            ref = tok.at[0, halves[0], :]
            remote(ref, ref, ts_sem.at[direction, k], ts_sem.at[direction, k], {"tensor": zp}).wait_send()

    def frame_rows(a):
        for direction in (0, 1):
            for k in (1, 2):
                mx_arrive(a, direction, k)

    def out_project(a):
        rows = pl.ds(a * 256, 256)

        def step(n, carry):
            cols = pl.ds(al(n * 512, 512), 512)
            lhs = jnp.concatenate([mx[t, h, rows, :] for t in range(4) for h in range(4)], axis=1)
            x = jnp.dot(lhs, wo[:, cols], preferred_element_type=F32)
            for k in (0, 1):
                t = 2 * a + k
                tok[t, :, cols] = (tok[t, :, cols].astype(F32) + x[k * ROWS : (k + 1) * ROWS]).astype(BF16)
            return carry

        lax.fori_loop(0, 4, step, 0)
        for k in (0, 1):
            norm_rows(tok.at[2 * a + k], gain2_ref, nrm.at[pl.ds(k * ROWS, ROWS), :], ROWS)

    def up_down(a):
        def up_step(n, carry):
            cols = pl.ds(al(n * 512, 512), 512)
            x = jnp.dot(nrm[...], wu[:, cols], preferred_element_type=F32)
            up[:, cols] = gelu(x).astype(BF16)
            return carry

        lax.fori_loop(0, 4, up_step, 0)

        def down_step(n, carry):
            cols = pl.ds(al(n * 512, 512), 512)
            x = jnp.dot(up[...], wd[:, cols], preferred_element_type=F32)
            fs[a, :, cols] = jnp.sum(x.reshape(32, 8, 512), axis=0)
            for k in (0, 1):
                part[2 * a + k, :, cols] = x[k * ROWS : (k + 1) * ROWS].astype(BF16)
            return carry

        lax.fori_loop(0, 4, down_step, 0)

    lo, hi = halves

    def rs_copy(k):
        src, dst, sem, to = (
            (part.at[z2, lo, :], mid.at[0], mid_recv.at[0], zp),
            (part.at[z2, hi, :], mid.at[1], mid_recv.at[1], zm),
            (part.at[zp, hi, :], fin.at[0, hi, :], fin_recv.at[0, 1], zp),
            (part.at[zm, lo, :], fin.at[1, lo, :], fin_recv.at[1, 0], zm),
            (part.at[zp, lo, :], fin.at[0, lo, :], fin_recv.at[0, 0], zp),
            (part.at[zm, hi, :], fin.at[1, hi, :], fin_recv.at[1, 1], zm),
        )[k]
        return remote(src, dst, rs_send.at[k], sem, {"tensor": to})

    def rs_first(a):
        for t, ks in ((z2, (0, 1)), (zp, (2,)), (zm, (3,))):

            @pl.when(t // 2 == a)
            def _():
                for k in ks:
                    rs_copy(k).start()

    frame_rows(0)
    arrive(wo.at[pl.ds(0, 768), :], d_recv)
    out_project(0)
    mx_relay(1)
    late_in[1].wait()
    late_in[2].wait()
    up_down(0)
    rs_first(0)
    frame_rows(1)
    out_project(1)
    up_down(1)

    def residual(i, total):
        at = pl.ds(al(i * 16, 16), 16)
        return total + jnp.sum(tok[z, at, :].astype(F32).reshape(2, 8, D), axis=0)

    own_rows = lax.fori_loop(0, 8, residual, jnp.zeros((8, D), F32))
    for k in (0, 1):
        mine = (z // 2 == k).astype(F32)
        zs[z, k : k + 1, :] = jnp.sum(fs[k] + own_rows * mine, axis=0, keepdims=True)
    for d in (1, 2, 3):
        send(zs.at[z], zs.at[z], z_send.at[d - 1], z_recv.at[z], {"tensor": (z + d) % 4})
    rs_first(1)
    for d in (1, 2, 3):
        t = (z + d) % 4
        arrive(zs.at[t], z_recv.at[t])
    means[s] = (zs[0] + zs[1] + zs[2] + zs[3]) * (1.0 / TOK_FRAME)
    for d in range(1, 16):
        send(means.at[s], means.at[s], s_send.at[d - 1], s_recv.at[s], {"seq": (s + d) % 16})
    for direction, (t, half) in enumerate(((zp, 0), (zm, 64))):
        arrive(mid.at[direction], mid_recv.at[direction])

        def add(i, carry):
            at = pl.ds(al(i * 16, 16), 16)
            to = pl.ds(al(half + i * 16, 16), 16)
            part[t, to, :] = (part[t, to, :].astype(F32) + mid[direction, at, :].astype(F32)).astype(BF16)
            return carry

        lax.fori_loop(0, 4, add, 0)
        rs_copy(4 + direction).start()

    for d in range(1, 16):
        t = (s + d) % 16
        arrive(means.at[t], s_recv.at[t])
    frame = 2 * lax.broadcasted_iota(jnp.int32, (16, 2, 128), 0) + lax.broadcasted_iota(jnp.int32, (16, 2, 128), 1)
    pg, pb, vw = small[2:3, :], small[3:4, :], small[4:5, :]

    def scan(i, state):
        m = means[i]
        gate = jax.nn.sigmoid(m * pg + pb)
        source = (1.0 - gate) * m
        for k in (0, 1):
            new = gate[k : k + 1] * state + source[k : k + 1]
            state = jnp.where(2 * i + k < length, new, state)
            states[i, k : k + 1, :] = state
        return state

    lax.fori_loop(0, 16, scan, jnp.zeros((1, D), F32))
    total = jnp.sum(states[...] * vw.reshape(1, 1, D), axis=-1, keepdims=True)
    values = jnp.where(frame < length, jnp.broadcast_to(total, (16, 2, 128)), 0.0)
    vals[0] = values
    send(vals.at[0], vals.at[1], v_sem.at[0], v_sem.at[1], {"dp": 1 - c})

    for direction in (0, 1):
        for half, rows in enumerate((lo, hi)):
            arrive(fin.at[direction, rows, :], fin_recv.at[direction, half])

    def output(i, carry):
        at = pl.ds(al(i * 16, 16), 16)
        total = part[z, at, :].astype(F32) + fin[0, at, :].astype(F32) + fin[1, at, :].astype(F32)
        hid_ref[at, :] = (tok[z, at, :].astype(F32) + total).astype(BF16)
        return carry

    lax.fori_loop(0, 8, output, 0)

    arrive(vals.at[1], v_sem.at[1])

    def gaps(v, n):
        valid = frame < n
        reward = jnp.sum(jnp.where(frame == n - 1, v, 0.0), axis=(0, 1), keepdims=True)
        return valid, jnp.where(valid, reward - v, 0.0)

    other = vf_ref[1 - c]
    count = (length + other).astype(F32)
    valid, gap = gaps(values, length)
    valid_o, gap_o = gaps(vals[1], other)
    add = lambda a: jnp.sum(a, axis=(0, 1), keepdims=True)
    mean = (add(gap) + add(gap_o)) / count
    centered = jnp.where(valid, gap - mean, 0.0)
    centered_o = jnp.where(valid_o, gap_o - mean, 0.0)
    variance = (add(centered * centered) + add(centered_o * centered_o)) / count
    adv = jnp.where(valid, centered * lax.rsqrt(variance + 1e-5), 0.0)
    lane = lax.broadcasted_iota(jnp.int32, (1, 128), 1)

    def own_pair(a):
        first = jnp.sum(jnp.where(frame == 2 * s, a, 0.0), axis=(0, 1))
        second = jnp.sum(jnp.where(frame == 2 * s + 1, a, 0.0), axis=(0, 1))
        return jnp.where(lane == 0, first.reshape(1, 128), second.reshape(1, 128))[:, 0:2]

    fv_ref[...] = own_pair(values)
    adv_ref[...] = own_pair(adv)
    @pl.when(flip == 1)
    def _():
        for n in range(4):
            for half, (src, dst) in enumerate(pieces(n)):
                remote(
                    stage.at[n, p, src, third], qx.at[p, dst, lanes],
                    a_send.at[n, 3, 0, half], qs_recv.at[n], {"seq": me.seq(p, 3 - g)},
                ).wait_send()

    for i in range(4):
        stays = (1 - flip) * (p == i).astype(jnp.int32)

        @pl.when(stays == 0)
        def _():
            for a in (0, 1):
                back(i, a).wait_send()

    rest = [w1_copy(d, k) for d in (0, 1) for k in range(3)]
    rest += w2_own() + w2_relay() + [copy for n in range(4) for copy in d2d(n)]
    rest += [mx_copy(a, d, k) for a in (0, 1) for d in (0, 1) for k in range(3)]
    rest += [rs_copy(k) for k in range(6)]
    for copy in rest + sends:
        copy.wait_send()


def local(
    tokens, attn_gain, w_qkv, w_out, mlp_gain, w_up, w_down, pool_gain, pool_bias, value_weight, valid_frames
):
    vmem = pltpu.VMEM
    dma = pltpu.SemaphoreType.DMA
    inside = pl.BlockSpec(memory_space=pltpu.VMEM)
    outside = pl.BlockSpec(memory_space=pl.ANY)
    hidden, values, advantages = pl.pallas_call(
        layer_kernel,
        out_shape=(
            jax.ShapeDtypeStruct((ROWS, D), BF16),
            jax.ShapeDtypeStruct((1, 2), F32),
            jax.ShapeDtypeStruct((1, 2), F32),
        ),
        in_specs=[pl.BlockSpec(memory_space=pltpu.SMEM)] + [outside] * 10,
        out_specs=(inside,) * 3,
        scratch_shapes=[
            vmem((4, ROWS, D), BF16),
            vmem((3, D, BLOCK), BF16),
            vmem((8, D), F32),
            vmem((ROWS, D), BF16),
            vmem((4, 4, ROWS, 384), BF16),
            vmem((4, BLOCK, 256), BF16),
            vmem((17, BLOCK, 384), BF16),
            vmem((17, DEPTH, BLOCK), BF16),
            vmem((4, 8, 256), F32),
            vmem((4, DEPTH, 256), F32),
            vmem((BLOCK, 256), F32),
            vmem((BLOCK, 256), F32),
            vmem((4, BLOCK, HEAD_DIM), BF16),
            vmem((4, 4, BLOCK, HEAD_DIM), BF16),
            vmem((D, D), BF16),
            vmem((D, D), BF16),
            vmem((D, D), BF16),
            vmem((4, ROWS, D), BF16),
            vmem((2, 64, D), BF16),
            vmem((2, ROWS, D), BF16),
            vmem((2 * ROWS, D), BF16),
            vmem((2 * ROWS, D), BF16),
            vmem((2, 8, D), F32),
            vmem((4, 2, D), F32),
            vmem((16, 2, D), F32),
            vmem((16, 2, D), F32),
            vmem((2, 16, 2, 128), F32),
            dma((6,)),
            dma((6,)),
            dma((2, 3)),
            dma((2, 3)),
            dma((4, 4, 2, 2)),
            dma((4,)),
            dma((4,)),
            dma((4,)),
            dma((2, 4, 4)),
            dma((2, 4)),
            dma((4,)),
            dma((4, 2)),
            dma((4, 2)),
            dma((2, 2, 3)),
            dma((2, 2, 3)),
            dma((2, 3)),
            dma((2, 3)),
            dma((2, 5)),
            dma((2,)),
            dma((2,)),
            dma((4, 3)),
            dma,
            dma((6,)),
            dma((2,)),
            dma((2, 2)),
            dma((3,)),
            dma((4,)),
            dma((15,)),
            dma((16,)),
            dma((2,)),
        ],
        compiler_params=pltpu.CompilerParams(
            collective_id=0, has_side_effects=True, vmem_limit_bytes=63 * 2**20
        ),
        cost_estimate=pl.CostEstimate(flops=4 * 10**10, bytes_accessed=4 * 10**7, transcendentals=10**7),
    )(
        valid_frames, tokens[0], w_qkv, w_out, w_up, w_down,
        *(v.reshape(1, D) for v in (attn_gain, mlp_gain, pool_gain, pool_bias, value_weight)),
    )
    return hidden[None], values, advantages


def solution(mesh):
    in_specs = (
        P("dp", ("seq", "tensor"), None),
        P(),
        P(None, None, "tensor"),
        P("tensor", None),
        P(),
        P(None, "tensor"),
        P("tensor", None),
        P(),
        P(),
        P(),
        P(),
    )
    out_specs = (P("dp", ("seq", "tensor"), None), P("dp", "seq"), P("dp", "seq"))
    return jax.shard_map(local, mesh=mesh, in_specs=in_specs, out_specs=out_specs, check_vma=False)
```

```python
import functools
import math

import jax
import jax.numpy as jnp
from jax import lax
from jax.experimental import pallas as pl
from jax.experimental.pallas import tpu as pltpu
from jax.sharding import PartitionSpec as P

HEAD_DIM = 128
TOK_FRAME = 256
ROWS = 128
HALF = 64
BLOCK = 512
D = 2048
DEPTH = 144
BF16 = jnp.bfloat16
F32 = jnp.float32
MESH = pl.DeviceIdType.MESH
QSCALE = math.log2(math.e) / math.sqrt(HEAD_DIM)
NEG = -1e30
ONWARD = (0, 1)
HOOKS = (8, 12, 28)
UNROLL = 4


def remote(src, dst, send_sem, recv_sem, where):
    return pltpu.make_async_remote_copy(
        src_ref=src, dst_ref=dst, send_sem=send_sem, recv_sem=recv_sem,
        device_id=where, device_id_type=MESH,
    )


def al(i, m):
    return pl.multiple_of(i, m)


class Place:
    def __init__(self):
        self.c = lax.axis_index("dp")
        s = lax.axis_index("seq")
        self.s = s
        self.z = lax.axis_index("tensor")
        y, x = s // 4, s % 4
        self.p = y * (1 - self.c) + x * self.c
        self.g = x * (1 - self.c) + y * self.c

    def seq(self, p, g):
        return (p * 4 + g) * (1 - self.c) + (g * 4 + p) * self.c

    def flip(self, p):
        return (1 - self.c) * (1 - p % 2) + self.c * (p // 2)

    def gq(self, p, g):
        return g + self.flip(p) * (3 - 2 * g)


def norm_rows(src, gain_ref, dst, rows):
    def body(i, carry):
        at = pl.ds(al(i * 16, 16), 16)
        x = src[at, :].astype(F32)
        square = jnp.mean(x * x, axis=-1, keepdims=True)
        dst[at, :] = (x * lax.rsqrt(square + 1e-5) * gain_ref[...]).astype(BF16)
        return carry

    lax.fori_loop(0, rows // 16, body, 0, unroll=True)


def gelu(x):
    return 0.5 * x * (1.0 + jnp.tanh(math.sqrt(2.0 / math.pi) * (x + 0.044715 * (x * x * x))))


def layer_kernel(
    vf_ref, tok_hbm, w_hbm, wo_hbm, wu_hbm, wd_hbm, g1_hbm, g2_hbm, pg_hbm, pb_hbm, vw_hbm,
    hid_ref, fv_ref, adv_ref,
    tok, w, small, normed, stage, qx, kx, vt, m_s, acc, s0, s1, o_stage, mx, wo, wu, wd,
    part, mid, fin, nrm, up, fs, zs, means, states, vals,
    tl_sem, w_sem, ts_sem, tr_sem, a_send, q_recv, k_recv, qs_recv,
    g_send, gk_recv, r_recv, o_send, o_recv, m_send, m_recv, w1_send, w1_recv, w2_send, w2_recv, w2r_recv,
    d_send, d_recv, rs_send, mid_recv, fin_recv, z_send, z_recv, s_send, s_recv, v_sem,
):
    me = Place()
    c, s, z, p, g = me.c, me.s, me.z, me.p, me.g
    zp, zm, z2 = (z + 1) % 4, (z + 3) % 4, (z + 2) % 4
    gp, gm, g2 = (g + 1) % 4, (g + 3) % 4, (g + 2) % 4
    flip = me.flip(p)
    gain_ref, gain2_ref = small.at[0:1, :], small.at[1:2, :]

    own_in = pltpu.make_async_copy(tok_hbm, tok.at[z], tl_sem.at[0])
    own_in.start()
    small_in = [
        pltpu.make_async_copy(src, small.at[k : k + 1, :], tl_sem.at[1 + k])
        for k, src in enumerate((g1_hbm, g2_hbm, pg_hbm, pb_hbm, vw_hbm))
    ]
    small_in[0].start()
    w_in = [pltpu.make_async_copy(w_hbm.at[k], w.at[k], w_sem.at[k]) for k in range(3)]
    for copy in w_in:
        copy.start()
    late_in = [
        pltpu.make_async_copy(wo_hbm, wo.at[pl.ds(al(z * BLOCK, BLOCK), BLOCK), :], w_sem.at[3]),
        pltpu.make_async_copy(wu_hbm, wu, w_sem.at[4]),
        pltpu.make_async_copy(wd_hbm, wd, w_sem.at[5]),
    ]

    barrier = pltpu.get_barrier_semaphore()
    for t in (zp, zm, z2):
        pl.semaphore_signal(barrier, inc=1, device_id={"tensor": t}, device_id_type=MESH)
    for d in range(1, 16):
        pl.semaphore_signal(barrier, inc=1, device_id={"seq": (s + d) % 16}, device_id_type=MESH)
    pl.semaphore_signal(barrier, inc=1, device_id={"dp": 1 - c}, device_id_type=MESH)
    own_in.wait()
    pl.semaphore_wait(barrier, 19)

    halves = (pl.ds(0, HALF), pl.ds(HALF, HALF))
    sends = []

    def send(src, dst, send_sem, recv_sem, to):
        copy = remote(src, dst, send_sem, recv_sem, to)
        copy.start()
        sends.append(copy)

    def start_only(src, dst, send_sem, recv_sem, to):
        remote(src, dst, send_sem, recv_sem, to).start()

    def arrive(ref, sem):
        remote(ref, ref, sem, sem, {"tensor": zp}).wait_recv()

    def tok_send(direction, k, t, half):
        ref = tok.at[t, halves[half], :]
        start_only(ref, ref, ts_sem.at[direction, k], tr_sem.at[direction, k], {"tensor": zp if direction == 0 else zm})

    def tok_wait(direction, k, t, half):
        arrive(tok.at[t, halves[half], :], tr_sem.at[direction, k])

    tok_send(0, 0, z, 0)
    tok_send(1, 0, z, 1)
    tok_send(0, 1, z, 1)
    tok_send(1, 1, z, 0)

    stages = (((z, 0), (z, 1)), ((zm, 0), (zp, 1)), ((zm, 1), (zp, 0)), ((z2, 0), (z2, 1)))

    def rows_of(piece):
        t, half = piece
        return pl.ds(al(t * ROWS + half * HALF, HALF), HALF)

    def project(n):
        for k, (t, half) in enumerate(stages[n]):
            norm_rows(tok.at[t, halves[half], :], gain_ref, normed.at[halves[k], :], HALF)
        for k in (1, 2, 0):
            for pair in range(2):
                out = jnp.dot(
                    normed[...], w[k, :, pair * 256 : pair * 256 + 256], preferred_element_type=F32
                )
                if k == 0:
                    out = out * QSCALE
                out = out.astype(BF16)
                at = slice((2 - k) * 128, (3 - k) * 128)
                stage[n, 2 * pair, :, at] = out[:, :128]
                stage[n, 2 * pair + 1, :, at] = out[:, 128:]

    def query_rows(piece, count):
        t, half = piece
        return pl.ds(al((t % 2) * 256 + (t // 2) * ROWS + half * HALF, HALF), count)

    both = pl.ds(0, 256)
    third = pl.ds(256, 128)
    lanes = pl.ds(0, HEAD_DIM)

    def pieces(n):
        if n in (0, 3):
            piece = stages[n][0]
            return ((pl.ds(0, ROWS), pl.ds(al(piece[0] * ROWS, ROWS), ROWS), query_rows(piece, ROWS)),)
        return tuple((halves[k], rows_of(piece), query_rows(piece, HALF)) for k, piece in enumerate(stages[n]))

    def hand_out(n):
        for k, (buf, sem, part) in enumerate(((kx, k_recv, both), (qx, q_recv, third))):
            for d in (2, 1, 3):
                h = (p + d) % 4
                to = {"seq": me.seq(h, me.gq(p, g) if k else g)}
                slot = p if k else g * 4 + p
                for half, (src, dst, dst_q) in enumerate(pieces(n)):
                    send(
                        stage.at[n, h, src, part], buf.at[slot, dst_q if k else dst, lanes if k else both],
                        a_send.at[n, d - 1, k, half], sem.at[n], to,
                    )
        for src, dst, _ in pieces(n):
            kx[g * 4 + p, dst, 0:256] = stage[n, p, src, 0:256]

        @pl.when(flip == 1)
        def _():
            for half, (src, _, dst) in enumerate(pieces(n)):
                remote(
                    stage.at[n, p, src, third], qx.at[p, dst, lanes],
                    a_send.at[n, 3, 0, half], qs_recv.at[n], {"seq": me.seq(p, 3 - g)},
                ).start()

        @pl.when(flip == 0)
        def _():
            for src, _, dst in pieces(n):
                qx[p, dst, 0:128] = stage[n, p, src, 256:384]

    def stage_in(count, buf, sem):
        arrive(buf.at[pl.ds(0, count), pl.ds(0, ROWS), lanes if buf is qx else both], sem)

    def ring_out(n):
        stage_in(3, kx, k_recv.at[n])
        for direction in (0, 1):
            to = {"seq": me.seq(p, gp if direction == 0 else gm)}
            for half, (_, dst, _) in enumerate(pieces(n)):
                ref = kx.at[pl.ds(g * 4, 4), dst, both]
                send(ref, ref, g_send.at[direction, n, half], gk_recv.at[direction, n], to)

    def relay(n):
        for direction in sorted(set(ONWARD)):
            stage_in(4, kx, gk_recv.at[direction, n])
            source, to = (gm, gp) if direction == 0 else (gp, gm)
            if ONWARD[0] == ONWARD[1]:
                runs = pieces(n)
            else:
                runs = ((0, rows_of(stages[n][direction]), 0),)
            for half, (_, dst, _) in enumerate(runs):
                ref = kx.at[pl.ds(source * 4, 4), dst, both]
                send(ref, ref, g_send.at[direction, n, 2 + half], r_recv.at[n], {"seq": me.seq(p, to)})

    def wo_rows(t, k, first, count):
        return wo.at[pl.ds(al(t * BLOCK + c * 256 + k * 64 + first, 32), count), :]

    def w1_copy(direction, k):
        to = zp if direction == 0 else zm
        t, first = ((z, 0), (z, 32), (zm, 0))[k] if direction == 0 else ((z, 32), (z, 0), (zp, 32))[k]
        ref = wo_rows(t, g, first, 32)
        return remote(ref, ref, w1_send.at[direction, k], w1_recv.at[direction, k], {"tensor": to})

    def w1_arrive(direction, k):
        arrive(wo.at[pl.ds(0, 32), :], w1_recv.at[direction, k])

    def w2_own():
        copies = []
        for direction in (0, 1):
            to = {"seq": me.seq(p, gp if direction == 0 else gm)}
            for k, t in enumerate((zp, zm, z2)):
                ref = wo_rows(t, g, 0, 64)
                copies.append(remote(ref, ref, w2_send.at[direction, k], w2_recv.at[direction], to))
        return copies

    def w2_relay():
        copies = []
        for direction in (0, 1):
            source, to = (gm, gp) if direction == 0 else (gp, gm)
            for k, ref in enumerate(
                (wo_rows(zm if direction else zp, source, 0, 64), wo_rows(z2, source, 32 * direction, 32))
            ):
                copies.append(
                    remote(ref, ref, w2_send.at[direction, 3 + k], w2r_recv.at[direction], {"seq": me.seq(p, to)})
                )
        return copies

    def d2d(n):
        k = (g, gm, gp, g2)[n]
        return [
            remote(ref, ref, d_send.at[n, i], d_recv, {"dp": 1 - c})
            for i, ref in enumerate(wo_rows(t, k, 0, 64) for t in (zp, zm, z2))
        ]

    def start(copies):
        for copy in copies:
            copy.start()

    small_in[0].wait()
    for copy in w_in:
        copy.wait()
    start(late_in)
    start(small_in[1:])
    project(0)
    hand_out(0)

    length = vf_ref[c]
    lane = lax.broadcasted_iota(jnp.int32, (BLOCK, 128), 1)
    row = lax.broadcasted_iota(jnp.int32, (BLOCK, 128), 0)

    def fill(slot, carry):
        block = me.seq(slot % 4, slot // 4)
        frame = 2 * block + row // TOK_FRAME
        bias = jnp.where((lane == 0) & (frame >= length), NEG, 0.0)
        mine = 0
        for i in range(4):
            mine = mine + (lane == 1 + i).astype(jnp.int32) * (
                me.seq(i, me.gq(i, g)) == block
            ).astype(jnp.int32)
        bias = jnp.where((mine > 0) & (row >= TOK_FRAME), NEG, bias)
        kx[slot, :, 256:384] = bias.astype(BF16)
        vt[slot, 128:DEPTH, :] = jnp.ones((DEPTH - 128, BLOCK), BF16)
        return carry

    lax.fori_loop(0, 16, fill, 0)
    kx[16, :, 0:256] = jnp.zeros((BLOCK, 256), BF16)
    kx[16, :, 256:384] = jnp.where(lane == 0, NEG, 0.0).astype(BF16)
    vt[16] = jnp.zeros((DEPTH, BLOCK), BF16)
    for i in range(4):
        on = (lane == 0) | ((lane == 1 + i) & (row % 256 < ROWS))
        qx[i, :, 128:256] = jnp.where(on, 1.0, 0.0).astype(BF16)

    tok_wait(0, 0, zm, 0)
    tok_send(0, 2, zm, 0)
    tok_wait(1, 0, zp, 1)
    tok_send(1, 2, zp, 1)
    ring_out(0)
    project(1)
    hand_out(1)
    tok_wait(0, 1, zm, 1)
    tok_wait(1, 1, zp, 0)
    project(2)
    hand_out(2)
    ring_out(1)
    relay(0)
    tok_wait(0, 2, z2, 0)
    tok_wait(1, 2, z2, 1)
    project(3)
    hand_out(3)
    late_in[0].wait()
    start([w1_copy(0, 0), w1_copy(1, 0), w1_copy(0, 1), w1_copy(1, 1)])
    ring_out(2)
    relay(1)
    ring_out(3)
    relay(2)
    for n in range(4):
        stage_in(3, qx, q_recv.at[n])

        @pl.when(flip == 1)
        def _():
            stage_in(1, qx, qs_recv.at[n])

    def turn(gg):
        def body(j, carry):
            vt[gg * 4 + j, 0:128, :] = kx[gg * 4 + j, :, 0:128].T
            return carry

        lax.fori_loop(0, 4, body, 0)

    w1_arrive(0, 0)
    w1_copy(0, 2).start()
    w1_arrive(1, 0)
    w1_copy(1, 2).start()
    turn(g)
    relay(3)
    for direction in (0, 1):
        for k in (1, 2):
            w1_arrive(direction, k)
    start(w2_own())
    start(d2d(0))
    for direction in (0, 1):
        if direction not in ONWARD:
            for n in range(4):
                stage_in(4, kx, gk_recv.at[direction, n])
    turn(gm)
    turn(gp)
    for n in range(4):
        stage_in(4, kx, r_recv.at[n])
    turn(g2)

    def slot_of(b, count):
        pad = b // count
        slot = (1 - c) * ((b % 4) * 4 + b // 4) + c * b
        return (1 - pad) * slot + pad * 16

    counts = [me.seq(i, me.gq(i, g)) + 1 for i in range(4)]
    first = [0]
    for count in counts:
        first.append(first[-1] + (count + 1) // 2)
    turns = first[4]

    def pick(at_i, choices):
        return sum(((at_i == k).astype(jnp.int32) * value for k, value in enumerate(choices)), 0)

    def unit(u):
        past = u // (2 * turns)
        u = u - past * (u - 2 * turns + 1)
        a, v = u // turns, u % turns
        i = sum(((v >= first[k]).astype(jnp.int32) for k in (1, 2, 3)), 0)
        j = v - pick(i, first[:4])
        count = pick(i, counts)
        return a, i, [
            (1 - past) * slot_of(2 * j + k, count) + past * 16 for k in (0, 1)
        ]

    def score(u):
        a, i, slots = unit(u)
        for k, slot in enumerate(slots):
            s0[k * BLOCK : (k + 1) * BLOCK, :] = lax.dot_general(
                kx[slot, :, 128:384], qx[i, pl.ds(al(a * 256, 256), 256), :], (((1,), (1,)), ((), ())),
                preferred_element_type=F32,
            )

    def soften(u):
        a, i, _ = unit(u)
        before = m_s[a * 4 + i, 0:1, :]
        peak = jnp.full((8, 256), -1e38, F32)
        for r in range(0, 2 * BLOCK, 128):
            peak = jnp.maximum(peak, jnp.max(s0[r : r + 128, :].reshape(16, 8, 256), axis=0))
        peak = jnp.maximum(before, jnp.max(peak, axis=0, keepdims=True))
        m_s[a * 4 + i, 0:1, :] = peak
        m_s[8, 0:1, :] = jnp.exp2(before - peak)
        for r in range(0, 2 * BLOCK, 128):
            s1[r : r + 128, :] = jnp.exp2(s0[r : r + 128, :] - peak).astype(BF16)

    def gather(u):
        a, i, slots = unit(u)
        out = acc[a * 4 + i] * m_s[8, 0:1, :]
        for k, slot in enumerate(slots):
            out = out + jnp.dot(vt[slot], s1[k * BLOCK : (k + 1) * BLOCK, :], preferred_element_type=F32)
        acc[a * 4 + i] = out

    def back(i, a):
        rows = pl.ds(a * 256, 256)
        return remote(
            o_stage.at[i, rows, :], mx.at[z, p, rows, :], o_send.at[i, a], o_recv.at[p, a],
            {"seq": me.seq(i, me.gq(i, g))},
        )

    def o_arrive(a):
        rows = pl.ds(a * 256, 256)
        for d in (1, 2, 3):
            h = (p + d) % 4
            arrive(mx.at[z, h, rows, :], o_recv.at[h, a])

        @pl.when(flip == 1)
        def _():
            arrive(mx.at[z, p, rows, :], o_recv.at[p, a])

    def mx_copy(a, direction, k):
        to = zp if direction == 0 else zm
        t, half = ((z, 0), (z, 1), (zm, 0))[k] if direction == 0 else ((z, 1), (z, 0), (zp, 1))[k]
        ref = mx.at[t, :, pl.ds(a * 256 + half * ROWS, ROWS), :]
        return remote(ref, ref, m_send.at[a, direction, k], m_recv.at[a, direction, k], {"tensor": to})

    def mx_arrive(a, direction, k):
        arrive(mx.at[z, :, pl.ds(0, ROWS), :], m_recv.at[a, direction, k])

    def mx_own(a):
        start([mx_copy(a, 0, 0), mx_copy(a, 1, 0), mx_copy(a, 0, 1), mx_copy(a, 1, 1)])

    def mx_relay(a):
        for direction in (0, 1):
            mx_arrive(a, direction, 0)
            mx_copy(a, direction, 2).start()

    def w2_onward():
        for direction in (0, 1):
            arrive(wo.at[pl.ds(0, 192), :], w2_recv.at[direction])
        start(w2_relay())
        start(d2d(1))
        start(d2d(2))

    def give_back(a):
        for i in range(4):
            rows = pl.ds(a * 256, 256)
            out = acc[a * 4 + i, 0:128, :] / acc[a * 4 + i, 128:129, :]
            o_stage[i, rows, :] = out.T.astype(BF16)
            stays = (1 - flip) * (p == i).astype(jnp.int32)

            @pl.when(stays == 0)
            def _():
                back(i, a).start()

            @pl.when(stays == 1)
            def _():
                mx[z, p, rows, :] = o_stage[i, rows, :]

    for k in range(8):
        m_s[k] = jnp.full((8, 256), -1e38, F32)
        acc[k] = jnp.zeros((DEPTH, 256), F32)
    def w2_last():
        for direction in (0, 1):
            arrive(wo.at[pl.ds(0, 96), :], w2r_recv.at[direction])
        start(d2d(3))

    score(0)
    soften(0)
    score(1)

    per = UNROLL
    half_way = (turns + per - 1) // per

    def turn_step(n, carry):
        @pl.when(n == half_way)
        def _():
            give_back(0)

        @pl.when(n == half_way + HOOKS[0] // per)
        def _():
            o_arrive(0)
            mx_own(0)

        pl.when(n == HOOKS[1] // per)(w2_onward)
        pl.when(n == HOOKS[2] // per)(w2_last)
        for k in range(per):
            gather(n * per + k)
            soften(n * per + k + 1)
            score(n * per + k + 2)
        return carry

    lax.fori_loop(0, (2 * turns + per - 1) // per, turn_step, 0)
    give_back(1)

    mx_relay(0)
    o_arrive(1)
    mx_own(1)
    for copy in small_in[1:]:
        copy.wait()
    for direction in (0, 1):
        for k in range(3):
            ref = tok.at[0, halves[0], :]
            remote(ref, ref, ts_sem.at[direction, k], ts_sem.at[direction, k], {"tensor": zp}).wait_send()

    def frame_rows(a):
        for direction in (0, 1):
            for k in (1, 2):
                mx_arrive(a, direction, k)

    def out_project(a):
        rows = pl.ds(a * 256, 256)

        def step(n, carry):
            cols = pl.ds(al(n * 512, 512), 512)
            lhs = jnp.concatenate([mx[t, h, rows, :] for t in range(4) for h in range(4)], axis=1)
            x = jnp.dot(lhs, wo[:, cols], preferred_element_type=F32)
            for k in (0, 1):
                t = a + 2 * k
                tok[t, :, cols] = (tok[t, :, cols].astype(F32) + x[k * ROWS : (k + 1) * ROWS]).astype(BF16)
            return carry

        lax.fori_loop(0, 4, step, 0)
        for k in (0, 1):
            norm_rows(tok.at[a + 2 * k], gain2_ref, nrm.at[pl.ds(k * ROWS, ROWS), :], ROWS)

    lo, hi = halves
    ways = ((zp, lo, hi), (zm, hi, lo))

    def mid_copy(direction, n):
        to, rows, _ = ways[direction]
        cols = pl.ds(n * 512, 512)
        return remote(
            part.at[z2, rows, cols], mid.at[direction, :, cols], rs_send.at[direction, n],
            mid_recv.at[direction, n], {"tensor": to},
        )

    def direct_copy(direction):
        to, _, rows = ways[direction]
        return remote(
            part.at[to, rows, :], fin.at[direction, rows, :], rs_send.at[direction, 4],
            fin_recv.at[direction, 0], {"tensor": to},
        )

    def sum_copy(direction, n):
        to, rows, _ = ways[direction]
        cols = pl.ds(n * 512, 512)
        return remote(
            part.at[to, rows, cols], fin.at[direction, rows, cols], rs_send.at[direction, 5 + n],
            fin_recv.at[direction, 1], {"tensor": to},
        )

    def up_down(a, between=lambda: None):
        def up_step(n, carry):
            cols = pl.ds(al(n * 512, 512), 512)
            x = jnp.dot(nrm[...], wu[:, cols], preferred_element_type=F32)
            up[:, cols] = gelu(x).astype(BF16)
            return carry

        lax.fori_loop(0, 4, up_step, 0)

        for n in range(4):
            cols = slice(n * 512, n * 512 + 512)
            x = jnp.dot(up[...], wd[:, cols], preferred_element_type=F32)
            for k in (0, 1):
                rows = x[k * ROWS : (k + 1) * ROWS]
                part[a + 2 * k, :, cols] = rows.astype(BF16)
                rows = jnp.sum(rows.reshape(16, 8, 512), axis=0)
                fs[k, :, cols] = fs[k, :, cols] + rows if a else rows
            if n == 3:
                between()

            @pl.when(z2 % 2 == a)
            def _():
                for direction in (0, 1):
                    mid_copy(direction, n).start()

    def rs_first(a):
        for t, direction in ((zp, 0), (zm, 1)):

            @pl.when(t % 2 == a)
            def _():
                direct_copy(direction).start()

    def rs_sums(a):
        @pl.when(zp % 2 == a)
        def _():
            for n in range(4):
                cols = slice(n * 512, n * 512 + 512)
                for direction, (t, half) in enumerate(((zp, 0), (zm, 64))):
                    arrive(mid.at[direction, :, pl.ds(n * 512, 512)], mid_recv.at[direction, n])
                    rows = slice(half, half + 64)
                    part[t, rows, cols] = (
                        part[t, rows, cols].astype(F32) + mid[direction, :, cols].astype(F32)
                    ).astype(BF16)
                    sum_copy(direction, n).start()

    frame_rows(0)
    arrive(wo.at[pl.ds(0, 768), :], d_recv)
    out_project(0)
    mx_relay(1)
    late_in[1].wait()
    late_in[2].wait()
    up_down(0)
    rs_first(0)
    frame_rows(1)
    out_project(1)
    def residual(i, total):
        at = pl.ds(al(i * 16, 16), 16)
        return total + jnp.sum(tok[z, at, :].astype(F32).reshape(2, 8, D), axis=0)

    fs[2] = lax.fori_loop(0, 8, residual, jnp.zeros((8, D), F32))

    def sums_out():
        for k in (0, 1):
            mine = (z // 2 == k).astype(F32)
            zs[z, k : k + 1, :] = jnp.sum(fs[k] + fs[2] * mine, axis=0, keepdims=True)
        for d in (1, 2, 3):
            send(zs.at[z], zs.at[z], z_send.at[d - 1], z_recv.at[z], {"tensor": (z + d) % 4})

    rs_sums(0)
    up_down(1, sums_out)
    rs_first(1)
    for d in (1, 2, 3):
        t = (z + d) % 4
        arrive(zs.at[t], z_recv.at[t])
    means[s] = (zs[0] + zs[1] + zs[2] + zs[3]) * (1.0 / TOK_FRAME)
    for d in range(1, 16):
        send(means.at[s], means.at[s], s_send.at[d - 1], s_recv.at[s], {"seq": (s + d) % 16})
    rs_sums(1)
    for d in range(1, 16):
        t = (s + d) % 16
        arrive(means.at[t], s_recv.at[t])
    frame = 2 * lax.broadcasted_iota(jnp.int32, (16, 2, 128), 0) + lax.broadcasted_iota(jnp.int32, (16, 2, 128), 1)
    pg, pb, vw = small[2:3, :], small[3:4, :], small[4:5, :]

    def scan(i, state):
        m = means[i]
        gate = jax.nn.sigmoid(m * pg + pb)
        source = (1.0 - gate) * m
        for k in (0, 1):
            new = gate[k : k + 1] * state + source[k : k + 1]
            state = jnp.where(2 * i + k < length, new, state)
            states[i, k : k + 1, :] = state
        return state

    lax.fori_loop(0, 16, scan, jnp.zeros((1, D), F32))
    total = jnp.sum(states[...] * vw.reshape(1, 1, D), axis=-1, keepdims=True)
    values = jnp.where(frame < length, jnp.broadcast_to(total, (16, 2, 128)), 0.0)
    vals[0] = values
    send(vals.at[0], vals.at[1], v_sem.at[0], v_sem.at[1], {"dp": 1 - c})

    for direction in (0, 1):
        for k in (0, 1):
            arrive(fin.at[direction, lo, :], fin_recv.at[direction, k])

    def output(i, carry):
        at = pl.ds(al(i * 16, 16), 16)
        total = part[z, at, :].astype(F32) + fin[0, at, :].astype(F32) + fin[1, at, :].astype(F32)
        hid_ref[at, :] = (tok[z, at, :].astype(F32) + total).astype(BF16)
        return carry

    lax.fori_loop(0, 8, output, 0)

    arrive(vals.at[1], v_sem.at[1])

    def gaps(v, n):
        valid = frame < n
        reward = jnp.sum(jnp.where(frame == n - 1, v, 0.0), axis=(0, 1), keepdims=True)
        return valid, jnp.where(valid, reward - v, 0.0)

    other = vf_ref[1 - c]
    count = (length + other).astype(F32)
    valid, gap = gaps(values, length)
    valid_o, gap_o = gaps(vals[1], other)
    add = lambda a: jnp.sum(a, axis=(0, 1), keepdims=True)
    mean = (add(gap) + add(gap_o)) / count
    centered = jnp.where(valid, gap - mean, 0.0)
    centered_o = jnp.where(valid_o, gap_o - mean, 0.0)
    variance = (add(centered * centered) + add(centered_o * centered_o)) / count
    adv = jnp.where(valid, centered * lax.rsqrt(variance + 1e-5), 0.0)
    lane = lax.broadcasted_iota(jnp.int32, (1, 128), 1)

    def own_pair(a):
        first = jnp.sum(jnp.where(frame == 2 * s, a, 0.0), axis=(0, 1))
        second = jnp.sum(jnp.where(frame == 2 * s + 1, a, 0.0), axis=(0, 1))
        return jnp.where(lane == 0, first.reshape(1, 128), second.reshape(1, 128))[:, 0:2]

    fv_ref[...] = own_pair(values)
    adv_ref[...] = own_pair(adv)
    @pl.when(flip == 1)
    def _():
        for n in range(4):
            for half, (src, _, dst) in enumerate(pieces(n)):
                remote(
                    stage.at[n, p, src, third], qx.at[p, dst, lanes],
                    a_send.at[n, 3, 0, half], qs_recv.at[n], {"seq": me.seq(p, 3 - g)},
                ).wait_send()

    for i in range(4):
        stays = (1 - flip) * (p == i).astype(jnp.int32)

        @pl.when(stays == 0)
        def _():
            for a in (0, 1):
                back(i, a).wait_send()

    rest = [w1_copy(d, k) for d in (0, 1) for k in range(3)]
    rest += w2_own() + w2_relay() + [copy for n in range(4) for copy in d2d(n)]
    rest += [mx_copy(a, d, k) for a in (0, 1) for d in (0, 1) for k in range(3)]
    for d in (0, 1):
        rest += [direct_copy(d)] + [copy(d, n) for copy in (mid_copy, sum_copy) for n in range(4)]
    for copy in rest + sends:
        copy.wait_send()


def local(
    tokens, attn_gain, w_qkv, w_out, mlp_gain, w_up, w_down, pool_gain, pool_bias, value_weight, valid_frames
):
    vmem = pltpu.VMEM
    dma = pltpu.SemaphoreType.DMA
    inside = pl.BlockSpec(memory_space=pltpu.VMEM)
    outside = pl.BlockSpec(memory_space=pl.ANY)
    hidden, values, advantages = pl.pallas_call(
        layer_kernel,
        out_shape=(
            jax.ShapeDtypeStruct((ROWS, D), BF16),
            jax.ShapeDtypeStruct((1, 2), F32),
            jax.ShapeDtypeStruct((1, 2), F32),
        ),
        in_specs=[pl.BlockSpec(memory_space=pltpu.SMEM)] + [outside] * 10,
        out_specs=(inside,) * 3,
        scratch_shapes=[
            vmem((4, ROWS, D), BF16),
            vmem((3, D, BLOCK), BF16),
            vmem((8, D), F32),
            vmem((ROWS, D), BF16),
            vmem((4, 4, ROWS, 384), BF16),
            vmem((4, BLOCK, 256), BF16),
            vmem((17, BLOCK, 384), BF16),
            vmem((17, DEPTH, BLOCK), BF16),
            vmem((9, 8, 256), F32),
            vmem((8, DEPTH, 256), F32),
            vmem((2 * BLOCK, 256), F32),
            vmem((2 * BLOCK, 256), BF16),
            vmem((4, BLOCK, HEAD_DIM), BF16),
            vmem((4, 4, BLOCK, HEAD_DIM), BF16),
            vmem((D, D), BF16),
            vmem((D, D), BF16),
            vmem((D, D), BF16),
            vmem((4, ROWS, D), BF16),
            vmem((2, 64, D), BF16),
            vmem((2, ROWS, D), BF16),
            vmem((2 * ROWS, D), BF16),
            vmem((2 * ROWS, D), BF16),
            vmem((3, 8, D), F32),
            vmem((4, 2, D), F32),
            vmem((16, 2, D), F32),
            vmem((16, 2, D), F32),
            vmem((2, 16, 2, 128), F32),
            dma((6,)),
            dma((6,)),
            dma((2, 3)),
            dma((2, 3)),
            dma((4, 4, 2, 2)),
            dma((4,)),
            dma((4,)),
            dma((4,)),
            dma((2, 4, 4)),
            dma((2, 4)),
            dma((4,)),
            dma((4, 2)),
            dma((4, 2)),
            dma((2, 2, 3)),
            dma((2, 2, 3)),
            dma((2, 3)),
            dma((2, 3)),
            dma((2, 5)),
            dma((2,)),
            dma((2,)),
            dma((4, 3)),
            dma,
            dma((2, 9)),
            dma((2, 4)),
            dma((2, 2)),
            dma((3,)),
            dma((4,)),
            dma((15,)),
            dma((16,)),
            dma((2,)),
        ],
        compiler_params=pltpu.CompilerParams(
            collective_id=0, has_side_effects=True, vmem_limit_bytes=63 * 2**20
        ),
        cost_estimate=pl.CostEstimate(flops=4 * 10**10, bytes_accessed=4 * 10**7, transcendentals=10**7),
    )(
        valid_frames, tokens[0], w_qkv, w_out, w_up, w_down,
        *(v.reshape(1, D) for v in (attn_gain, mlp_gain, pool_gain, pool_bias, value_weight)),
    )
    return hidden[None], values, advantages


def solution(mesh):
    in_specs = (
        P("dp", ("seq", "tensor"), None),
        P(),
        P(None, None, "tensor"),
        P("tensor", None),
        P(),
        P(None, "tensor"),
        P("tensor", None),
        P(),
        P(),
        P(),
        P(),
    )
    out_specs = (P("dp", ("seq", "tensor"), None), P("dp", "seq"), P("dp", "seq"))
    return jax.shard_map(local, mesh=mesh, in_specs=in_specs, out_specs=out_specs, check_vma=False)
```

```python
import functools
import math

import jax
import jax.numpy as jnp
from jax import lax
from jax.experimental import pallas as pl
from jax.experimental.pallas import tpu as pltpu
from jax.sharding import PartitionSpec as P

HEAD_DIM = 128
TOK_FRAME = 256
ROWS = 128
HALF = 64
BLOCK = 512
D = 2048
DEPTH = 144
BF16 = jnp.bfloat16
F32 = jnp.float32
MESH = pl.DeviceIdType.MESH
QSCALE = math.log2(math.e) / math.sqrt(HEAD_DIM)
NEG = -1e30
ONWARD = (0, 1)
HOOKS = (12, 20)
UNROLL = 4


def remote(src, dst, send_sem, recv_sem, where):
    return pltpu.make_async_remote_copy(
        src_ref=src, dst_ref=dst, send_sem=send_sem, recv_sem=recv_sem,
        device_id=where, device_id_type=MESH,
    )


def al(i, m):
    return pl.multiple_of(i, m)


class Place:
    def __init__(self):
        self.c = lax.axis_index("dp")
        s = lax.axis_index("seq")
        self.s = s
        self.z = lax.axis_index("tensor")
        y, x = s // 4, s % 4
        self.p = y * (1 - self.c) + x * self.c
        self.g = x * (1 - self.c) + y * self.c

    def seq(self, p, g):
        return (p * 4 + g) * (1 - self.c) + (g * 4 + p) * self.c

    def flip(self, p):
        return (1 - self.c) * (1 - p % 2) + self.c * (p // 2)

    def gq(self, p, g):
        return g + self.flip(p) * (3 - 2 * g)


def norm_rows(src, gain_ref, dst, rows):
    def body(i, carry):
        at = pl.ds(al(i * 16, 16), 16)
        x = src[at, :].astype(F32)
        square = jnp.mean(x * x, axis=-1, keepdims=True)
        dst[at, :] = (x * lax.rsqrt(square + 1e-5) * gain_ref[...]).astype(BF16)
        return carry

    lax.fori_loop(0, rows // 16, body, 0, unroll=True)


def gelu(x):
    return 0.5 * x * (1.0 + jnp.tanh(math.sqrt(2.0 / math.pi) * (x + 0.044715 * (x * x * x))))


def layer_kernel(
    vf_ref, tok_hbm, w_hbm, wo_hbm, wu_hbm, wd_hbm, g1_hbm, g2_hbm, pg_hbm, pb_hbm, vw_hbm,
    hid_ref, fv_ref, adv_ref,
    tok, w, small, normed, stage, qx, kx, vt, m_s, acc, s0, s1, o_stage, mx, wo, wu, wd,
    part, mid, fin, nrm, up, fs, zs, means, states, vals,
    tl_sem, w_sem, ts_sem, tr_sem, a_send, q_recv, k_recv, qs_recv,
    g_send, gk_recv, r_recv, o_send, o_recv, m_send, m_recv, w1_send, w1_recv, w2_send, w2_recv, w2r_recv,
    d_send, d_recv, rs_send, mid_recv, fin_recv, z_send, z_recv, s_send, s_recv, v_sem,
):
    me = Place()
    c, s, z, p, g = me.c, me.s, me.z, me.p, me.g
    zp, zm, z2 = (z + 1) % 4, (z + 3) % 4, (z + 2) % 4
    gp, gm, g2 = (g + 1) % 4, (g + 3) % 4, (g + 2) % 4
    flip = me.flip(p)
    gain_ref, gain2_ref = small.at[0:1, :], small.at[1:2, :]

    own_in = pltpu.make_async_copy(tok_hbm, tok.at[z], tl_sem.at[0])
    own_in.start()
    small_in = [
        pltpu.make_async_copy(src, small.at[k : k + 1, :], tl_sem.at[1 + k])
        for k, src in enumerate((g1_hbm, g2_hbm, pg_hbm, pb_hbm, vw_hbm))
    ]
    small_in[0].start()
    w_in = [pltpu.make_async_copy(w_hbm.at[k], w.at[k], w_sem.at[k]) for k in range(3)]
    for copy in w_in:
        copy.start()
    late_in = [
        pltpu.make_async_copy(wo_hbm, wo.at[pl.ds(al(z * BLOCK, BLOCK), BLOCK), :], w_sem.at[3]),
        pltpu.make_async_copy(wu_hbm, wu, w_sem.at[4]),
        pltpu.make_async_copy(wd_hbm, wd, w_sem.at[5]),
    ]

    barrier = pltpu.get_barrier_semaphore()
    for t in (zp, zm, z2):
        pl.semaphore_signal(barrier, inc=1, device_id={"tensor": t}, device_id_type=MESH)
    for d in range(1, 16):
        pl.semaphore_signal(barrier, inc=1, device_id={"seq": (s + d) % 16}, device_id_type=MESH)
    pl.semaphore_signal(barrier, inc=1, device_id={"dp": 1 - c}, device_id_type=MESH)
    own_in.wait()
    pl.semaphore_wait(barrier, 19)

    halves = (pl.ds(0, HALF), pl.ds(HALF, HALF))
    sends = []

    def send(src, dst, send_sem, recv_sem, to):
        copy = remote(src, dst, send_sem, recv_sem, to)
        copy.start()
        sends.append(copy)

    def start_only(src, dst, send_sem, recv_sem, to):
        remote(src, dst, send_sem, recv_sem, to).start()

    def arrive(ref, sem):
        remote(ref, ref, sem, sem, {"tensor": zp}).wait_recv()

    def tok_send(direction, k, t, half):
        ref = tok.at[t, halves[half], :]
        start_only(ref, ref, ts_sem.at[direction, k], tr_sem.at[direction, k], {"tensor": zp if direction == 0 else zm})

    def tok_wait(direction, k, t, half):
        arrive(tok.at[t, halves[half], :], tr_sem.at[direction, k])

    tok_send(0, 0, z, 0)
    tok_send(1, 0, z, 1)
    tok_send(0, 1, z, 1)
    tok_send(1, 1, z, 0)

    stages = (((z, 0), (z, 1)), ((zm, 0), (zp, 1)), ((zm, 1), (zp, 0)), ((z2, 0), (z2, 1)))

    def rows_of(piece):
        t, half = piece
        return pl.ds(al(t * ROWS + half * HALF, HALF), HALF)

    def project(n):
        for k, (t, half) in enumerate(stages[n]):
            norm_rows(tok.at[t, halves[half], :], gain_ref, normed.at[halves[k], :], HALF)
        for k in (1, 2, 0):
            for pair in range(2):
                out = jnp.dot(
                    normed[...], w[k, :, pair * 256 : pair * 256 + 256], preferred_element_type=F32
                )
                if k == 0:
                    out = out * QSCALE
                out = out.astype(BF16)
                at = slice((2 - k) * 128, (3 - k) * 128)
                stage[n, 2 * pair, :, at] = out[:, :128]
                stage[n, 2 * pair + 1, :, at] = out[:, 128:]

    def query_rows(piece, count):
        t, half = piece
        return pl.ds(al((t % 2) * 256 + (t // 2) * ROWS + half * HALF, HALF), count)

    both = pl.ds(0, 256)
    third = pl.ds(256, 128)
    lanes = pl.ds(0, HEAD_DIM)

    def pieces(n):
        if n in (0, 3):
            piece = stages[n][0]
            return ((pl.ds(0, ROWS), pl.ds(al(piece[0] * ROWS, ROWS), ROWS), query_rows(piece, ROWS)),)
        return tuple((halves[k], rows_of(piece), query_rows(piece, HALF)) for k, piece in enumerate(stages[n]))

    def hand_out(n):
        for k, (buf, sem, part) in enumerate(((kx, k_recv, both), (qx, q_recv, third))):
            for d in (2, 1, 3):
                h = (p + d) % 4
                to = {"seq": me.seq(h, me.gq(p, g) if k else g)}
                slot = p if k else g * 4 + p
                for half, (src, dst, dst_q) in enumerate(pieces(n)):
                    send(
                        stage.at[n, h, src, part], buf.at[slot, dst_q if k else dst, lanes if k else both],
                        a_send.at[n, d - 1, k, half], sem.at[n], to,
                    )
        for src, dst, _ in pieces(n):
            kx[g * 4 + p, dst, 0:256] = stage[n, p, src, 0:256]

        @pl.when(flip == 1)
        def _():
            for half, (src, _, dst) in enumerate(pieces(n)):
                remote(
                    stage.at[n, p, src, third], qx.at[p, dst, lanes],
                    a_send.at[n, 3, 0, half], qs_recv.at[n], {"seq": me.seq(p, 3 - g)},
                ).start()

        @pl.when(flip == 0)
        def _():
            for src, _, dst in pieces(n):
                qx[p, dst, 0:128] = stage[n, p, src, 256:384]

    def stage_in(count, buf, sem):
        arrive(buf.at[pl.ds(0, count), pl.ds(0, ROWS), lanes if buf is qx else both], sem)

    def ring_out(n):
        stage_in(3, kx, k_recv.at[n])
        for direction in (0, 1):
            to = {"seq": me.seq(p, gp if direction == 0 else gm)}
            for half, (_, dst, _) in enumerate(pieces(n)):
                ref = kx.at[pl.ds(g * 4, 4), dst, both]
                send(ref, ref, g_send.at[direction, n, half], gk_recv.at[direction, n], to)

    def relay(n):
        for direction in sorted(set(ONWARD)):
            stage_in(4, kx, gk_recv.at[direction, n])
            source, to = (gm, gp) if direction == 0 else (gp, gm)
            if ONWARD[0] == ONWARD[1]:
                runs = pieces(n)
            else:
                runs = ((0, rows_of(stages[n][direction]), 0),)
            for half, (_, dst, _) in enumerate(runs):
                ref = kx.at[pl.ds(source * 4, 4), dst, both]
                send(ref, ref, g_send.at[direction, n, 2 + half], r_recv.at[n], {"seq": me.seq(p, to)})

    def wo_rows(t, k, first, count):
        return wo.at[pl.ds(al(t * BLOCK + c * 256 + k * 64 + first, 32), count), :]

    def w1_copy(direction, k):
        to = zp if direction == 0 else zm
        t, first = ((z, 0), (z, 32), (zm, 0))[k] if direction == 0 else ((z, 32), (z, 0), (zp, 32))[k]
        ref = wo_rows(t, g, first, 32)
        return remote(ref, ref, w1_send.at[direction, k], w1_recv.at[direction, k], {"tensor": to})

    def w1_arrive(direction, k):
        arrive(wo.at[pl.ds(0, 32), :], w1_recv.at[direction, k])

    def w2_own():
        copies = []
        for direction in (0, 1):
            to = {"seq": me.seq(p, gp if direction == 0 else gm)}
            for k, t in enumerate((zp, zm, z2)):
                ref = wo_rows(t, g, 0, 64)
                copies.append(remote(ref, ref, w2_send.at[direction, k], w2_recv.at[direction], to))
        return copies

    def w2_relay():
        copies = []
        for direction in (0, 1):
            source, to = (gm, gp) if direction == 0 else (gp, gm)
            for k, ref in enumerate(
                (wo_rows(zm if direction else zp, source, 0, 64), wo_rows(z2, source, 32 * direction, 32))
            ):
                copies.append(
                    remote(ref, ref, w2_send.at[direction, 3 + k], w2r_recv.at[direction], {"seq": me.seq(p, to)})
                )
        return copies

    def d2d(n):
        k = (g, gm, gp, g2)[n]
        return [
            remote(ref, ref, d_send.at[n, i], d_recv, {"dp": 1 - c})
            for i, ref in enumerate(wo_rows(t, k, 0, 64) for t in (zp, zm, z2))
        ]

    def start(copies):
        for copy in copies:
            copy.start()

    small_in[0].wait()
    for copy in w_in:
        copy.wait()
    start(late_in)
    start(small_in[1:])
    project(0)
    hand_out(0)

    length = vf_ref[c]
    lane = lax.broadcasted_iota(jnp.int32, (BLOCK, 128), 1)
    row = lax.broadcasted_iota(jnp.int32, (BLOCK, 128), 0)

    def fill(slot, carry):
        block = me.seq(slot % 4, slot // 4)
        frame = 2 * block + row // TOK_FRAME
        bias = jnp.where((lane == 0) & (frame >= length), NEG, 0.0)
        mine = 0
        for i in range(4):
            mine = mine + (lane == 1 + i).astype(jnp.int32) * (
                me.seq(i, me.gq(i, g)) == block
            ).astype(jnp.int32)
        bias = jnp.where((mine > 0) & (row >= TOK_FRAME), NEG, bias)
        kx[slot, :, 256:384] = bias.astype(BF16)
        vt[slot, 128:DEPTH, :] = jnp.ones((DEPTH - 128, BLOCK), BF16)
        return carry

    lax.fori_loop(0, 16, fill, 0)
    kx[16, :, 0:256] = jnp.zeros((BLOCK, 256), BF16)
    kx[16, :, 256:384] = jnp.where(lane == 0, NEG, 0.0).astype(BF16)
    vt[16] = jnp.zeros((DEPTH, BLOCK), BF16)
    for i in range(4):
        on = (lane == 0) | ((lane == 1 + i) & (row % 256 < ROWS))
        qx[i, :, 128:256] = jnp.where(on, 1.0, 0.0).astype(BF16)

    tok_wait(0, 0, zm, 0)
    tok_send(0, 2, zm, 0)
    tok_wait(1, 0, zp, 1)
    tok_send(1, 2, zp, 1)
    ring_out(0)
    project(1)
    hand_out(1)
    tok_wait(0, 1, zm, 1)
    tok_wait(1, 1, zp, 0)
    project(2)
    hand_out(2)
    ring_out(1)
    relay(0)
    tok_wait(0, 2, z2, 0)
    tok_wait(1, 2, z2, 1)
    project(3)
    hand_out(3)
    late_in[0].wait()
    start([w1_copy(0, 0), w1_copy(1, 0), w1_copy(0, 1), w1_copy(1, 1)])
    ring_out(2)
    relay(1)
    ring_out(3)
    relay(2)
    for n in range(4):
        stage_in(3, qx, q_recv.at[n])

        @pl.when(flip == 1)
        def _():
            stage_in(1, qx, qs_recv.at[n])

    def turn(gg):
        def body(j, carry):
            vt[gg * 4 + j, 0:128, :] = kx[gg * 4 + j, :, 0:128].T
            return carry

        lax.fori_loop(0, 4, body, 0)

    w1_arrive(0, 0)
    w1_copy(0, 2).start()
    w1_arrive(1, 0)
    w1_copy(1, 2).start()
    turn(g)
    relay(3)
    for direction in (0, 1):
        for k in (1, 2):
            w1_arrive(direction, k)
    start(w2_own())
    start(d2d(0))
    for direction in (0, 1):
        if direction not in ONWARD:
            for n in range(4):
                stage_in(4, kx, gk_recv.at[direction, n])
    turn(gm)
    turn(gp)
    for n in range(4):
        stage_in(4, kx, r_recv.at[n])
    turn(g2)

    def slot_of(b, count):
        pad = (b >= count).astype(jnp.int32)
        slot = (1 - c) * (lax.rem(b, 4) * 4 + lax.div(b, 4)) + c * b
        return slot + pad * (16 - slot)

    counts = [me.seq(i, me.gq(i, g)) + 1 for i in range(4)]
    first = [0]
    for count in counts:
        first.append(first[-1] + (count + 1) // 2)
    turns = first[4]

    def pick(at_i, choices):
        return sum(((at_i == k).astype(jnp.int32) * value for k, value in enumerate(choices)), 0)

    def unit(u):
        past = (u >= 2 * turns).astype(jnp.int32)
        u = u - past * (u - 2 * turns + 1)
        a = (u >= turns).astype(jnp.int32)
        v = u - a * turns
        i = sum(((v >= first[k]).astype(jnp.int32) for k in (1, 2, 3)), 0)
        j = v - pick(i, first[:4])
        count = pick(i, counts)
        slots = tuple(slot + past * (16 - slot) for slot in (slot_of(2 * j, count), slot_of(2 * j + 1, count)))
        return a, i, *slots

    def score(now):
        a, i, *slots = now
        for k, slot in enumerate(slots):
            s0[k * BLOCK : (k + 1) * BLOCK, :] = lax.dot_general(
                kx[slot, :, 128:384], qx[i, pl.ds(al(a * 256, 256), 256), :], (((1,), (1,)), ((), ())),
                preferred_element_type=F32,
            )

    def soften(now):
        a, i, *_ = now
        before = m_s[a * 4 + i, 0:1, :]
        peak = jnp.full((8, 256), -1e38, F32)
        for r in range(0, 2 * BLOCK, 128):
            peak = jnp.maximum(peak, jnp.max(s0[r : r + 128, :].reshape(16, 8, 256), axis=0))
        peak = jnp.maximum(before, jnp.max(peak, axis=0, keepdims=True))
        m_s[a * 4 + i, 0:1, :] = peak
        m_s[8, 0:1, :] = jnp.exp2(before - peak)
        for r in range(0, 2 * BLOCK, 128):
            s1[r : r + 128, :] = jnp.exp2(s0[r : r + 128, :] - peak).astype(BF16)

    def gather(now):
        a, i, *slots = now
        out = acc[a * 4 + i] * m_s[8, 0:1, :]
        for k, slot in enumerate(slots):
            out = out + jnp.dot(vt[slot], s1[k * BLOCK : (k + 1) * BLOCK, :], preferred_element_type=F32)
        acc[a * 4 + i] = out

    def back(i, a):
        rows = pl.ds(a * 256, 256)
        return remote(
            o_stage.at[i, rows, :], mx.at[z, p, rows, :], o_send.at[i, a], o_recv.at[p, a],
            {"seq": me.seq(i, me.gq(i, g))},
        )

    def o_arrive(a):
        rows = pl.ds(a * 256, 256)
        for d in (1, 2, 3):
            h = (p + d) % 4
            arrive(mx.at[z, h, rows, :], o_recv.at[h, a])

        @pl.when(flip == 1)
        def _():
            arrive(mx.at[z, p, rows, :], o_recv.at[p, a])

    def mx_copy(a, direction, k):
        to = zp if direction == 0 else zm
        t, half = ((z, 0), (z, 1), (zm, 0))[k] if direction == 0 else ((z, 1), (z, 0), (zp, 1))[k]
        ref = mx.at[t, :, pl.ds(a * 256 + half * ROWS, ROWS), :]
        return remote(ref, ref, m_send.at[a, direction, k], m_recv.at[a, direction, k], {"tensor": to})

    def mx_arrive(a, direction, k):
        arrive(mx.at[z, :, pl.ds(0, ROWS), :], m_recv.at[a, direction, k])

    def mx_own(a):
        start([mx_copy(a, 0, 0), mx_copy(a, 1, 0), mx_copy(a, 0, 1), mx_copy(a, 1, 1)])

    def mx_relay(a):
        for direction in (0, 1):
            mx_arrive(a, direction, 0)
            mx_copy(a, direction, 2).start()

    def w2_onward():
        for direction in (0, 1):
            arrive(wo.at[pl.ds(0, 192), :], w2_recv.at[direction])
        start(w2_relay())
        start(d2d(1))
        start(d2d(2))

    def give_back(a):
        for i in range(4):
            rows = pl.ds(a * 256, 256)
            out = acc[a * 4 + i, 0:128, :] / acc[a * 4 + i, 128:129, :]
            o_stage[i, rows, :] = out.T.astype(BF16)
            stays = (1 - flip) * (p == i).astype(jnp.int32)

            @pl.when(stays == 0)
            def _():
                back(i, a).start()

            @pl.when(stays == 1)
            def _():
                mx[z, p, rows, :] = o_stage[i, rows, :]

    for k in range(8):
        m_s[k] = jnp.full((8, 256), -1e38, F32)
        acc[k] = jnp.zeros((DEPTH, 256), F32)
    def w2_last():
        for direction in (0, 1):
            arrive(wo.at[pl.ds(0, 96), :], w2r_recv.at[direction])
        start(d2d(3))

    score(unit(0))
    soften(unit(0))
    score(unit(1))

    per = UNROLL
    half_way = (turns + per - 1) // per

    def turn_step(n, carry):
        @pl.when(n == half_way)
        def _():
            give_back(0)

        @pl.when(n == half_way + HOOKS[0] // per)
        def _():
            o_arrive(0)
            mx_own(0)

        pl.when(n == HOOKS[1] // per)(w2_onward)
        units = [*carry, *(unit((n + 1) * per + k) for k in (2, *range(3, per + 2)))]
        for k in range(per):
            gather(carry[k])
            soften(carry[k + 1])
            score(carry[k + 2])
        return tuple(units[per:])

    lax.fori_loop(0, (2 * turns + per - 1) // per, turn_step, tuple(unit(k) for k in range(per + 2)))
    give_back(1)

    mx_relay(0)
    w2_last()
    o_arrive(1)
    mx_own(1)
    for copy in small_in[1:]:
        copy.wait()
    for direction in (0, 1):
        for k in range(3):
            ref = tok.at[0, halves[0], :]
            remote(ref, ref, ts_sem.at[direction, k], ts_sem.at[direction, k], {"tensor": zp}).wait_send()

    def frame_rows(a):
        for direction in (0, 1):
            for k in (1, 2):
                mx_arrive(a, direction, k)

    def out_project(a):
        rows = pl.ds(a * 256, 256)

        for n in range(4):
            cols = slice(n * 512, n * 512 + 512)
            lhs = jnp.concatenate([mx[t, h, rows, :] for t in range(4) for h in range(4)], axis=1)
            x = jnp.dot(lhs, wo[:, cols], preferred_element_type=F32)
            for k in (0, 1):
                t = a + 2 * k
                tok[t, :, cols] = (tok[t, :, cols].astype(F32) + x[k * ROWS : (k + 1) * ROWS]).astype(BF16)
        for k in (0, 1):
            norm_rows(tok.at[a + 2 * k], gain2_ref, nrm.at[pl.ds(k * ROWS, ROWS), :], ROWS)

    lo, hi = halves
    ways = ((zp, lo, hi), (zm, hi, lo))

    def mid_copy(direction, n):
        to, rows, _ = ways[direction]
        cols = pl.ds(n * 512, 512)
        return remote(
            part.at[z2, rows, cols], mid.at[direction, :, cols], rs_send.at[direction, n],
            mid_recv.at[direction, n], {"tensor": to},
        )

    def direct_copy(direction):
        to, _, rows = ways[direction]
        return remote(
            part.at[to, rows, :], fin.at[direction, rows, :], rs_send.at[direction, 4],
            fin_recv.at[direction, 0], {"tensor": to},
        )

    def sum_copy(direction, n):
        to, rows, _ = ways[direction]
        cols = pl.ds(n * 512, 512)
        return remote(
            part.at[to, rows, cols], fin.at[direction, rows, cols], rs_send.at[direction, 5 + n],
            fin_recv.at[direction, 1], {"tensor": to},
        )

    def up_down(a, between=lambda: None):
        for n in range(4):
            cols = slice(n * 512, n * 512 + 512)
            x = jnp.dot(nrm[...], wu[:, cols], preferred_element_type=F32)
            up[:, cols] = gelu(x).astype(BF16)

        for n in range(4):
            cols = slice(n * 512, n * 512 + 512)
            x = jnp.dot(up[...], wd[:, cols], preferred_element_type=F32)
            for k in (0, 1):
                rows = x[k * ROWS : (k + 1) * ROWS]
                part[a + 2 * k, :, cols] = rows.astype(BF16)
                rows = jnp.sum(rows.reshape(16, 8, 512), axis=0)
                fs[k, :, cols] = fs[k, :, cols] + rows if a else rows
            if n == 3:
                between()
            if a == 1 and n < 3:
                continue

            @pl.when(z2 % 2 == a)
            def _():
                for m in range(4) if a else (n,):
                    for direction in (0, 1):
                        mid_copy(direction, m).start()

    def rs_first(a):
        for t, direction in ((zp, 0), (zm, 1)):

            @pl.when(t % 2 == a)
            def _():
                direct_copy(direction).start()

    def rs_sums(a):
        @pl.when(zp % 2 == a)
        def _():
            for n in range(4):
                cols = slice(n * 512, n * 512 + 512)
                for direction, (t, half) in enumerate(((zp, 0), (zm, 64))):
                    arrive(mid.at[direction, :, pl.ds(n * 512, 512)], mid_recv.at[direction, n])
                    rows = slice(half, half + 64)
                    part[t, rows, cols] = (
                        part[t, rows, cols].astype(F32) + mid[direction, :, cols].astype(F32)
                    ).astype(BF16)
                    sum_copy(direction, n).start()

    frame_rows(0)
    arrive(wo.at[pl.ds(0, 768), :], d_recv)
    out_project(0)
    mx_relay(1)
    late_in[1].wait()
    late_in[2].wait()
    up_down(0)
    rs_first(0)
    frame_rows(1)
    out_project(1)
    def residual(i, total):
        at = pl.ds(al(i * 16, 16), 16)
        return total + jnp.sum(tok[z, at, :].astype(F32).reshape(2, 8, D), axis=0)

    fs[2] = lax.fori_loop(0, 8, residual, jnp.zeros((8, D), F32))

    def sums_out():
        for k in (0, 1):
            mine = (z // 2 == k).astype(F32)
            zs[z, k : k + 1, :] = jnp.sum(fs[k] + fs[2] * mine, axis=0, keepdims=True)
        for d in (1, 2, 3):
            send(zs.at[z], zs.at[z], z_send.at[d - 1], z_recv.at[z], {"tensor": (z + d) % 4})

    rs_sums(0)
    up_down(1, sums_out)
    rs_first(1)
    for d in (1, 2, 3):
        t = (z + d) % 4
        arrive(zs.at[t], z_recv.at[t])
    means[s] = (zs[0] + zs[1] + zs[2] + zs[3]) * (1.0 / TOK_FRAME)
    for d in range(1, 16):
        send(means.at[s], means.at[s], s_send.at[d - 1], s_recv.at[s], {"seq": (s + d) % 16})
    rs_sums(1)
    for d in range(1, 16):
        t = (s + d) % 16
        arrive(means.at[t], s_recv.at[t])
    frame = 2 * lax.broadcasted_iota(jnp.int32, (16, 2, 128), 0) + lax.broadcasted_iota(jnp.int32, (16, 2, 128), 1)
    pg, pb, vw = small[2:3, :], small[3:4, :], small[4:5, :]

    def scan(i, state):
        m = means[i]
        gate = jax.nn.sigmoid(m * pg + pb)
        source = (1.0 - gate) * m
        for k in (0, 1):
            new = gate[k : k + 1] * state + source[k : k + 1]
            state = jnp.where(2 * i + k < length, new, state)
            states[i, k : k + 1, :] = state
        return state

    lax.fori_loop(0, 16, scan, jnp.zeros((1, D), F32))
    total = jnp.sum(states[...] * vw.reshape(1, 1, D), axis=-1, keepdims=True)
    values = jnp.where(frame < length, jnp.broadcast_to(total, (16, 2, 128)), 0.0)
    vals[0] = values
    send(vals.at[0], vals.at[1], v_sem.at[0], v_sem.at[1], {"dp": 1 - c})

    for direction in (0, 1):
        for k in (0, 1):
            arrive(fin.at[direction, lo, :], fin_recv.at[direction, k])

    def output(i, carry):
        at = pl.ds(al(i * 16, 16), 16)
        total = part[z, at, :].astype(F32) + fin[0, at, :].astype(F32) + fin[1, at, :].astype(F32)
        hid_ref[at, :] = (tok[z, at, :].astype(F32) + total).astype(BF16)
        return carry

    lax.fori_loop(0, 8, output, 0)

    arrive(vals.at[1], v_sem.at[1])

    def gaps(v, n):
        valid = frame < n
        reward = jnp.sum(jnp.where(frame == n - 1, v, 0.0), axis=(0, 1), keepdims=True)
        return valid, jnp.where(valid, reward - v, 0.0)

    other = vf_ref[1 - c]
    count = (length + other).astype(F32)
    valid, gap = gaps(values, length)
    valid_o, gap_o = gaps(vals[1], other)
    add = lambda a: jnp.sum(a, axis=(0, 1), keepdims=True)
    mean = (add(gap) + add(gap_o)) / count
    centered = jnp.where(valid, gap - mean, 0.0)
    centered_o = jnp.where(valid_o, gap_o - mean, 0.0)
    variance = (add(centered * centered) + add(centered_o * centered_o)) / count
    adv = jnp.where(valid, centered * lax.rsqrt(variance + 1e-5), 0.0)
    lane = lax.broadcasted_iota(jnp.int32, (1, 128), 1)

    def own_pair(a):
        first = jnp.sum(jnp.where(frame == 2 * s, a, 0.0), axis=(0, 1))
        second = jnp.sum(jnp.where(frame == 2 * s + 1, a, 0.0), axis=(0, 1))
        return jnp.where(lane == 0, first.reshape(1, 128), second.reshape(1, 128))[:, 0:2]

    fv_ref[...] = own_pair(values)
    adv_ref[...] = own_pair(adv)
    @pl.when(flip == 1)
    def _():
        for n in range(4):
            for half, (src, _, dst) in enumerate(pieces(n)):
                remote(
                    stage.at[n, p, src, third], qx.at[p, dst, lanes],
                    a_send.at[n, 3, 0, half], qs_recv.at[n], {"seq": me.seq(p, 3 - g)},
                ).wait_send()

    for i in range(4):
        stays = (1 - flip) * (p == i).astype(jnp.int32)

        @pl.when(stays == 0)
        def _():
            for a in (0, 1):
                back(i, a).wait_send()

    rest = [w1_copy(d, k) for d in (0, 1) for k in range(3)]
    rest += w2_own() + w2_relay() + [copy for n in range(4) for copy in d2d(n)]
    rest += [mx_copy(a, d, k) for a in (0, 1) for d in (0, 1) for k in range(3)]
    for d in (0, 1):
        rest += [direct_copy(d)] + [copy(d, n) for copy in (mid_copy, sum_copy) for n in range(4)]
    for copy in rest + sends:
        copy.wait_send()


def hand_over(hid_ref, fv_ref, adv_ref, hid_out, fv_out, adv_out, sem):
    copies = [
        pltpu.make_async_copy(hid_ref, hid_out.at[0], sem.at[0]),
        pltpu.make_async_copy(fv_ref, fv_out, sem.at[1]),
        pltpu.make_async_copy(adv_ref, adv_out, sem.at[2]),
    ]
    for copy in copies:
        copy.start()
    for copy in copies:
        copy.wait()


def local(
    tokens, attn_gain, w_qkv, w_out, mlp_gain, w_up, w_down, pool_gain, pool_bias, value_weight, valid_frames
):
    vmem = pltpu.VMEM
    dma = pltpu.SemaphoreType.DMA
    inside = pl.BlockSpec(memory_space=pltpu.VMEM)
    outside = pl.BlockSpec(memory_space=pl.ANY)
    hidden, values, advantages = pl.pallas_call(
        layer_kernel,
        out_shape=(
            jax.ShapeDtypeStruct((ROWS, D), BF16),
            jax.ShapeDtypeStruct((1, 2), F32),
            jax.ShapeDtypeStruct((1, 2), F32),
        ),
        in_specs=[pl.BlockSpec(memory_space=pltpu.SMEM)] + [outside] * 10,
        out_specs=(inside,) * 3,
        scratch_shapes=[
            vmem((4, ROWS, D), BF16),
            vmem((3, D, BLOCK), BF16),
            vmem((8, D), F32),
            vmem((ROWS, D), BF16),
            vmem((4, 4, ROWS, 384), BF16),
            vmem((4, BLOCK, 256), BF16),
            vmem((17, BLOCK, 384), BF16),
            vmem((17, DEPTH, BLOCK), BF16),
            vmem((9, 8, 256), F32),
            vmem((8, DEPTH, 256), F32),
            vmem((2 * BLOCK, 256), F32),
            vmem((2 * BLOCK, 256), BF16),
            vmem((4, BLOCK, HEAD_DIM), BF16),
            vmem((4, 4, BLOCK, HEAD_DIM), BF16),
            vmem((D, D), BF16),
            vmem((D, D), BF16),
            vmem((D, D), BF16),
            vmem((4, ROWS, D), BF16),
            vmem((2, 64, D), BF16),
            vmem((2, ROWS, D), BF16),
            vmem((2 * ROWS, D), BF16),
            vmem((2 * ROWS, D), BF16),
            vmem((3, 8, D), F32),
            vmem((4, 2, D), F32),
            vmem((16, 2, D), F32),
            vmem((16, 2, D), F32),
            vmem((2, 16, 2, 128), F32),
            dma((6,)),
            dma((6,)),
            dma((2, 3)),
            dma((2, 3)),
            dma((4, 4, 2, 2)),
            dma((4,)),
            dma((4,)),
            dma((4,)),
            dma((2, 4, 4)),
            dma((2, 4)),
            dma((4,)),
            dma((4, 2)),
            dma((4, 2)),
            dma((2, 2, 3)),
            dma((2, 2, 3)),
            dma((2, 3)),
            dma((2, 3)),
            dma((2, 5)),
            dma((2,)),
            dma((2,)),
            dma((4, 3)),
            dma,
            dma((2, 9)),
            dma((2, 4)),
            dma((2, 2)),
            dma((3,)),
            dma((4,)),
            dma((15,)),
            dma((16,)),
            dma((2,)),
        ],
        compiler_params=pltpu.CompilerParams(
            collective_id=0, has_side_effects=True, vmem_limit_bytes=63 * 2**20
        ),
        cost_estimate=pl.CostEstimate(flops=4 * 10**10, bytes_accessed=4 * 10**7, transcendentals=10**7),
    )(
        valid_frames, tokens[0], w_qkv, w_out, w_up, w_down,
        *(v.reshape(1, D) for v in (attn_gain, mlp_gain, pool_gain, pool_bias, value_weight)),
    )
    return pl.pallas_call(
        hand_over,
        out_shape=(
            jax.ShapeDtypeStruct((1, ROWS, D), BF16),
            jax.ShapeDtypeStruct((1, 2), F32),
            jax.ShapeDtypeStruct((1, 2), F32),
        ),
        in_specs=[inside] * 3,
        out_specs=(outside,) * 3,
        scratch_shapes=[dma((3,))],
    )(hidden, values, advantages)


def solution(mesh):
    in_specs = (
        P("dp", ("seq", "tensor"), None),
        P(),
        P(None, None, "tensor"),
        P("tensor", None),
        P(),
        P(None, "tensor"),
        P("tensor", None),
        P(),
        P(),
        P(),
        P(),
    )
    out_specs = (P("dp", ("seq", "tensor"), None), P("dp", "seq"), P("dp", "seq"))
    return jax.shard_map(local, mesh=mesh, in_specs=in_specs, out_specs=out_specs, check_vma=False)
```

```python
import functools
import math

import jax
import jax.numpy as jnp
from jax import lax
from jax.experimental import pallas as pl
from jax.experimental.pallas import tpu as pltpu
from jax.sharding import PartitionSpec as P

HEAD_DIM = 128
TOK_FRAME = 256
ROWS = 128
HALF = 64
BLOCK = 512
D = 2048
DEPTH = 144
BF16 = jnp.bfloat16
F32 = jnp.float32
MESH = pl.DeviceIdType.MESH
QSCALE = math.log2(math.e) / math.sqrt(HEAD_DIM)
NEG = -1e30
ONWARD = (0, 1)
HOOKS = (9, 21)
UNROLL = 3


def remote(src, dst, send_sem, recv_sem, where):
    return pltpu.make_async_remote_copy(
        src_ref=src, dst_ref=dst, send_sem=send_sem, recv_sem=recv_sem,
        device_id=where, device_id_type=MESH,
    )


def al(i, m):
    return pl.multiple_of(i, m)


class Place:
    def __init__(self):
        self.c = lax.axis_index("dp")
        s = lax.axis_index("seq")
        self.s = s
        self.z = lax.axis_index("tensor")
        y, x = s // 4, s % 4
        self.p = y * (1 - self.c) + x * self.c
        self.g = x * (1 - self.c) + y * self.c

    def seq(self, p, g):
        return (p * 4 + g) * (1 - self.c) + (g * 4 + p) * self.c

    def flip(self, p):
        return (1 - self.c) * (1 - p % 2) + self.c * (p // 2)

    def gq(self, p, g):
        return g + self.flip(p) * (3 - 2 * g)


def norm_rows(src, gain_ref, dst, rows):
    def body(i, carry):
        at = pl.ds(al(i * 16, 16), 16)
        x = src[at, :].astype(F32)
        square = jnp.mean(x * x, axis=-1, keepdims=True)
        dst[at, :] = (x * lax.rsqrt(square + 1e-5) * gain_ref[...]).astype(BF16)
        return carry

    lax.fori_loop(0, rows // 16, body, 0, unroll=True)


def gelu(x):
    return 0.5 * x * (1.0 + jnp.tanh(math.sqrt(2.0 / math.pi) * (x + 0.044715 * (x * x * x))))


def layer_kernel(
    vf_ref, tok_hbm, w_hbm, wo_hbm, wu_hbm, wd_hbm, g1_hbm, g2_hbm, pg_hbm, pb_hbm, vw_hbm,
    hid_ref, fv_ref, adv_ref,
    tok, w, small, normed, stage, qx, kx, vt, m_s, acc, s0, s1, o_stage, mx, wo, wu, wd,
    part, mid, fin, nrm, up, fs, zs, means, states, vals,
    tl_sem, w_sem, ts_sem, tr_sem, a_send, q_recv, k_recv, qs_recv,
    g_send, gk_recv, r_recv, o_send, o_recv, m_send, m_recv, w1_send, w1_recv, w2_send, w2_recv, w2r_recv,
    d_send, d_recv, rs_send, mid_recv, fin_recv, z_send, z_recv, s_send, s_recv, v_sem,
):
    me = Place()
    c, s, z, p, g = me.c, me.s, me.z, me.p, me.g
    zp, zm, z2 = (z + 1) % 4, (z + 3) % 4, (z + 2) % 4
    gp, gm, g2 = (g + 1) % 4, (g + 3) % 4, (g + 2) % 4
    flip = me.flip(p)
    gain_ref, gain2_ref = small.at[0:1, :], small.at[1:2, :]

    own_in = pltpu.make_async_copy(tok_hbm, tok.at[z], tl_sem.at[0])
    own_in.start()
    small_in = [
        pltpu.make_async_copy(src, small.at[k : k + 1, :], tl_sem.at[1 + k])
        for k, src in enumerate((g1_hbm, g2_hbm, pg_hbm, pb_hbm, vw_hbm))
    ]
    small_in[0].start()
    w_in = [pltpu.make_async_copy(w_hbm.at[k], w.at[k], w_sem.at[k]) for k in range(3)]
    for copy in w_in:
        copy.start()
    late_in = [
        pltpu.make_async_copy(wo_hbm, wo.at[pl.ds(al(z * BLOCK, BLOCK), BLOCK), :], w_sem.at[3]),
        pltpu.make_async_copy(wu_hbm, wu, w_sem.at[4]),
        pltpu.make_async_copy(wd_hbm, wd, w_sem.at[5]),
    ]

    barrier = pltpu.get_barrier_semaphore()
    for t in (zp, zm, z2):
        pl.semaphore_signal(barrier, inc=1, device_id={"tensor": t}, device_id_type=MESH)
    for d in range(1, 16):
        pl.semaphore_signal(barrier, inc=1, device_id={"seq": (s + d) % 16}, device_id_type=MESH)
    pl.semaphore_signal(barrier, inc=1, device_id={"dp": 1 - c}, device_id_type=MESH)
    own_in.wait()
    pl.semaphore_wait(barrier, 19)

    halves = (pl.ds(0, HALF), pl.ds(HALF, HALF))
    sends = []

    def send(src, dst, send_sem, recv_sem, to):
        copy = remote(src, dst, send_sem, recv_sem, to)
        copy.start()
        sends.append(copy)

    def start_only(src, dst, send_sem, recv_sem, to):
        remote(src, dst, send_sem, recv_sem, to).start()

    def arrive(ref, sem):
        remote(ref, ref, sem, sem, {"tensor": zp}).wait_recv()

    def tok_send(direction, k, t, half):
        ref = tok.at[t, halves[half], :]
        start_only(ref, ref, ts_sem.at[direction, k], tr_sem.at[direction, k], {"tensor": zp if direction == 0 else zm})

    def tok_wait(direction, k, t, half):
        arrive(tok.at[t, halves[half], :], tr_sem.at[direction, k])

    tok_send(0, 0, z, 0)
    tok_send(1, 0, z, 1)
    tok_send(0, 1, z, 1)
    tok_send(1, 1, z, 0)

    stages = (((z, 0), (z, 1)), ((zm, 0), (zp, 1)), ((zm, 1), (zp, 0)), ((z2, 0), (z2, 1)))

    def rows_of(piece):
        t, half = piece
        return pl.ds(al(t * ROWS + half * HALF, HALF), HALF)

    def project(n):
        for k, (t, half) in enumerate(stages[n]):
            norm_rows(tok.at[t, halves[half], :], gain_ref, normed.at[halves[k], :], HALF)
        for k in (1, 2, 0):
            for pair in range(2):
                out = jnp.dot(
                    normed[...], w[k, :, pair * 256 : pair * 256 + 256], preferred_element_type=F32
                )
                if k == 0:
                    out = out * QSCALE
                out = out.astype(BF16)
                at = slice((2 - k) * 128, (3 - k) * 128)
                stage[n, 2 * pair, :, at] = out[:, :128]
                stage[n, 2 * pair + 1, :, at] = out[:, 128:]

    def query_rows(piece, count):
        t, half = piece
        return pl.ds(al((t % 2) * 256 + (t // 2) * ROWS + half * HALF, HALF), count)

    both = pl.ds(0, 256)
    third = pl.ds(256, 128)
    lanes = pl.ds(0, HEAD_DIM)

    def pieces(n):
        if n in (0, 3):
            piece = stages[n][0]
            return ((pl.ds(0, ROWS), pl.ds(al(piece[0] * ROWS, ROWS), ROWS), query_rows(piece, ROWS)),)
        return tuple((halves[k], rows_of(piece), query_rows(piece, HALF)) for k, piece in enumerate(stages[n]))

    def hand_out(n):
        for k, (buf, sem, part) in enumerate(((kx, k_recv, both), (qx, q_recv, third))):
            for d in (2, 1, 3):
                h = (p + d) % 4
                to = {"seq": me.seq(h, me.gq(p, g) if k else g)}
                slot = p if k else g * 4 + p
                for half, (src, dst, dst_q) in enumerate(pieces(n)):
                    send(
                        stage.at[n, h, src, part], buf.at[slot, dst_q if k else dst, lanes if k else both],
                        a_send.at[n, d - 1, k, half], sem.at[n], to,
                    )
        for src, dst, _ in pieces(n):
            kx[g * 4 + p, dst, 0:256] = stage[n, p, src, 0:256]

        @pl.when(flip == 1)
        def _():
            for half, (src, _, dst) in enumerate(pieces(n)):
                remote(
                    stage.at[n, p, src, third], qx.at[p, dst, lanes],
                    a_send.at[n, 3, 0, half], qs_recv.at[n], {"seq": me.seq(p, 3 - g)},
                ).start()

        @pl.when(flip == 0)
        def _():
            for src, _, dst in pieces(n):
                qx[p, dst, 0:128] = stage[n, p, src, 256:384]

    def stage_in(count, buf, sem):
        arrive(buf.at[pl.ds(0, count), pl.ds(0, ROWS), lanes if buf is qx else both], sem)

    def ring_out(n):
        stage_in(3, kx, k_recv.at[n])
        for direction in (0, 1):
            to = {"seq": me.seq(p, gp if direction == 0 else gm)}
            for half, (_, dst, _) in enumerate(pieces(n)):
                ref = kx.at[pl.ds(g * 4, 4), dst, both]
                send(ref, ref, g_send.at[direction, n, half], gk_recv.at[direction, n], to)

    def relay(n):
        for direction in sorted(set(ONWARD)):
            stage_in(4, kx, gk_recv.at[direction, n])
            source, to = (gm, gp) if direction == 0 else (gp, gm)
            if ONWARD[0] == ONWARD[1]:
                runs = pieces(n)
            else:
                runs = ((0, rows_of(stages[n][direction]), 0),)
            for half, (_, dst, _) in enumerate(runs):
                ref = kx.at[pl.ds(source * 4, 4), dst, both]
                send(ref, ref, g_send.at[direction, n, 2 + half], r_recv.at[n], {"seq": me.seq(p, to)})

    def wo_rows(t, k, first, count):
        return wo.at[pl.ds(al(t * BLOCK + c * 256 + k * 64 + first, 32), count), :]

    def w1_copy(direction, k):
        to = zp if direction == 0 else zm
        t, first = ((z, 0), (z, 32), (zm, 0))[k] if direction == 0 else ((z, 32), (z, 0), (zp, 32))[k]
        ref = wo_rows(t, g, first, 32)
        return remote(ref, ref, w1_send.at[direction, k], w1_recv.at[direction, k], {"tensor": to})

    def w1_arrive(direction, k):
        arrive(wo.at[pl.ds(0, 32), :], w1_recv.at[direction, k])

    def w2_own():
        copies = []
        for direction in (0, 1):
            to = {"seq": me.seq(p, gp if direction == 0 else gm)}
            for k, t in enumerate((zp, zm, z2)):
                ref = wo_rows(t, g, 0, 64)
                copies.append(remote(ref, ref, w2_send.at[direction, k], w2_recv.at[direction], to))
        return copies

    def w2_relay():
        copies = []
        for direction in (0, 1):
            source, to = (gm, gp) if direction == 0 else (gp, gm)
            for k, ref in enumerate(
                (wo_rows(zm if direction else zp, source, 0, 64), wo_rows(z2, source, 32 * direction, 32))
            ):
                copies.append(
                    remote(ref, ref, w2_send.at[direction, 3 + k], w2r_recv.at[direction], {"seq": me.seq(p, to)})
                )
        return copies

    def d2d(n):
        k = (g, gm, gp, g2)[n]
        return [
            remote(ref, ref, d_send.at[n, i], d_recv, {"dp": 1 - c})
            for i, ref in enumerate(wo_rows(t, k, 0, 64) for t in (zp, zm, z2))
        ]

    def start(copies):
        for copy in copies:
            copy.start()

    small_in[0].wait()
    for copy in w_in:
        copy.wait()
    start(late_in)
    start(small_in[1:])
    project(0)
    hand_out(0)

    length = vf_ref[c]
    lane = lax.broadcasted_iota(jnp.int32, (BLOCK, 128), 1)
    row = lax.broadcasted_iota(jnp.int32, (BLOCK, 128), 0)

    def fill(slot, carry):
        block = me.seq(slot % 4, slot // 4)
        frame = 2 * block + row // TOK_FRAME
        bias = jnp.where((lane == 0) & (frame >= length), NEG, 0.0)
        mine = 0
        for i in range(4):
            mine = mine + (lane == 1 + i).astype(jnp.int32) * (
                me.seq(i, me.gq(i, g)) == block
            ).astype(jnp.int32)
        bias = jnp.where((mine > 0) & (row >= TOK_FRAME), NEG, bias)
        kx[slot, :, 256:384] = bias.astype(BF16)
        vt[slot, 128:DEPTH, :] = jnp.ones((DEPTH - 128, BLOCK), BF16)
        return carry

    lax.fori_loop(0, 16, fill, 0)
    kx[16, :, 0:256] = jnp.zeros((BLOCK, 256), BF16)
    kx[16, :, 256:384] = jnp.where(lane == 0, NEG, 0.0).astype(BF16)
    vt[16] = jnp.zeros((DEPTH, BLOCK), BF16)
    for i in range(4):
        on = (lane == 0) | ((lane == 1 + i) & (row % 256 < ROWS))
        qx[i, :, 128:256] = jnp.where(on, 1.0, 0.0).astype(BF16)

    tok_wait(0, 0, zm, 0)
    tok_send(0, 2, zm, 0)
    tok_wait(1, 0, zp, 1)
    tok_send(1, 2, zp, 1)
    ring_out(0)
    project(1)
    hand_out(1)
    tok_wait(0, 1, zm, 1)
    tok_wait(1, 1, zp, 0)
    project(2)
    hand_out(2)
    ring_out(1)
    relay(0)
    tok_wait(0, 2, z2, 0)
    tok_wait(1, 2, z2, 1)
    project(3)
    hand_out(3)
    late_in[0].wait()
    start([w1_copy(0, 0), w1_copy(1, 0), w1_copy(0, 1), w1_copy(1, 1)])
    ring_out(2)
    relay(1)
    ring_out(3)
    relay(2)
    for n in range(4):
        stage_in(3, qx, q_recv.at[n])

        @pl.when(flip == 1)
        def _():
            stage_in(1, qx, qs_recv.at[n])

    def turn(gg):
        def body(j, carry):
            vt[gg * 4 + j, 0:128, :] = kx[gg * 4 + j, :, 0:128].T
            return carry

        lax.fori_loop(0, 4, body, 0)

    w1_arrive(0, 0)
    w1_copy(0, 2).start()
    w1_arrive(1, 0)
    w1_copy(1, 2).start()
    turn(g)
    relay(3)
    for direction in (0, 1):
        for k in (1, 2):
            w1_arrive(direction, k)
    start(w2_own())
    start(d2d(0))
    for direction in (0, 1):
        if direction not in ONWARD:
            for n in range(4):
                stage_in(4, kx, gk_recv.at[direction, n])
    turn(gm)
    turn(gp)
    for n in range(4):
        stage_in(4, kx, r_recv.at[n])
    turn(g2)

    def slot_of(b, count):
        pad = (b >= count).astype(jnp.int32)
        slot = (1 - c) * (lax.rem(b, 4) * 4 + lax.div(b, 4)) + c * b
        return slot + pad * (16 - slot)

    counts = [me.seq(i, me.gq(i, g)) + 1 for i in range(4)]
    first = [0]
    for count in counts:
        first.append(first[-1] + (count + 1) // 2)
    turns = first[4]

    def pick(at_i, choices):
        return sum(((at_i == k).astype(jnp.int32) * value for k, value in enumerate(choices)), 0)

    def unit(u):
        past = (u >= 2 * turns).astype(jnp.int32)
        u = u - past * (u - 2 * turns + 1)
        a = (u >= turns).astype(jnp.int32)
        v = u - a * turns
        i = sum(((v >= first[k]).astype(jnp.int32) for k in (1, 2, 3)), 0)
        j = v - pick(i, first[:4])
        count = pick(i, counts)
        slots = tuple(slot + past * (16 - slot) for slot in (slot_of(2 * j, count), slot_of(2 * j + 1, count)))
        return a, i, *slots

    def score(now):
        a, i, *slots = now
        for k, slot in enumerate(slots):
            s0[k * BLOCK : (k + 1) * BLOCK, :] = lax.dot_general(
                kx[slot, :, 128:384], qx[i, pl.ds(al(a * 256, 256), 256), :], (((1,), (1,)), ((), ())),
                preferred_element_type=F32,
            )

    def soften(now):
        a, i, *_ = now
        before = m_s[a * 4 + i, 0:1, :]
        peak = jnp.full((8, 256), -1e38, F32)
        for r in range(0, 2 * BLOCK, 128):
            peak = jnp.maximum(peak, jnp.max(s0[r : r + 128, :].reshape(16, 8, 256), axis=0))
        peak = jnp.maximum(before, jnp.max(peak, axis=0, keepdims=True))
        m_s[a * 4 + i, 0:1, :] = peak
        m_s[8, 0:1, :] = jnp.exp2(before - peak)
        for r in range(0, 2 * BLOCK, 128):
            s1[r : r + 128, :] = jnp.exp2(s0[r : r + 128, :] - peak).astype(BF16)

    def gather(now):
        a, i, *slots = now
        out = acc[a * 4 + i] * m_s[8, 0:1, :]
        for k, slot in enumerate(slots):
            out = out + jnp.dot(vt[slot], s1[k * BLOCK : (k + 1) * BLOCK, :], preferred_element_type=F32)
        acc[a * 4 + i] = out

    def back(i, a):
        rows = pl.ds(a * 256, 256)
        return remote(
            o_stage.at[i, rows, :], mx.at[z, p, rows, :], o_send.at[i, a], o_recv.at[p, a],
            {"seq": me.seq(i, me.gq(i, g))},
        )

    def o_arrive(a):
        rows = pl.ds(a * 256, 256)
        for d in (1, 2, 3):
            h = (p + d) % 4
            arrive(mx.at[z, h, rows, :], o_recv.at[h, a])

        @pl.when(flip == 1)
        def _():
            arrive(mx.at[z, p, rows, :], o_recv.at[p, a])

    def mx_copy(a, direction, k):
        to = zp if direction == 0 else zm
        t, half = ((z, 0), (z, 1), (zm, 0))[k] if direction == 0 else ((z, 1), (z, 0), (zp, 1))[k]
        ref = mx.at[t, :, pl.ds(a * 256 + half * ROWS, ROWS), :]
        return remote(ref, ref, m_send.at[a, direction, k], m_recv.at[a, direction, k], {"tensor": to})

    def mx_arrive(a, direction, k):
        arrive(mx.at[z, :, pl.ds(0, ROWS), :], m_recv.at[a, direction, k])

    def mx_own(a):
        start([mx_copy(a, 0, 0), mx_copy(a, 1, 0), mx_copy(a, 0, 1), mx_copy(a, 1, 1)])

    def mx_relay(a):
        for direction in (0, 1):
            mx_arrive(a, direction, 0)
            mx_copy(a, direction, 2).start()

    def w2_onward():
        for direction in (0, 1):
            arrive(wo.at[pl.ds(0, 192), :], w2_recv.at[direction])
        start(w2_relay())
        start(d2d(1))
        start(d2d(2))

    def give_back(a):
        for i in range(4):
            rows = pl.ds(a * 256, 256)
            out = acc[a * 4 + i, 0:128, :] / acc[a * 4 + i, 128:129, :]
            o_stage[i, rows, :] = out.T.astype(BF16)
            stays = (1 - flip) * (p == i).astype(jnp.int32)

            @pl.when(stays == 0)
            def _():
                back(i, a).start()

            @pl.when(stays == 1)
            def _():
                mx[z, p, rows, :] = o_stage[i, rows, :]

    for k in range(8):
        m_s[k] = jnp.full((8, 256), -1e38, F32)
        acc[k] = jnp.zeros((DEPTH, 256), F32)
    def w2_last():
        for direction in (0, 1):
            arrive(wo.at[pl.ds(0, 96), :], w2r_recv.at[direction])
        start(d2d(3))

    score(unit(0))
    soften(unit(0))
    score(unit(1))

    per = UNROLL
    half_way = (turns + per - 1) // per

    def turn_step(n, carry):
        @pl.when(n == half_way)
        def _():
            give_back(0)

        @pl.when(n == half_way + HOOKS[0] // per)
        def _():
            o_arrive(0)
            mx_own(0)

        pl.when(n == HOOKS[1] // per)(w2_onward)
        units = [*carry, *(unit((n + 1) * per + k) for k in (2, *range(3, per + 2)))]
        for k in range(per):
            gather(carry[k])
            soften(carry[k + 1])
            score(carry[k + 2])
        return tuple(units[per:])

    lax.fori_loop(0, (2 * turns + per - 1) // per, turn_step, tuple(unit(k) for k in range(per + 2)))
    give_back(1)

    mx_relay(0)
    w2_last()
    o_arrive(1)
    mx_own(1)
    for copy in small_in[1:]:
        copy.wait()
    for direction in (0, 1):
        for k in range(3):
            ref = tok.at[0, halves[0], :]
            remote(ref, ref, ts_sem.at[direction, k], ts_sem.at[direction, k], {"tensor": zp}).wait_send()

    def frame_rows(a):
        for direction in (0, 1):
            for k in (1, 2):
                mx_arrive(a, direction, k)

    def out_project(a):
        rows = pl.ds(a * 256, 256)

        for n in range(4):
            cols = slice(n * 512, n * 512 + 512)
            lhs = jnp.concatenate([mx[t, h, rows, :] for t in range(4) for h in range(4)], axis=1)
            x = jnp.dot(lhs, wo[:, cols], preferred_element_type=F32)
            for k in (0, 1):
                t = a + 2 * k
                tok[t, :, cols] = (tok[t, :, cols].astype(F32) + x[k * ROWS : (k + 1) * ROWS]).astype(BF16)
        for k in (0, 1):
            norm_rows(tok.at[a + 2 * k], gain2_ref, nrm.at[pl.ds(k * ROWS, ROWS), :], ROWS)

    lo, hi = halves
    ways = ((zp, lo, hi), (zm, hi, lo))

    def mid_copy(direction, n):
        to, rows, _ = ways[direction]
        cols = pl.ds(n * 512, 512)
        return remote(
            part.at[z2, rows, cols], mid.at[direction, :, cols], rs_send.at[direction, n],
            mid_recv.at[direction, n], {"tensor": to},
        )

    def direct_copy(direction):
        to, _, rows = ways[direction]
        return remote(
            part.at[to, rows, :], fin.at[direction, rows, :], rs_send.at[direction, 4],
            fin_recv.at[direction, 0], {"tensor": to},
        )

    def sum_copy(direction, n):
        to, rows, _ = ways[direction]
        cols = pl.ds(n * 512, 512)
        return remote(
            part.at[to, rows, cols], fin.at[direction, rows, cols], rs_send.at[direction, 5 + n],
            fin_recv.at[direction, 1], {"tensor": to},
        )

    def up_down(a, between=lambda: None):
        for n in range(4):
            cols = slice(n * 512, n * 512 + 512)
            x = jnp.dot(nrm[...], wu[:, cols], preferred_element_type=F32)
            up[:, cols] = gelu(x).astype(BF16)

        for n in range(4):
            cols = slice(n * 512, n * 512 + 512)
            x = jnp.dot(up[...], wd[:, cols], preferred_element_type=F32)
            for k in (0, 1):
                rows = x[k * ROWS : (k + 1) * ROWS]
                part[a + 2 * k, :, cols] = rows.astype(BF16)
                rows = jnp.sum(rows.reshape(16, 8, 512), axis=0)
                fs[k, :, cols] = fs[k, :, cols] + rows if a else rows
            if n == 3:
                between()
            if a == 1 and n < 3:
                continue

            @pl.when(z2 % 2 == a)
            def _():
                for m in range(4) if a else (n,):
                    for direction in (0, 1):
                        mid_copy(direction, m).start()

    def rs_first(a):
        for t, direction in ((zp, 0), (zm, 1)):

            @pl.when(t % 2 == a)
            def _():
                direct_copy(direction).start()

    def rs_sums(a):
        @pl.when(zp % 2 == a)
        def _():
            for n in range(4):
                cols = slice(n * 512, n * 512 + 512)
                for direction, (t, half) in enumerate(((zp, 0), (zm, 64))):
                    arrive(mid.at[direction, :, pl.ds(n * 512, 512)], mid_recv.at[direction, n])
                    rows = slice(half, half + 64)
                    part[t, rows, cols] = (
                        part[t, rows, cols].astype(F32) + mid[direction, :, cols].astype(F32)
                    ).astype(BF16)
                    sum_copy(direction, n).start()

    frame_rows(0)
    arrive(wo.at[pl.ds(0, 768), :], d_recv)
    out_project(0)
    mx_relay(1)
    late_in[1].wait()
    late_in[2].wait()
    up_down(0)
    rs_first(0)
    frame_rows(1)
    out_project(1)
    def residual(i, total):
        at = pl.ds(al(i * 16, 16), 16)
        return total + jnp.sum(tok[z, at, :].astype(F32).reshape(2, 8, D), axis=0)

    fs[2] = lax.fori_loop(0, 8, residual, jnp.zeros((8, D), F32))

    def sums_out():
        for k in (0, 1):
            mine = (z // 2 == k).astype(F32)
            zs[z, k : k + 1, :] = jnp.sum(fs[k] + fs[2] * mine, axis=0, keepdims=True)
        for d in (1, 2, 3):
            send(zs.at[z], zs.at[z], z_send.at[d - 1], z_recv.at[z], {"tensor": (z + d) % 4})

    rs_sums(0)
    up_down(1, sums_out)
    rs_first(1)
    for d in (1, 2, 3):
        t = (z + d) % 4
        arrive(zs.at[t], z_recv.at[t])
    means[s] = (zs[0] + zs[1] + zs[2] + zs[3]) * (1.0 / TOK_FRAME)
    for d in range(1, 16):
        send(means.at[s], means.at[s], s_send.at[d - 1], s_recv.at[s], {"seq": (s + d) % 16})
    rs_sums(1)
    for d in range(1, 16):
        t = (s + d) % 16
        arrive(means.at[t], s_recv.at[t])
    frame = 2 * lax.broadcasted_iota(jnp.int32, (16, 2, 128), 0) + lax.broadcasted_iota(jnp.int32, (16, 2, 128), 1)
    pg, pb, vw = small[2:3, :], small[3:4, :], small[4:5, :]

    def scan(i, state):
        m = means[i]
        gate = jax.nn.sigmoid(m * pg + pb)
        source = (1.0 - gate) * m
        for k in (0, 1):
            new = gate[k : k + 1] * state + source[k : k + 1]
            state = jnp.where(2 * i + k < length, new, state)
            states[i, k : k + 1, :] = state
        return state

    lax.fori_loop(0, 16, scan, jnp.zeros((1, D), F32))
    total = jnp.sum(states[...] * vw.reshape(1, 1, D), axis=-1, keepdims=True)
    values = jnp.where(frame < length, jnp.broadcast_to(total, (16, 2, 128)), 0.0)
    vals[0] = values
    send(vals.at[0], vals.at[1], v_sem.at[0], v_sem.at[1], {"dp": 1 - c})

    for direction in (0, 1):
        for k in (0, 1):
            arrive(fin.at[direction, lo, :], fin_recv.at[direction, k])

    def output(i, carry):
        at = pl.ds(al(i * 16, 16), 16)
        total = part[z, at, :].astype(F32) + fin[0, at, :].astype(F32) + fin[1, at, :].astype(F32)
        hid_ref[at, :] = (tok[z, at, :].astype(F32) + total).astype(BF16)
        return carry

    lax.fori_loop(0, 8, output, 0)

    arrive(vals.at[1], v_sem.at[1])

    def gaps(v, n):
        valid = frame < n
        reward = jnp.sum(jnp.where(frame == n - 1, v, 0.0), axis=(0, 1), keepdims=True)
        return valid, jnp.where(valid, reward - v, 0.0)

    other = vf_ref[1 - c]
    count = (length + other).astype(F32)
    valid, gap = gaps(values, length)
    valid_o, gap_o = gaps(vals[1], other)
    add = lambda a: jnp.sum(a, axis=(0, 1), keepdims=True)
    mean = (add(gap) + add(gap_o)) / count
    centered = jnp.where(valid, gap - mean, 0.0)
    centered_o = jnp.where(valid_o, gap_o - mean, 0.0)
    variance = (add(centered * centered) + add(centered_o * centered_o)) / count
    adv = jnp.where(valid, centered * lax.rsqrt(variance + 1e-5), 0.0)
    lane = lax.broadcasted_iota(jnp.int32, (1, 128), 1)

    def own_pair(a):
        first = jnp.sum(jnp.where(frame == 2 * s, a, 0.0), axis=(0, 1))
        second = jnp.sum(jnp.where(frame == 2 * s + 1, a, 0.0), axis=(0, 1))
        return jnp.where(lane == 0, first.reshape(1, 128), second.reshape(1, 128))[:, 0:2]

    fv_ref[...] = own_pair(values)
    adv_ref[...] = own_pair(adv)
    @pl.when(flip == 1)
    def _():
        for n in range(4):
            for half, (src, _, dst) in enumerate(pieces(n)):
                remote(
                    stage.at[n, p, src, third], qx.at[p, dst, lanes],
                    a_send.at[n, 3, 0, half], qs_recv.at[n], {"seq": me.seq(p, 3 - g)},
                ).wait_send()

    for i in range(4):
        stays = (1 - flip) * (p == i).astype(jnp.int32)

        @pl.when(stays == 0)
        def _():
            for a in (0, 1):
                back(i, a).wait_send()

    rest = [w1_copy(d, k) for d in (0, 1) for k in range(3)]
    rest += w2_own() + w2_relay() + [copy for n in range(4) for copy in d2d(n)]
    rest += [mx_copy(a, d, k) for a in (0, 1) for d in (0, 1) for k in range(3)]
    for d in (0, 1):
        rest += [direct_copy(d)] + [copy(d, n) for copy in (mid_copy, sum_copy) for n in range(4)]
    for copy in rest + sends:
        copy.wait_send()


def hand_over(hid_ref, fv_ref, adv_ref, hid_out, fv_out, adv_out, sem):
    copies = [
        pltpu.make_async_copy(hid_ref, hid_out.at[0], sem.at[0]),
        pltpu.make_async_copy(fv_ref, fv_out, sem.at[1]),
        pltpu.make_async_copy(adv_ref, adv_out, sem.at[2]),
    ]
    for copy in copies:
        copy.start()
    for copy in copies:
        copy.wait()


def local(
    tokens, attn_gain, w_qkv, w_out, mlp_gain, w_up, w_down, pool_gain, pool_bias, value_weight, valid_frames
):
    vmem = pltpu.VMEM
    dma = pltpu.SemaphoreType.DMA
    inside = pl.BlockSpec(memory_space=pltpu.VMEM)
    outside = pl.BlockSpec(memory_space=pl.ANY)
    hidden, values, advantages = pl.pallas_call(
        layer_kernel,
        out_shape=(
            jax.ShapeDtypeStruct((ROWS, D), BF16),
            jax.ShapeDtypeStruct((1, 2), F32),
            jax.ShapeDtypeStruct((1, 2), F32),
        ),
        in_specs=[pl.BlockSpec(memory_space=pltpu.SMEM)] + [outside] * 10,
        out_specs=(inside,) * 3,
        scratch_shapes=[
            vmem((4, ROWS, D), BF16),
            vmem((3, D, BLOCK), BF16),
            vmem((8, D), F32),
            vmem((ROWS, D), BF16),
            vmem((4, 4, ROWS, 384), BF16),
            vmem((4, BLOCK, 256), BF16),
            vmem((17, BLOCK, 384), BF16),
            vmem((17, DEPTH, BLOCK), BF16),
            vmem((9, 8, 256), F32),
            vmem((8, DEPTH, 256), F32),
            vmem((2 * BLOCK, 256), F32),
            vmem((2 * BLOCK, 256), BF16),
            vmem((4, BLOCK, HEAD_DIM), BF16),
            vmem((4, 4, BLOCK, HEAD_DIM), BF16),
            vmem((D, D), BF16),
            vmem((D, D), BF16),
            vmem((D, D), BF16),
            vmem((4, ROWS, D), BF16),
            vmem((2, 64, D), BF16),
            vmem((2, ROWS, D), BF16),
            vmem((2 * ROWS, D), BF16),
            vmem((2 * ROWS, D), BF16),
            vmem((3, 8, D), F32),
            vmem((4, 2, D), F32),
            vmem((16, 2, D), F32),
            vmem((16, 2, D), F32),
            vmem((2, 16, 2, 128), F32),
            dma((6,)),
            dma((6,)),
            dma((2, 3)),
            dma((2, 3)),
            dma((4, 4, 2, 2)),
            dma((4,)),
            dma((4,)),
            dma((4,)),
            dma((2, 4, 4)),
            dma((2, 4)),
            dma((4,)),
            dma((4, 2)),
            dma((4, 2)),
            dma((2, 2, 3)),
            dma((2, 2, 3)),
            dma((2, 3)),
            dma((2, 3)),
            dma((2, 5)),
            dma((2,)),
            dma((2,)),
            dma((4, 3)),
            dma,
            dma((2, 9)),
            dma((2, 4)),
            dma((2, 2)),
            dma((3,)),
            dma((4,)),
            dma((15,)),
            dma((16,)),
            dma((2,)),
        ],
        compiler_params=pltpu.CompilerParams(
            collective_id=0, has_side_effects=True, vmem_limit_bytes=63 * 2**20
        ),
        cost_estimate=pl.CostEstimate(flops=4 * 10**10, bytes_accessed=4 * 10**7, transcendentals=10**7),
    )(
        valid_frames, tokens[0], w_qkv, w_out, w_up, w_down,
        *(v.reshape(1, D) for v in (attn_gain, mlp_gain, pool_gain, pool_bias, value_weight)),
    )
    return pl.pallas_call(
        hand_over,
        out_shape=(
            jax.ShapeDtypeStruct((1, ROWS, D), BF16),
            jax.ShapeDtypeStruct((1, 2), F32),
            jax.ShapeDtypeStruct((1, 2), F32),
        ),
        in_specs=[inside] * 3,
        out_specs=(outside,) * 3,
        scratch_shapes=[dma((3,))],
    )(hidden, values, advantages)


def solution(mesh):
    in_specs = (
        P("dp", ("seq", "tensor"), None),
        P(),
        P(None, None, "tensor"),
        P("tensor", None),
        P(),
        P(None, "tensor"),
        P("tensor", None),
        P(),
        P(),
        P(),
        P(),
    )
    out_specs = (P("dp", ("seq", "tensor"), None), P("dp", "seq"), P("dp", "seq"))
    return jax.shard_map(local, mesh=mesh, in_specs=in_specs, out_specs=out_specs, check_vma=False)
```

```python
import functools
import math

import jax
import jax.numpy as jnp
from jax import lax
from jax.experimental import pallas as pl
from jax.experimental.pallas import tpu as pltpu
from jax.sharding import PartitionSpec as P

HEAD_DIM = 128
TOK_FRAME = 256
ROWS = 128
HALF = 64
BLOCK = 512
D = 2048
DEPTH = 144
BF16 = jnp.bfloat16
F32 = jnp.float32
MESH = pl.DeviceIdType.MESH
QSCALE = math.log2(math.e) / math.sqrt(HEAD_DIM)
NEG = -1e30
ONWARD = (0, 1)
HOOKS = (9, 21)
UNROLL = 3


def remote(src, dst, send_sem, recv_sem, where):
    return pltpu.make_async_remote_copy(
        src_ref=src, dst_ref=dst, send_sem=send_sem, recv_sem=recv_sem,
        device_id=where, device_id_type=MESH,
    )


def al(i, m):
    return pl.multiple_of(i, m)


class Place:
    def __init__(self):
        self.c = lax.axis_index("dp")
        s = lax.axis_index("seq")
        self.s = s
        self.z = lax.axis_index("tensor")
        y, x = s // 4, s % 4
        self.p = y * (1 - self.c) + x * self.c
        self.g = x * (1 - self.c) + y * self.c

    def seq(self, p, g):
        return (p * 4 + g) * (1 - self.c) + (g * 4 + p) * self.c

    def flip(self, p):
        return (1 - self.c) * (1 - p % 2) + self.c * (p // 2)

    def gq(self, p, g):
        return g + self.flip(p) * (3 - 2 * g)


def norm_rows(src, gain_ref, dst, rows):
    def body(i, carry):
        at = pl.ds(al(i * 16, 16), 16)
        x = src[at, :].astype(F32)
        square = jnp.mean(x * x, axis=-1, keepdims=True)
        dst[at, :] = (x * lax.rsqrt(square + 1e-5) * gain_ref[...]).astype(BF16)
        return carry

    lax.fori_loop(0, rows // 16, body, 0, unroll=True)


def gelu(x):
    return 0.5 * x * (1.0 + jnp.tanh(math.sqrt(2.0 / math.pi) * (x + 0.044715 * (x * x * x))))


def layer_kernel(
    vf_ref, tok_hbm, w_hbm, wo_hbm, wu_hbm, wd_hbm, g1_hbm, g2_hbm, pg_hbm, pb_hbm, vw_hbm,
    hid_ref, fv_ref, adv_ref,
    tok, w, small, normed, stage, qx, kx, vt, m_s, acc, s0, s1, o_stage, mx, wo, wu, wd,
    part, mid, fin, nrm, up, fs, zs, means, states, vals,
    tl_sem, w_sem, ts_sem, tr_sem, a_send, q_recv, k_recv, qs_recv,
    g_send, gk_recv, r_recv, o_send, o_recv, m_send, m_recv, w1_send, w1_recv, w2_send, w2_recv, w2r_recv,
    d_send, d_recv, rs_send, mid_recv, fin_recv, z_send, z_recv, s_send, s_recv, v_sem,
):
    me = Place()
    c, s, z, p, g = me.c, me.s, me.z, me.p, me.g
    zp, zm, z2 = (z + 1) % 4, (z + 3) % 4, (z + 2) % 4
    gp, gm, g2 = (g + 1) % 4, (g + 3) % 4, (g + 2) % 4
    flip = me.flip(p)
    gain_ref, gain2_ref = small.at[0:1, :], small.at[1:2, :]

    own_in = pltpu.make_async_copy(tok_hbm, tok.at[z], tl_sem.at[0])
    own_in.start()
    small_in = [
        pltpu.make_async_copy(src, small.at[k : k + 1, :], tl_sem.at[1 + k])
        for k, src in enumerate((g1_hbm, g2_hbm, pg_hbm, pb_hbm, vw_hbm))
    ]
    small_in[0].start()
    w_in = [pltpu.make_async_copy(w_hbm.at[k], w.at[k], w_sem.at[k]) for k in range(3)]
    for copy in w_in:
        copy.start()
    late_in = [
        pltpu.make_async_copy(wo_hbm, wo.at[pl.ds(al(z * BLOCK, BLOCK), BLOCK), :], w_sem.at[3]),
        pltpu.make_async_copy(wu_hbm, wu, w_sem.at[4]),
        pltpu.make_async_copy(wd_hbm, wd, w_sem.at[5]),
    ]

    barrier = pltpu.get_barrier_semaphore()
    for t in (zp, zm, z2):
        pl.semaphore_signal(barrier, inc=1, device_id={"tensor": t}, device_id_type=MESH)
    for d in range(1, 16):
        pl.semaphore_signal(barrier, inc=1, device_id={"seq": (s + d) % 16}, device_id_type=MESH)
    pl.semaphore_signal(barrier, inc=1, device_id={"dp": 1 - c}, device_id_type=MESH)
    own_in.wait()
    pl.semaphore_wait(barrier, 19)

    halves = (pl.ds(0, HALF), pl.ds(HALF, HALF))
    sends = []

    def send(src, dst, send_sem, recv_sem, to):
        copy = remote(src, dst, send_sem, recv_sem, to)
        copy.start()
        sends.append(copy)

    def start_only(src, dst, send_sem, recv_sem, to):
        remote(src, dst, send_sem, recv_sem, to).start()

    def arrive(ref, sem):
        remote(ref, ref, sem, sem, {"tensor": zp}).wait_recv()

    def tok_send(direction, k, t, half):
        ref = tok.at[t, halves[half], :]
        start_only(ref, ref, ts_sem.at[direction, k], tr_sem.at[direction, k], {"tensor": zp if direction == 0 else zm})

    def tok_wait(direction, k, t, half):
        arrive(tok.at[t, halves[half], :], tr_sem.at[direction, k])

    tok_send(0, 0, z, 0)
    tok_send(1, 0, z, 1)
    tok_send(0, 1, z, 1)
    tok_send(1, 1, z, 0)

    stages = (((z, 0), (z, 1)), ((zm, 0), (zp, 1)), ((zm, 1), (zp, 0)), ((z2, 0), (z2, 1)))

    def rows_of(piece):
        t, half = piece
        return pl.ds(al(t * ROWS + half * HALF, HALF), HALF)

    def project(n):
        for k, (t, half) in enumerate(stages[n]):
            norm_rows(tok.at[t, halves[half], :], gain_ref, normed.at[halves[k], :], HALF)
        for k in (1, 2, 0):
            for pair in range(2):
                out = jnp.dot(
                    normed[...], w[k, :, pair * 256 : pair * 256 + 256], preferred_element_type=F32
                )
                if k == 0:
                    out = out * QSCALE
                out = out.astype(BF16)
                at = slice((2 - k) * 128, (3 - k) * 128)
                stage[n, 2 * pair, :, at] = out[:, :128]
                stage[n, 2 * pair + 1, :, at] = out[:, 128:]

    def query_rows(piece, count):
        t, half = piece
        return pl.ds(al((t % 2) * 256 + (t // 2) * ROWS + half * HALF, HALF), count)

    both = pl.ds(0, 256)
    third = pl.ds(256, 128)
    lanes = pl.ds(0, HEAD_DIM)

    def pieces(n):
        if n in (0, 3):
            piece = stages[n][0]
            return ((pl.ds(0, ROWS), pl.ds(al(piece[0] * ROWS, ROWS), ROWS), query_rows(piece, ROWS)),)
        return tuple((halves[k], rows_of(piece), query_rows(piece, HALF)) for k, piece in enumerate(stages[n]))

    def hand_out(n):
        for k, (buf, sem, part) in enumerate(((kx, k_recv, both), (qx, q_recv, third))):
            for d in (2, 1, 3):
                h = (p + d) % 4
                to = {"seq": me.seq(h, me.gq(p, g) if k else g)}
                slot = p if k else g * 4 + p
                for half, (src, dst, dst_q) in enumerate(pieces(n)):
                    send(
                        stage.at[n, h, src, part], buf.at[slot, dst_q if k else dst, lanes if k else both],
                        a_send.at[n, d - 1, k, half], sem.at[n], to,
                    )
        for src, dst, _ in pieces(n):
            kx[g * 4 + p, dst, 0:256] = stage[n, p, src, 0:256]

        @pl.when(flip == 1)
        def _():
            for half, (src, _, dst) in enumerate(pieces(n)):
                remote(
                    stage.at[n, p, src, third], qx.at[p, dst, lanes],
                    a_send.at[n, 3, 0, half], qs_recv.at[n], {"seq": me.seq(p, 3 - g)},
                ).start()

        @pl.when(flip == 0)
        def _():
            for src, _, dst in pieces(n):
                qx[p, dst, 0:128] = stage[n, p, src, 256:384]

    def stage_in(count, buf, sem):
        arrive(buf.at[pl.ds(0, count), pl.ds(0, ROWS), lanes if buf is qx else both], sem)

    def ring_out(n):
        stage_in(3, kx, k_recv.at[n])
        for direction in (0, 1):
            to = {"seq": me.seq(p, gp if direction == 0 else gm)}
            for half, (_, dst, _) in enumerate(pieces(n)):
                ref = kx.at[pl.ds(g * 4, 4), dst, both]
                send(ref, ref, g_send.at[direction, n, half], gk_recv.at[direction, n], to)

    def relay(n):
        for direction in sorted(set(ONWARD)):
            stage_in(4, kx, gk_recv.at[direction, n])
            source, to = (gm, gp) if direction == 0 else (gp, gm)
            if ONWARD[0] == ONWARD[1]:
                runs = pieces(n)
            else:
                runs = ((0, rows_of(stages[n][direction]), 0),)
            for half, (_, dst, _) in enumerate(runs):
                ref = kx.at[pl.ds(source * 4, 4), dst, both]
                send(ref, ref, g_send.at[direction, n, 2 + half], r_recv.at[n], {"seq": me.seq(p, to)})

    def wo_rows(t, k, first, count):
        return wo.at[pl.ds(al(t * BLOCK + c * 256 + k * 64 + first, 32), count), :]

    def w1_copy(direction, k):
        to = zp if direction == 0 else zm
        t, first = ((z, 0), (z, 32), (zm, 0))[k] if direction == 0 else ((z, 32), (z, 0), (zp, 32))[k]
        ref = wo_rows(t, g, first, 32)
        return remote(ref, ref, w1_send.at[direction, k], w1_recv.at[direction, k], {"tensor": to})

    def w1_arrive(direction, k):
        arrive(wo.at[pl.ds(0, 32), :], w1_recv.at[direction, k])

    def w2_own():
        copies = []
        for direction in (0, 1):
            to = {"seq": me.seq(p, gp if direction == 0 else gm)}
            for k, t in enumerate((zp, zm, z2)):
                ref = wo_rows(t, g, 0, 64)
                copies.append(remote(ref, ref, w2_send.at[direction, k], w2_recv.at[direction], to))
        return copies

    def w2_relay():
        copies = []
        for direction in (0, 1):
            source, to = (gm, gp) if direction == 0 else (gp, gm)
            for k, ref in enumerate(
                (wo_rows(zm if direction else zp, source, 0, 64), wo_rows(z2, source, 32 * direction, 32))
            ):
                copies.append(
                    remote(ref, ref, w2_send.at[direction, 3 + k], w2r_recv.at[direction], {"seq": me.seq(p, to)})
                )
        return copies

    def d2d(n):
        k = (g, gm, gp, g2)[n]
        return [
            remote(ref, ref, d_send.at[n, i], d_recv, {"dp": 1 - c})
            for i, ref in enumerate(wo_rows(t, k, 0, 64) for t in (zp, zm, z2))
        ]

    def start(copies):
        for copy in copies:
            copy.start()

    small_in[0].wait()
    for copy in w_in:
        copy.wait()
    start(late_in)
    start(small_in[1:])
    project(0)
    hand_out(0)

    length = vf_ref[c]
    lane = lax.broadcasted_iota(jnp.int32, (BLOCK, 128), 1)
    row = lax.broadcasted_iota(jnp.int32, (BLOCK, 128), 0)

    def fill(slot, carry):
        block = me.seq(slot % 4, slot // 4)
        frame = 2 * block + row // TOK_FRAME
        bias = jnp.where((lane == 0) & (frame >= length), NEG, 0.0)
        mine = 0
        for i in range(4):
            mine = mine + (lane == 1 + i).astype(jnp.int32) * (
                me.seq(i, me.gq(i, g)) == block
            ).astype(jnp.int32)
        bias = jnp.where((mine > 0) & (row >= TOK_FRAME), NEG, bias)
        kx[slot, :, 256:384] = bias.astype(BF16)
        vt[slot, 128:DEPTH, :] = jnp.ones((DEPTH - 128, BLOCK), BF16)
        return carry

    lax.fori_loop(0, 16, fill, 0)
    kx[16, :, 0:256] = jnp.zeros((BLOCK, 256), BF16)
    kx[16, :, 256:384] = jnp.where(lane == 0, NEG, 0.0).astype(BF16)
    vt[16] = jnp.zeros((DEPTH, BLOCK), BF16)
    for i in range(4):
        on = (lane == 0) | ((lane == 1 + i) & (row % 256 < ROWS))
        qx[i, :, 128:256] = jnp.where(on, 1.0, 0.0).astype(BF16)

    tok_wait(0, 0, zm, 0)
    tok_send(0, 2, zm, 0)
    tok_wait(1, 0, zp, 1)
    tok_send(1, 2, zp, 1)
    ring_out(0)
    project(1)
    hand_out(1)
    tok_wait(0, 1, zm, 1)
    tok_wait(1, 1, zp, 0)
    project(2)
    hand_out(2)
    ring_out(1)
    relay(0)
    tok_wait(0, 2, z2, 0)
    tok_wait(1, 2, z2, 1)
    project(3)
    hand_out(3)
    late_in[0].wait()
    start([w1_copy(0, 0), w1_copy(1, 0), w1_copy(0, 1), w1_copy(1, 1)])
    ring_out(2)
    relay(1)
    ring_out(3)
    relay(2)
    for n in range(4):
        stage_in(3, qx, q_recv.at[n])

        @pl.when(flip == 1)
        def _():
            stage_in(1, qx, qs_recv.at[n])

    def turn(gg):
        def body(j, carry):
            vt[gg * 4 + j, 0:128, :] = kx[gg * 4 + j, :, 0:128].T
            return carry

        lax.fori_loop(0, 4, body, 0)

    w1_arrive(0, 0)
    w1_copy(0, 2).start()
    w1_arrive(1, 0)
    w1_copy(1, 2).start()
    turn(g)
    relay(3)
    for direction in (0, 1):
        for k in (1, 2):
            w1_arrive(direction, k)
    start(w2_own())
    start(d2d(0))
    for direction in (0, 1):
        if direction not in ONWARD:
            for n in range(4):
                stage_in(4, kx, gk_recv.at[direction, n])
    turn(gm)
    turn(gp)
    for n in range(4):
        stage_in(4, kx, r_recv.at[n])
    turn(g2)

    def slot_of(b, count):
        pad = (b >= count).astype(jnp.int32)
        slot = (1 - c) * (lax.rem(b, 4) * 4 + lax.div(b, 4)) + c * b
        return slot + pad * (16 - slot)

    counts = [me.seq(i, me.gq(i, g)) + 1 for i in range(4)]
    first = [0]
    for count in counts:
        first.append(first[-1] + (count + 1) // 2)
    turns = first[4]

    def pick(at_i, choices):
        return sum(((at_i == k).astype(jnp.int32) * value for k, value in enumerate(choices)), 0)

    def unit(u):
        past = (u >= 2 * turns).astype(jnp.int32)
        u = u - past * (u - 2 * turns + 1)
        a = (u >= turns).astype(jnp.int32)
        v = u - a * turns
        i = sum(((v >= first[k]).astype(jnp.int32) for k in (1, 2, 3)), 0)
        j = v - pick(i, first[:4])
        count = pick(i, counts)
        slots = tuple(slot + past * (16 - slot) for slot in (slot_of(2 * j, count), slot_of(2 * j + 1, count)))
        return a, i, *slots

    def score(now):
        a, i, *slots = now
        for k, slot in enumerate(slots):
            s0[k * BLOCK : (k + 1) * BLOCK, :] = lax.dot_general(
                kx[slot, :, 128:384], qx[i, pl.ds(al(a * 256, 256), 256), :], (((1,), (1,)), ((), ())),
                preferred_element_type=F32,
            )

    def soften(now):
        a, i, *_ = now
        before = m_s[a * 4 + i, 0:1, :]
        peak = jnp.full((8, 256), -1e38, F32)
        for r in range(0, 2 * BLOCK, 128):
            peak = jnp.maximum(peak, jnp.max(s0[r : r + 128, :].reshape(16, 8, 256), axis=0))
        peak = jnp.maximum(before, jnp.max(peak, axis=0, keepdims=True))
        m_s[a * 4 + i, 0:1, :] = peak
        m_s[8, 0:1, :] = jnp.exp2(before - peak)
        for r in range(0, 2 * BLOCK, 128):
            s1[r : r + 128, :] = jnp.exp2(s0[r : r + 128, :] - peak).astype(BF16)

    def gather(now):
        a, i, *slots = now
        out = acc[a * 4 + i] * m_s[8, 0:1, :]
        for k, slot in enumerate(slots):
            out = out + jnp.dot(vt[slot], s1[k * BLOCK : (k + 1) * BLOCK, :], preferred_element_type=F32)
        acc[a * 4 + i] = out

    def back(i, a):
        rows = pl.ds(a * 256, 256)
        return remote(
            o_stage.at[i, rows, :], mx.at[z, p, rows, :], o_send.at[i, a], o_recv.at[p, a],
            {"seq": me.seq(i, me.gq(i, g))},
        )

    def o_arrive(a):
        rows = pl.ds(a * 256, 256)
        for d in (1, 2, 3):
            h = (p + d) % 4
            arrive(mx.at[z, h, rows, :], o_recv.at[h, a])

        @pl.when(flip == 1)
        def _():
            arrive(mx.at[z, p, rows, :], o_recv.at[p, a])

    def mx_copy(a, direction, k):
        to = zp if direction == 0 else zm
        t, half = ((z, 0), (z, 1), (zm, 0))[k] if direction == 0 else ((z, 1), (z, 0), (zp, 1))[k]
        ref = mx.at[t, :, pl.ds(a * 256 + half * ROWS, ROWS), :]
        return remote(ref, ref, m_send.at[a, direction, k], m_recv.at[a, direction, k], {"tensor": to})

    def mx_arrive(a, direction, k):
        arrive(mx.at[z, :, pl.ds(0, ROWS), :], m_recv.at[a, direction, k])

    def mx_own(a):
        start([mx_copy(a, 0, 0), mx_copy(a, 1, 0), mx_copy(a, 0, 1), mx_copy(a, 1, 1)])

    def mx_relay(a):
        for direction in (0, 1):
            mx_arrive(a, direction, 0)
            mx_copy(a, direction, 2).start()

    def w2_onward():
        for direction in (0, 1):
            arrive(wo.at[pl.ds(0, 192), :], w2_recv.at[direction])
        start(w2_relay())
        start(d2d(1))
        start(d2d(2))

    def give_back(a):
        for i in range(4):
            rows = pl.ds(a * 256, 256)
            out = acc[a * 4 + i, 0:128, :] / acc[a * 4 + i, 128:129, :]
            o_stage[i, rows, :] = out.T.astype(BF16)
            stays = (1 - flip) * (p == i).astype(jnp.int32)

            @pl.when(stays == 0)
            def _():
                back(i, a).start()

            @pl.when(stays == 1)
            def _():
                mx[z, p, rows, :] = o_stage[i, rows, :]

    for k in range(8):
        m_s[k] = jnp.full((8, 256), -1e38, F32)
        acc[k] = jnp.zeros((DEPTH, 256), F32)
    def w2_last():
        for direction in (0, 1):
            arrive(wo.at[pl.ds(0, 96), :], w2r_recv.at[direction])
        start(d2d(3))

    score(unit(0))
    soften(unit(0))
    score(unit(1))

    per = UNROLL
    half_way = (turns + per - 1) // per

    def turn_step(n, carry):
        @pl.when(n == half_way)
        def _():
            give_back(0)

        @pl.when(n == half_way + HOOKS[0] // per)
        def _():
            o_arrive(0)
            mx_own(0)

        pl.when(n == HOOKS[1] // per)(w2_onward)
        units = [*carry, *(unit((n + 1) * per + k) for k in (2, *range(3, per + 2)))]
        for k in range(per):
            gather(carry[k])
            soften(carry[k + 1])
            score(carry[k + 2])
        return tuple(units[per:])

    lax.fori_loop(0, (2 * turns + per - 1) // per, turn_step, tuple(unit(k) for k in range(per + 2)))
    give_back(1)

    mx_relay(0)
    w2_last()
    o_arrive(1)
    mx_own(1)
    for copy in small_in[1:]:
        copy.wait()
    for direction in (0, 1):
        for k in range(3):
            ref = tok.at[0, halves[0], :]
            remote(ref, ref, ts_sem.at[direction, k], ts_sem.at[direction, k], {"tensor": zp}).wait_send()

    def frame_rows(a):
        for direction in (0, 1):
            for k in (1, 2):
                mx_arrive(a, direction, k)

    def out_project(a):
        rows = pl.ds(a * 256, 256)

        for n in range(4):
            cols = slice(n * 512, n * 512 + 512)
            lhs = jnp.concatenate([mx[t, h, rows, :] for t in range(4) for h in range(4)], axis=1)
            x = jnp.dot(lhs, wo[:, cols], preferred_element_type=F32)
            for k in (0, 1):
                t = a + 2 * k
                tok[t, :, cols] = (tok[t, :, cols].astype(F32) + x[k * ROWS : (k + 1) * ROWS]).astype(BF16)
        for k in (0, 1):
            norm_rows(tok.at[a + 2 * k], gain2_ref, nrm.at[pl.ds(k * ROWS, ROWS), :], ROWS)

    lo, hi = halves
    ways = ((zp, lo, hi), (zm, hi, lo))

    def mid_copy(direction, n):
        to, rows, _ = ways[direction]
        cols = pl.ds(n * 512, 512)
        return remote(
            part.at[z2, rows, cols], mid.at[direction, :, cols], rs_send.at[direction, n],
            mid_recv.at[direction, n], {"tensor": to},
        )

    def direct_copy(direction):
        to, _, rows = ways[direction]
        return remote(
            part.at[to, rows, :], fin.at[direction, rows, :], rs_send.at[direction, 4],
            fin_recv.at[direction, 0], {"tensor": to},
        )

    def sum_copy(direction, n):
        to, rows, _ = ways[direction]
        cols = pl.ds(n * 512, 512)
        return remote(
            part.at[to, rows, cols], fin.at[direction, rows, cols], rs_send.at[direction, 5 + n],
            fin_recv.at[direction, 1], {"tensor": to},
        )

    def up_down(a, between=lambda: None):
        for n in range(4):
            cols = slice(n * 512, n * 512 + 512)
            x = jnp.dot(nrm[...], wu[:, cols], preferred_element_type=F32)
            up[:, cols] = gelu(x).astype(BF16)

        for n in range(4):
            cols = slice(n * 512, n * 512 + 512)
            x = jnp.dot(up[...], wd[:, cols], preferred_element_type=F32)
            for k in (0, 1):
                rows = x[k * ROWS : (k + 1) * ROWS]
                part[a + 2 * k, :, cols] = rows.astype(BF16)
                rows = jnp.sum(rows.reshape(16, 8, 512), axis=0)
                fs[k, :, cols] = fs[k, :, cols] + rows if a else rows
            if n == 3:
                between()
            if a == 1 and n < 3:
                continue

            @pl.when(z2 % 2 == a)
            def _():
                for m in range(4) if a else (n,):
                    for direction in (0, 1):
                        mid_copy(direction, m).start()

    def rs_first(a):
        for t, direction in ((zp, 0), (zm, 1)):

            @pl.when(t % 2 == a)
            def _():
                direct_copy(direction).start()

    def rs_sums(a):
        @pl.when(zp % 2 == a)
        def _():
            for n in range(4):
                cols = slice(n * 512, n * 512 + 512)
                for direction, (t, half) in enumerate(((zp, 0), (zm, 64))):
                    arrive(mid.at[direction, :, pl.ds(n * 512, 512)], mid_recv.at[direction, n])
                    rows = slice(half, half + 64)
                    part[t, rows, cols] = (
                        part[t, rows, cols].astype(F32) + mid[direction, :, cols].astype(F32)
                    ).astype(BF16)
                    sum_copy(direction, n).start()

    frame_rows(0)
    arrive(wo.at[pl.ds(0, 768), :], d_recv)
    out_project(0)
    mx_relay(1)
    late_in[1].wait()
    late_in[2].wait()
    up_down(0)
    rs_first(0)
    frame_rows(1)
    out_project(1)
    def residual(i, total):
        at = pl.ds(al(i * 16, 16), 16)
        return total + jnp.sum(tok[z, at, :].astype(F32).reshape(2, 8, D), axis=0)

    fs[2] = lax.fori_loop(0, 8, residual, jnp.zeros((8, D), F32))

    def sums_out():
        for k in (0, 1):
            mine = (z // 2 == k).astype(F32)
            zs[z, k : k + 1, :] = jnp.sum(fs[k] + fs[2] * mine, axis=0, keepdims=True)
        for d in (2, 1, 3):
            send(zs.at[z], zs.at[z], z_send.at[d - 1], z_recv.at[z], {"tensor": (z + d) % 4})

    rs_sums(0)
    up_down(1, sums_out)
    rs_first(1)
    for d in (1, 2, 3):
        t = (z + d) % 4
        arrive(zs.at[t], z_recv.at[t])
    means[s] = (zs[0] + zs[1] + zs[2] + zs[3]) * (1.0 / TOK_FRAME)
    steps = sorted(((dy, dx) for dy in range(4) for dx in range(4)), key=lambda d: -min(d[0], 4 - d[0]) - min(d[1], 4 - d[1]))
    for k, (dy, dx) in enumerate(steps[:15]):
        to = {"seq": (s // 4 + dy) % 4 * 4 + (s % 4 + dx) % 4}
        send(means.at[s], means.at[s], s_send.at[k], s_recv.at[s], to)
    rs_sums(1)
    for d in range(1, 16):
        t = (s + d) % 16
        arrive(means.at[t], s_recv.at[t])
    frame = 2 * lax.broadcasted_iota(jnp.int32, (16, 2, 128), 0) + lax.broadcasted_iota(jnp.int32, (16, 2, 128), 1)
    pg, pb, vw = small[2:3, :], small[3:4, :], small[4:5, :]

    def scan(i, state):
        m = means[i]
        gate = jax.nn.sigmoid(m * pg + pb)
        source = (1.0 - gate) * m
        for k in (0, 1):
            new = gate[k : k + 1] * state + source[k : k + 1]
            state = jnp.where(2 * i + k < length, new, state)
            states[i, k : k + 1, :] = state
        return state

    lax.fori_loop(0, 16, scan, jnp.zeros((1, D), F32))
    total = jnp.sum(states[...] * vw.reshape(1, 1, D), axis=-1, keepdims=True)
    values = jnp.where(frame < length, jnp.broadcast_to(total, (16, 2, 128)), 0.0)
    vals[0] = values
    send(vals.at[0], vals.at[1], v_sem.at[0], v_sem.at[1], {"dp": 1 - c})

    for direction in (0, 1):
        for k in (0, 1):
            arrive(fin.at[direction, lo, :], fin_recv.at[direction, k])

    def output(i, carry):
        at = pl.ds(al(i * 16, 16), 16)
        total = part[z, at, :].astype(F32) + fin[0, at, :].astype(F32) + fin[1, at, :].astype(F32)
        hid_ref[at, :] = (tok[z, at, :].astype(F32) + total).astype(BF16)
        return carry

    lax.fori_loop(0, 8, output, 0)

    arrive(vals.at[1], v_sem.at[1])

    def gaps(v, n):
        valid = frame < n
        reward = jnp.sum(jnp.where(frame == n - 1, v, 0.0), axis=(0, 1), keepdims=True)
        return valid, jnp.where(valid, reward - v, 0.0)

    other = vf_ref[1 - c]
    count = (length + other).astype(F32)
    valid, gap = gaps(values, length)
    valid_o, gap_o = gaps(vals[1], other)
    add = lambda a: jnp.sum(a, axis=(0, 1), keepdims=True)
    mean = (add(gap) + add(gap_o)) / count
    centered = jnp.where(valid, gap - mean, 0.0)
    centered_o = jnp.where(valid_o, gap_o - mean, 0.0)
    variance = (add(centered * centered) + add(centered_o * centered_o)) / count
    adv = jnp.where(valid, centered * lax.rsqrt(variance + 1e-5), 0.0)
    lane = lax.broadcasted_iota(jnp.int32, (1, 128), 1)

    def own_pair(a):
        first = jnp.sum(jnp.where(frame == 2 * s, a, 0.0), axis=(0, 1))
        second = jnp.sum(jnp.where(frame == 2 * s + 1, a, 0.0), axis=(0, 1))
        return jnp.where(lane == 0, first.reshape(1, 128), second.reshape(1, 128))[:, 0:2]

    fv_ref[...] = own_pair(values)
    adv_ref[...] = own_pair(adv)
    @pl.when(flip == 1)
    def _():
        for n in range(4):
            for half, (src, _, dst) in enumerate(pieces(n)):
                remote(
                    stage.at[n, p, src, third], qx.at[p, dst, lanes],
                    a_send.at[n, 3, 0, half], qs_recv.at[n], {"seq": me.seq(p, 3 - g)},
                ).wait_send()

    for i in range(4):
        stays = (1 - flip) * (p == i).astype(jnp.int32)

        @pl.when(stays == 0)
        def _():
            for a in (0, 1):
                back(i, a).wait_send()

    rest = [w1_copy(d, k) for d in (0, 1) for k in range(3)]
    rest += w2_own() + w2_relay() + [copy for n in range(4) for copy in d2d(n)]
    rest += [mx_copy(a, d, k) for a in (0, 1) for d in (0, 1) for k in range(3)]
    for d in (0, 1):
        rest += [direct_copy(d)] + [copy(d, n) for copy in (mid_copy, sum_copy) for n in range(4)]
    for copy in rest + sends:
        copy.wait_send()


def hand_over(hid_ref, fv_ref, adv_ref, hid_out, fv_out, adv_out, sem):
    copies = [
        pltpu.make_async_copy(hid_ref, hid_out.at[0], sem.at[0]),
        pltpu.make_async_copy(fv_ref, fv_out, sem.at[1]),
        pltpu.make_async_copy(adv_ref, adv_out, sem.at[2]),
    ]
    for copy in copies:
        copy.start()
    for copy in copies:
        copy.wait()


def local(
    tokens, attn_gain, w_qkv, w_out, mlp_gain, w_up, w_down, pool_gain, pool_bias, value_weight, valid_frames
):
    vmem = pltpu.VMEM
    dma = pltpu.SemaphoreType.DMA
    inside = pl.BlockSpec(memory_space=pltpu.VMEM)
    outside = pl.BlockSpec(memory_space=pl.ANY)
    hidden, values, advantages = pl.pallas_call(
        layer_kernel,
        out_shape=(
            jax.ShapeDtypeStruct((ROWS, D), BF16),
            jax.ShapeDtypeStruct((1, 2), F32),
            jax.ShapeDtypeStruct((1, 2), F32),
        ),
        in_specs=[pl.BlockSpec(memory_space=pltpu.SMEM)] + [outside] * 10,
        out_specs=(inside,) * 3,
        scratch_shapes=[
            vmem((4, ROWS, D), BF16),
            vmem((3, D, BLOCK), BF16),
            vmem((8, D), F32),
            vmem((ROWS, D), BF16),
            vmem((4, 4, ROWS, 384), BF16),
            vmem((4, BLOCK, 256), BF16),
            vmem((17, BLOCK, 384), BF16),
            vmem((17, DEPTH, BLOCK), BF16),
            vmem((9, 8, 256), F32),
            vmem((8, DEPTH, 256), F32),
            vmem((2 * BLOCK, 256), F32),
            vmem((2 * BLOCK, 256), BF16),
            vmem((4, BLOCK, HEAD_DIM), BF16),
            vmem((4, 4, BLOCK, HEAD_DIM), BF16),
            vmem((D, D), BF16),
            vmem((D, D), BF16),
            vmem((D, D), BF16),
            vmem((4, ROWS, D), BF16),
            vmem((2, 64, D), BF16),
            vmem((2, ROWS, D), BF16),
            vmem((2 * ROWS, D), BF16),
            vmem((2 * ROWS, D), BF16),
            vmem((3, 8, D), F32),
            vmem((4, 2, D), F32),
            vmem((16, 2, D), F32),
            vmem((16, 2, D), F32),
            vmem((2, 16, 2, 128), F32),
            dma((6,)),
            dma((6,)),
            dma((2, 3)),
            dma((2, 3)),
            dma((4, 4, 2, 2)),
            dma((4,)),
            dma((4,)),
            dma((4,)),
            dma((2, 4, 4)),
            dma((2, 4)),
            dma((4,)),
            dma((4, 2)),
            dma((4, 2)),
            dma((2, 2, 3)),
            dma((2, 2, 3)),
            dma((2, 3)),
            dma((2, 3)),
            dma((2, 5)),
            dma((2,)),
            dma((2,)),
            dma((4, 3)),
            dma,
            dma((2, 9)),
            dma((2, 4)),
            dma((2, 2)),
            dma((3,)),
            dma((4,)),
            dma((15,)),
            dma((16,)),
            dma((2,)),
        ],
        compiler_params=pltpu.CompilerParams(
            collective_id=0, has_side_effects=True, vmem_limit_bytes=63 * 2**20
        ),
        cost_estimate=pl.CostEstimate(flops=4 * 10**10, bytes_accessed=4 * 10**7, transcendentals=10**7),
    )(
        valid_frames, tokens[0], w_qkv, w_out, w_up, w_down,
        *(v.reshape(1, D) for v in (attn_gain, mlp_gain, pool_gain, pool_bias, value_weight)),
    )
    return pl.pallas_call(
        hand_over,
        out_shape=(
            jax.ShapeDtypeStruct((1, ROWS, D), BF16),
            jax.ShapeDtypeStruct((1, 2), F32),
            jax.ShapeDtypeStruct((1, 2), F32),
        ),
        in_specs=[inside] * 3,
        out_specs=(outside,) * 3,
        scratch_shapes=[dma((3,))],
    )(hidden, values, advantages)


def solution(mesh):
    in_specs = (
        P("dp", ("seq", "tensor"), None),
        P(),
        P(None, None, "tensor"),
        P("tensor", None),
        P(),
        P(None, "tensor"),
        P("tensor", None),
        P(),
        P(),
        P(),
        P(),
    )
    out_specs = (P("dp", ("seq", "tensor"), None), P("dp", "seq"), P("dp", "seq"))
    return jax.shard_map(local, mesh=mesh, in_specs=in_specs, out_specs=out_specs, check_vma=False)
```
